128 devices in a mesh: cp: 2 (over core), fsdp: 64 (over z, y, x).
Axes of the slice: x: 4, y: 4, z: 4, core: 2. Of those that a mesh axis runs over, the one named last changes fastest.
Arguments:
- tokens: int32 [1024, 256], P('fsdp', 'cp')
- lengths: int32 [1024], P('fsdp')
- embed_table: bfloat16 [33, 640], replicated
- layer_vecs: float32 [9, 640], P(None, 'fsdp')
- w_qkv: bfloat16 [640, 3, 20, 32], P('fsdp')
- w_out: bfloat16 [640, 640], P('fsdp')
- w_up: bfloat16 [640, 2560], P('fsdp')
- b_up: float32 [2560], P('fsdp')
- w_down: bfloat16 [2560, 640], P('fsdp')
- grad_out: bfloat16 [1024, 256, 640], P('fsdp', 'cp')
Outputs:
- output 1: bfloat16 [1024, 256, 640], P('fsdp', 'cp')
- output 2: float32 [33, 640], replicated
- output 3: float32 [9, 640], P(None, 'fsdp')
- output 4: float32 [640, 3, 20, 32], P('fsdp')
- output 5: float32 [640, 640], P('fsdp')
- output 6: float32 [640, 2560], P('fsdp')
- output 7: float32 [2560], P('fsdp')
- output 8: float32 [2560, 640], P('fsdp')
All inputs are finite; a program needn't handle non-finite values.
Results may differ from the reference program's by a relative error of at most 0.00989253.
Values are sent between devices in bfloat16 or wider.
A program may use at most 1 GiB of HBM per device.

```python
import jax
import jax.numpy as jnp
from jax import lax

NUM_SEQS = 1024
SEQ_LEN = 256
MODEL_DIM = 640
NUM_HEADS = 20
FFN_DIM = 2560
VOCAB_SIZE = 33
BOS_ID = 0
PAD_ID = 1
EOS_ID = 2
MASK_ID = 32
HEAD_DIM = MODEL_DIM // NUM_HEADS
LN_EPS = 1e-5
ROPE_BASE = 10000.0
TRAIN_RATIO = 0.15 * 0.8
NEG_BIG = -1e30


def draw_tokens(rng_key):
    key_list = jax.random.split(rng_key, 4)
    lengths = jax.random.randint(key_list[0], (NUM_SEQS,), SEQ_LEN // 4, SEQ_LEN + 1)
    lengths = lengths.at[0].set(SEQ_LEN).at[1].set(SEQ_LEN // 4)
    positions = jnp.arange(SEQ_LEN)[None, :]
    len_col = lengths[:, None]
    residues = jax.random.randint(key_list[1], (NUM_SEQS, SEQ_LEN), 4, 31)
    win_start = jax.random.randint(key_list[2], (NUM_SEQS, 1), 0, SEQ_LEN)
    in_win = (positions >= win_start) & (positions < win_start + SEQ_LEN // 4)
    hit_draw = jax.random.randint(key_list[3], (NUM_SEQS, SEQ_LEN), 0, 100)
    is_mask = hit_draw < jnp.where(in_win, 45, 5)
    tokens = jnp.where(is_mask, MASK_ID, residues)
    tokens = jnp.where(positions >= len_col, PAD_ID, tokens)
    tokens = jnp.where(positions == len_col - 1, EOS_ID, tokens)
    tokens = jnp.where(positions == 0, BOS_ID, tokens)
    return tokens.astype(jnp.int32), lengths.astype(jnp.int32)


def setup_inputs(seed: int = 0) -> dict:
    key_list = jax.random.split(jax.random.key(seed), 9)
    tokens, lengths = draw_tokens(key_list[0])
    embed_table = jax.random.normal(key_list[1], (VOCAB_SIZE, MODEL_DIM), jnp.float32)
    row_scale = jnp.array([0.2, 0.3, 0.3, 0.3, SEQ_LEN ** -0.5, 0.3, 0.2, 0.3, 0.3], jnp.float32)
    row_shift = jnp.array([1.0, 0.0, 0.0, 0.0, 0.0, 0.0, 1.0, 0.0, 0.0], jnp.float32)
    layer_vecs = row_shift[:, None] + row_scale[:, None] * jax.random.normal(key_list[2], (9, MODEL_DIM), jnp.float32)
    w_qkv = jax.random.normal(key_list[3], (MODEL_DIM, 3, NUM_HEADS, HEAD_DIM), jnp.float32) * MODEL_DIM ** -0.5
    w_out = jax.random.normal(key_list[4], (MODEL_DIM, MODEL_DIM), jnp.float32) * (SEQ_LEN / (2.0 * MODEL_DIM)) ** 0.5
    w_up = jax.random.normal(key_list[5], (MODEL_DIM, FFN_DIM), jnp.float32) * MODEL_DIM ** -0.5
    b_up = 0.5 * jax.random.normal(key_list[6], (FFN_DIM,), jnp.float32)
    w_down = jax.random.normal(key_list[7], (FFN_DIM, MODEL_DIM), jnp.float32) * FFN_DIM ** -0.5
    grad_out = jax.random.normal(key_list[8], (NUM_SEQS, SEQ_LEN, MODEL_DIM), jnp.float32)
    return {
        'tokens': tokens,
        'lengths': lengths,
        'embed_table': embed_table.astype(jnp.bfloat16),
        'layer_vecs': layer_vecs,
        'w_qkv': w_qkv.astype(jnp.bfloat16),
        'w_out': w_out.astype(jnp.bfloat16),
        'w_up': w_up.astype(jnp.bfloat16),
        'b_up': b_up,
        'w_down': w_down.astype(jnp.bfloat16),
        'grad_out': grad_out.astype(jnp.bfloat16),
    }


def rounded(z_in):
    return z_in + lax.stop_gradient(z_in.astype(jnp.bfloat16).astype(jnp.float32) - z_in)


def layer_norm(z_in, ln_gain, ln_bias):
    row_mean = jnp.mean(z_in, axis=-1, keepdims=True)
    centered = z_in - row_mean
    row_var = jnp.mean(centered * centered, axis=-1, keepdims=True)
    return centered * lax.rsqrt(row_var + LN_EPS) * ln_gain + ln_bias


def rotate(z_in, cos_t, sin_t):
    lower_half, upper_half = jnp.split(z_in, 2, axis=-1)
    return jnp.concatenate([lower_half * cos_t - upper_half * sin_t, upper_half * cos_t + lower_half * sin_t], axis=-1)


def one_sequence(params, embed_f32, tok_row, len_row):
    layer_vecs, w_qkv, w_out, w_up, b_up, w_down = params
    positions = jnp.arange(SEQ_LEN)
    is_mask = tok_row == MASK_ID
    key_valid = positions < len_row
    n_mask = jnp.sum(is_mask.astype(jnp.float32))
    drop_scale = (1.0 - TRAIN_RATIO) / (1.0 - n_mask / len_row.astype(jnp.float32))
    keep_scale = jnp.where(is_mask | jnp.logical_not(key_valid), 0.0, drop_scale)
    embedded = embed_f32[tok_row] * keep_scale[:, None]
    norm_in = rounded(layer_norm(embedded, layer_vecs[0], layer_vecs[1]))
    qkv_lin = jnp.dot(norm_in, w_qkv.reshape(MODEL_DIM, 3 * MODEL_DIM)) + layer_vecs[2:5].reshape(3 * MODEL_DIM)
    qkv_lin = qkv_lin.reshape(SEQ_LEN, 3, NUM_HEADS, HEAD_DIM)
    inv_freq = 1.0 / (ROPE_BASE ** (jnp.arange(0, HEAD_DIM, 2, dtype=jnp.float32) / HEAD_DIM))
    angles = positions.astype(jnp.float32)[:, None] * inv_freq[None, :]
    cos_t = jnp.cos(angles)[:, None, :]
    sin_t = jnp.sin(angles)[:, None, :]
    q_heads = rounded(rotate(qkv_lin[:, 0] * HEAD_DIM ** -0.5, cos_t, sin_t))
    k_heads = rounded(rotate(qkv_lin[:, 1], cos_t, sin_t))
    v_heads = rounded(qkv_lin[:, 2])

    def one_head(head_in):
        q_h, k_h, v_h = head_in
        scores = jnp.dot(q_h, k_h.T)
        scores = jnp.where(key_valid[None, :], scores, NEG_BIG)
        return jnp.dot(jax.nn.softmax(scores, axis=-1), v_h)

    per_head = lax.map(jax.checkpoint(one_head), (q_heads.transpose(1, 0, 2), k_heads.transpose(1, 0, 2), v_heads.transpose(1, 0, 2)))
    attn_out = rounded(per_head.transpose(1, 0, 2).reshape(SEQ_LEN, MODEL_DIM))
    resid_mid = embedded + jnp.dot(attn_out, w_out) + layer_vecs[5]
    norm_mid = rounded(layer_norm(resid_mid, layer_vecs[6], layer_vecs[7]))
    gelu_out = rounded(jax.nn.gelu(jnp.dot(norm_mid, w_up) + b_up, approximate=False))
    return resid_mid + jnp.dot(gelu_out, w_down) + layer_vecs[8]


def reference(tokens, lengths, embed_table, layer_vecs, w_qkv, w_out, w_up, b_up, w_down, grad_out):
    params = (layer_vecs, w_qkv.astype(jnp.float32), w_out.astype(jnp.float32), w_up.astype(jnp.float32), b_up, w_down.astype(jnp.float32))
    seq_fn = jax.checkpoint(one_sequence)

    def forward(params_in, embed_f32):
        def per_row(seq_row):
            return seq_fn(params_in, embed_f32, seq_row[0], seq_row[1])
        return lax.map(per_row, (tokens, lengths))

    layer_out, pullback = jax.vjp(forward, params, embed_table.astype(jnp.float32))
    d_params, d_embed = pullback(grad_out.astype(jnp.float32))
    return (layer_out.astype(jnp.bfloat16), d_embed, d_params[0], d_params[1], d_params[2], d_params[3], d_params[4], d_params[5])
```

```python
import functools

import jax
import jax.numpy as jnp
from jax import lax
from jax.experimental import pallas as pl
from jax.experimental.pallas import tpu as pltpu
from jax.sharding import PartitionSpec as P

MASK_ID = 32
LN_EPS = 1e-5
ROPE_BASE = 10000.0
TRAIN_RATIO = 0.15 * 0.8
NEG_BIG = -1e30
SIDE = 4
COLORS = 3
NB = 10
HALF = 5
SMALL_ROWS = 120
MESH_ID = pl.DeviceIdType.MESH
ANY = pl.BlockSpec(memory_space=pl.ANY)

GATHER_ORDER = ((2, 1, 0), (1, 0, 2), (0, 2, 1))
REDUCE_ORDER = ((0, 1, 2), (1, 2, 0), (2, 0, 1))


def my_coords():
    chip = lax.axis_index('fsdp')
    return [chip // 16, lax.rem(chip // 4, 4), lax.rem(chip, 4)]


def moved(coords, dim, by):
    out = list(coords)
    out[dim] = lax.rem(coords[dim] + by + SIDE, SIDE)
    return out


def chip_id(coords):
    return {'fsdp': coords[0] * 16 + coords[1] * 4 + coords[2]}


def entry_barrier(coords, cp):
    barrier = pltpu.get_barrier_semaphore()
    for dim in range(3):
        for by in (1, 2, 3):
            pl.semaphore_signal(barrier, inc=1, device_id=chip_id(moved(coords, dim, by)), device_id_type=MESH_ID)
    pl.semaphore_signal(barrier, inc=1, device_id={'cp': 1 - cp}, device_id_type=MESH_ID)
    pl.semaphore_wait(barrier, 10)


def push(src, dst, send_sem, recv_sem, target):
    return pltpu.make_async_remote_copy(src_ref=src, dst_ref=dst, send_sem=send_sem, recv_sem=recv_sem, device_id=target, device_id_type=MESH_ID)


def gather_kernel(w_loc, s_loc, g_own, t_own, w_all, s_all, g_oth, t_oth, ssem, rsem, fsend, frecv, s_ssem, s_rsem, psend, precv, lsem):
    cp = lax.axis_index('cp')
    me = my_coords()
    mate = {'cp': 1 - cp}
    own_w = pltpu.make_async_copy(w_loc, w_all.at[:, me[0], me[1], me[2]], lsem.at[0])
    own_s = pltpu.make_async_copy(s_loc, s_all.at[me[0], me[1], me[2]], lsem.at[1])
    own_w.start()
    own_s.start()
    entry_barrier(me, cp)
    swap_g = push(g_own.at[pl.ds(8 * (1 - cp), 8)], g_oth, psend.at[0], precv.at[0], mate)
    swap_t = push(t_own.at[pl.ds(8 * (1 - cp), 8)], t_oth, psend.at[1], precv.at[1], mate)
    swap_t.start()

    def region(ref, first, count, dims, at):
        index = [slice(None) if d in dims else at[d] for d in range(3)]
        return ref.at[(pl.ds(first, count), *index)]

    def small_region(dims, at):
        index = [slice(None) if d in dims else at[d] for d in range(3)]
        return s_all.at[tuple(index)]

    forwards = []
    pending = []
    own_s.wait()
    own_w.wait()
    for phase in range(3):
        firsts = {}
        for color in range(COLORS):
            dim = GATHER_ORDER[color][phase]
            done = GATHER_ORDER[color][:phase]
            base = cp * (COLORS * NB) + color * NB
            mine = region(w_all, base, NB, done, me)
            right, left = chip_id(moved(me, dim, 1)), chip_id(moved(me, dim, 3))
            to_right = push(mine, mine, ssem.at[color, phase, 0], rsem.at[color, phase, 0], right)
            to_left = push(mine, mine, ssem.at[color, phase, 1], rsem.at[color, phase, 1], left)
            to_right.start()
            to_left.start()
            firsts[color] = (to_right, to_left)
            pending += [to_right, to_left]
            if color == 0:
                s_mine = small_region(done, me)
                s_right = push(s_mine, s_mine, s_ssem.at[phase, 0], s_rsem.at[phase, 0], right)
                s_left = push(s_mine, s_mine, s_ssem.at[phase, 1], s_rsem.at[phase, 1], left)
                s_right.start()
                s_left.start()
                pending += [s_right, s_left]
        seconds = {}
        for color in range(COLORS):
            dim = GATHER_ORDER[color][phase]
            done = GATHER_ORDER[color][:phase]
            base = cp * (COLORS * NB) + color * NB
            right, left = chip_id(moved(me, dim, 1)), chip_id(moved(me, dim, 3))
            from_left, from_right = moved(me, dim, 3), moved(me, dim, 1)
            to_right, to_left = firsts[color]
            to_right.wait_recv()
            part = region(w_all, base, HALF, done, from_left)
            on_right = push(part, part, ssem.at[color, phase, 2], rsem.at[color, phase, 2], right)
            on_right.start()
            whole_l = region(w_all, base, NB, done, from_left)
            fwd_l = push(whole_l, whole_l, fsend.at[color, phase, 0], frecv.at[color, phase, 0], mate)
            fwd_l.start()
            to_left.wait_recv()
            part = region(w_all, base + HALF, HALF, done, from_right)
            on_left = push(part, part, ssem.at[color, phase, 3], rsem.at[color, phase, 3], left)
            on_left.start()
            whole_r = region(w_all, base, NB, done, from_right)
            fwd_r = push(whole_r, whole_r, fsend.at[color, phase, 1], frecv.at[color, phase, 1], mate)
            fwd_r.start()
            seconds[color] = (on_right, on_left)
            pending += [on_right, on_left]
            forwards += [fwd_l, fwd_r]
            if color == 0:
                s_right.wait_recv()
                s_left.wait_recv()
                s_part = small_region(done, from_left)
                s_on = push(s_part, s_part, s_ssem.at[phase, 2], s_rsem.at[phase, 2], right)
                s_on.start()
                pending.append(s_on)
        for color in range(COLORS):
            dim = GATHER_ORDER[color][phase]
            done = GATHER_ORDER[color][:phase]
            base = cp * (COLORS * NB) + color * NB
            on_right, on_left = seconds[color]
            on_right.wait_recv()
            on_left.wait_recv()
            far = region(w_all, base, NB, done, moved(me, dim, 2))
            fwd_f = push(far, far, fsend.at[color, phase, 2], frecv.at[color, phase, 2], mate)
            fwd_f.start()
            forwards.append(fwd_f)
            if color == 0:
                s_on.wait_recv()
        if phase == 0:
            swap_g.start()
    for copy in forwards:
        copy.wait_recv()
    swap_g.wait()
    swap_t.wait()
    for copy in pending + forwards:
        copy.wait_send()


def gather_all(w_loc, s_loc, grad_out, tokens):
    bf16, f32 = jnp.bfloat16, jnp.float32
    blocks = w_loc.shape[0]
    seqs, pos, width = grad_out.shape
    dma = pltpu.SemaphoreType.DMA
    return pl.pallas_call(
        gather_kernel,
        out_shape=(
            jax.ShapeDtypeStruct((blocks, SIDE, SIDE, SIDE, NB, 128), bf16),
            jax.ShapeDtypeStruct((SIDE, SIDE, SIDE, 8, 128), f32),
            jax.ShapeDtypeStruct((seqs // 2, pos, width), bf16),
            jax.ShapeDtypeStruct((seqs // 2, pos), jnp.int32),
        ),
        in_specs=[ANY] * 4,
        out_specs=(ANY,) * 4,
        scratch_shapes=[dma((3, 3, 4)), dma((3, 3, 4)), dma((3, 3, 3)), dma((3, 3, 3)), dma((3, 3)), dma((3, 3)), dma((2,)), dma((2,)), dma((2,))],
        compiler_params=pltpu.CompilerParams(collective_id=0, has_side_effects=True),
        name='gather_weights',
    )(w_loc, s_loc, grad_out, tokens)


def reduce_kernel(g_all, small, y_oth, g_out, s_out, y_recv, held, pair, ra0, rb0, ra1, rb1, ra2, rb2, s_pair, s_slots, s_acc,
                  lsem, psend, precv, ssem, rsem, s_ssem, s_rsem, osend, orecv, msem):
    cp = lax.axis_index('cp')
    me = my_coords()
    mate = {'cp': 1 - cp}
    per = COLORS * NB
    loads = []
    for color in range(COLORS):
        load = pltpu.make_async_copy(g_all.at[pl.ds(cp * per + color * NB, NB)], held.at[pl.ds(color * NB, NB)], lsem.at[color])
        load.start()
        loads.append(load)
    s_load = pltpu.make_async_copy(small, s_acc, lsem.at[3])
    s_load.start()
    entry_barrier(me, cp)
    sends = []
    s_swap = push(small, s_pair, psend.at[3], precv.at[3], mate)
    s_swap.start()
    swaps = []
    for color in range(COLORS):
        swap = push(g_all.at[pl.ds((1 - cp) * per + color * NB, NB)], pair.at[pl.ds(color * NB, NB)], psend.at[color], precv.at[color], mate)
        swap.start()
        swaps.append(swap)
    y_swap = push(y_oth, y_recv, psend.at[4], precv.at[4], mate)
    y_swap.start()

    bufs = ((ra0, rb0), (ra1, rb1), (ra2, rb2))

    def index_of(dims, at):
        return [slice(None) if d in dims else at[d] for d in range(3)]

    def region(first, count, dims, at):
        return held.at[(pl.ds(first, count), *index_of(dims, at))]

    def start_phase(color, phase):
        dim = REDUCE_ORDER[color][phase]
        rest = REDUCE_ORDER[color][phase + 1:]
        base = color * NB
        ra, rb = bufs[phase]
        right, left = moved(me, dim, 1), moved(me, dim, 3)
        far = moved(me, dim, 2)
        out = [
            push(region(base, HALF, rest, far), ra.at[color, 0], ssem.at[color, phase, 0], rsem.at[color, phase, 0], chip_id(right)),
            push(region(base + HALF, HALF, rest, far), ra.at[color, 1], ssem.at[color, phase, 1], rsem.at[color, phase, 1], chip_id(left)),
            push(region(base + HALF, HALF, rest, right), rb.at[color, 0, pl.ds(HALF, HALF)], ssem.at[color, phase, 2], rsem.at[color, phase, 2], chip_id(right)),
            push(region(base, HALF, rest, left), rb.at[color, 1, pl.ds(0, HALF)], ssem.at[color, phase, 3], rsem.at[color, phase, 3], chip_id(left)),
        ]
        for copy in out:
            copy.start()
        sends.extend(out)
        return out

    def middle(color, phase, copies):
        dim = REDUCE_ORDER[color][phase]
        rest = REDUCE_ORDER[color][phase + 1:]
        base = color * NB
        ra, rb = bufs[phase]
        right, left = moved(me, dim, 1), moved(me, dim, 3)
        copies[0].wait_recv()
        to_r = index_of(rest, right)

        @pl.loop(0, HALF)
        def _(b):
            held[(base + b, *to_r)] += ra[color, 0, b]

        fwd_r = push(region(base, HALF, rest, right), rb.at[color, 0, pl.ds(0, HALF)], ssem.at[color, phase, 4], rsem.at[color, phase, 4], chip_id(right))
        fwd_r.start()
        copies[1].wait_recv()
        to_l = index_of(rest, left)

        @pl.loop(0, HALF)
        def _(b):
            held[(base + HALF + b, *to_l)] += ra[color, 1, b]

        fwd_l = push(region(base + HALF, HALF, rest, left), rb.at[color, 1, pl.ds(HALF, HALF)], ssem.at[color, phase, 5], rsem.at[color, phase, 5], chip_id(left))
        fwd_l.start()
        sends.extend([fwd_r, fwd_l])
        return [fwd_r, fwd_l]

    def finish(color, phase, copies, late):
        rest = REDUCE_ORDER[color][phase + 1:]
        base = color * NB
        ra, rb = bufs[phase]
        copies[2].wait_recv()
        copies[3].wait_recv()
        late[0].wait_recv()
        late[1].wait_recv()
        here = index_of(rest, me)

        @pl.loop(0, NB)
        def _(b):
            held[(base + b, *here)] += rb[color, 0, b] + rb[color, 1, b]

    s_copies = []

    def small_start(phase):
        dim = REDUCE_ORDER[0][phase]
        out = []
        for by in (1, 2, 3):
            out.append(push(s_acc.at[cp], s_slots.at[phase, by - 1], s_ssem.at[phase, by - 1], s_rsem.at[phase, by - 1], chip_id(moved(me, dim, by))))
        for copy in out:
            copy.start()
        return out

    def small_finish(phase, copies):
        dim = REDUCE_ORDER[0][phase]
        for copy in copies:
            copy.wait()
        mine = me[dim]
        total = None
        own = s_acc[cp]
        got = [own] + [s_slots[phase, by] for by in range(3)]
        for coord in range(SIDE):
            gap = lax.rem(mine - coord + SIDE, SIDE)
            value = jnp.where(gap == 0, got[0], jnp.where(gap == 1, got[1], jnp.where(gap == 2, got[2], got[3])))
            total = value if total is None else total + value
        s_acc[cp] = total

    s_load.wait()
    s_swap.wait()
    s_acc[...] = s_acc[...] + s_pair[...]
    s_out_copies = small_start(0)
    started = []
    for color in range(COLORS):
        loads[color].wait()
        swaps[color].wait_recv()

        @pl.loop(0, NB)
        def _(b):
            for z in range(SIDE):
                held[color * NB + b, z] += pair[color * NB + b, z]

        started.append(start_phase(color, 0))
    for phase in range(3):
        late = [middle(color, phase, started[color]) for color in range(COLORS)]
        nxt = []
        for color in range(COLORS):
            finish(color, phase, started[color], late[color])
            if phase < 2:
                nxt.append(start_phase(color, phase + 1))
        small_finish(phase, s_out_copies)
        if phase < 2:
            s_out_copies = small_start(phase + 1)
        started = nxt
    mine = held.at[:, me[0], me[1], me[2]]
    out_far = push(mine, g_out.at[pl.ds(cp * per, per)], osend.at[0], orecv.at[0], mate)
    out_far.start()
    s_far = push(s_acc.at[cp], s_out.at[cp], osend.at[1], orecv.at[1], mate)
    s_far.start()
    out_own = pltpu.make_async_copy(mine, g_out.at[pl.ds(cp * per, per)], msem.at[0])
    out_own.start()
    s_own = pltpu.make_async_copy(s_acc.at[cp], s_out.at[cp], msem.at[1])
    s_own.start()
    for copy in sends:
        copy.wait_send()
    for copy in swaps:
        copy.wait_send()
    y_swap.wait()
    out_own.wait()
    s_own.wait()
    out_far.wait()
    s_far.wait()


def reduce_all(g_all, small, y_oth):
    f32 = jnp.float32
    blocks = g_all.shape[0]
    dma = pltpu.SemaphoreType.DMA
    vm = pltpu.VMEM
    return pl.pallas_call(
        reduce_kernel,
        out_shape=(
            jax.ShapeDtypeStruct((blocks, NB, 128), f32),
            jax.ShapeDtypeStruct(small.shape, f32),
            jax.ShapeDtypeStruct(y_oth.shape, y_oth.dtype),
        ),
        in_specs=[ANY] * 3,
        out_specs=(ANY,) * 3,
        scratch_shapes=[
            vm((blocks // 2, SIDE, SIDE, SIDE, NB, 128), f32),
            vm((blocks // 2, SIDE, SIDE, SIDE, NB, 128), f32),
            vm((COLORS, 2, HALF, SIDE, SIDE, NB, 128), f32),
            vm((COLORS, 2, NB, SIDE, SIDE, NB, 128), f32),
            vm((COLORS, 2, HALF, SIDE, NB, 128), f32),
            vm((COLORS, 2, NB, SIDE, NB, 128), f32),
            vm((COLORS, 2, HALF, NB, 128), f32),
            vm((COLORS, 2, NB, NB, 128), f32),
            vm(small.shape, f32),
            vm((3, 3) + small.shape[1:], f32),
            vm(small.shape, f32),
            dma((4,)), dma((5,)), dma((5,)), dma((3, 3, 6)), dma((3, 3, 6)), dma((3, 3)), dma((3, 3)), dma((2,)), dma((2,)), dma((2,)),
        ],
        compiler_params=pltpu.CompilerParams(collective_id=1, has_side_effects=True, vmem_limit_bytes=62 * 1024 * 1024),
        name='reduce_grads',
    )(g_all, small, y_oth)


def layer_norm(z_in, ln_gain, ln_bias):
    row_mean = jnp.mean(z_in, axis=-1, keepdims=True)
    centered = z_in - row_mean
    row_var = jnp.mean(centered * centered, axis=-1, keepdims=True)
    return centered * lax.rsqrt(row_var + LN_EPS) * ln_gain + ln_bias


def gelu_exact(z_in):
    return jax.nn.gelu(z_in, approximate=False)


def rope_tables(positions, head_dim):
    inv_freq = 1.0 / (ROPE_BASE ** (jnp.arange(0, head_dim, 2, dtype=jnp.float32) / head_dim))
    angles = positions.astype(jnp.float32)[:, None] * inv_freq[None, :]
    return jnp.cos(angles)[:, None, :], jnp.sin(angles)[:, None, :]


def rotate(z_in, cos_t, sin_t):
    lower_half, upper_half = jnp.split(z_in, 2, axis=-1)
    return jnp.concatenate([lower_half * cos_t - upper_half * sin_t, upper_half * cos_t + lower_half * sin_t], axis=-1)


def layer_compute(tokens, lengths, positions, embed_table, vecs_all, w_all, up_b, grad_out):
    f32, bf16 = jnp.float32, jnp.bfloat16
    n_seq, seq_len = tokens.shape
    vocab_size, model_dim = embed_table.shape
    n_heads, head_dim = 20, 32
    mats = w_all.reshape(60, model_dim, 128)
    qkv_w = mats[:15].transpose(1, 0, 2).reshape(model_dim, 3, n_heads, head_dim)
    out_w = mats[15:20].transpose(1, 0, 2).reshape(model_dim, model_dim)
    up_w = mats[20:40].transpose(1, 0, 2).reshape(model_dim, 2560)
    down_w = mats[40:60].reshape(4, 5, model_dim, 128).transpose(0, 2, 1, 3).reshape(2560, model_dim)
    len_col = lengths[:, None]
    is_mask = tokens == MASK_ID
    tok_valid = positions[None, :] < len_col
    mask_count = jnp.sum(is_mask.astype(jnp.int32), axis=1)
    drop_scale = (1.0 - TRAIN_RATIO) / (1.0 - mask_count.astype(f32) / lengths.astype(f32))
    keep_scale = jnp.where(is_mask | jnp.logical_not(tok_valid), 0.0, drop_scale[:, None])[:, :, None]
    one_hot = (tokens[:, :, None] == jnp.arange(vocab_size)).astype(bf16)
    embedded = jnp.einsum('bsv,vd->bsd', one_hot, embed_table, preferred_element_type=f32) * keep_scale
    norm_in32, ln1_pull = jax.vjp(layer_norm, embedded, vecs_all[0], vecs_all[1])
    norm_in = norm_in32.astype(bf16)
    qkv_lin = jnp.einsum('bsd,dthe->bsthe', norm_in, qkv_w, preferred_element_type=f32) + vecs_all[2:5].reshape(3, n_heads, head_dim)
    cos_t, sin_t = rope_tables(positions, head_dim)
    q_rot = rotate(qkv_lin[:, :, 0] * head_dim ** -0.5, cos_t, sin_t).astype(bf16)
    k_rot = rotate(qkv_lin[:, :, 1], cos_t, sin_t).astype(bf16)
    v_val = qkv_lin[:, :, 2].astype(bf16)
    scores = jnp.einsum('bqhd,bkhd->bhqk', q_rot, k_rot, preferred_element_type=f32)
    scores = jnp.where(tok_valid[:, None, None, :], scores, NEG_BIG)
    weights = jax.nn.softmax(scores, axis=-1)
    weights_b = weights.astype(bf16)
    attn32 = jnp.einsum('bhqk,bkhd->bqhd', weights_b, v_val, preferred_element_type=f32)
    attn_out = attn32.astype(bf16).reshape(n_seq, seq_len, model_dim)
    resid_mid = embedded + jnp.einsum('bsd,de->bse', attn_out, out_w, preferred_element_type=f32) + vecs_all[5]
    norm_mid32, ln2_pull = jax.vjp(layer_norm, resid_mid, vecs_all[6], vecs_all[7])
    norm_mid = norm_mid32.astype(bf16)
    up_lin = jnp.einsum('bsd,df->bsf', norm_mid, up_w, preferred_element_type=f32) + up_b
    gelu32, gelu_pull = jax.vjp(gelu_exact, up_lin)
    gelu_out = gelu32.astype(bf16)
    layer_out = (resid_mid + jnp.einsum('bsf,fd->bsd', gelu_out, down_w, preferred_element_type=f32) + vecs_all[8]).astype(bf16)

    grad32 = grad_out.astype(f32)
    d_down = jnp.einsum('bsf,bsd->fd', gelu_out, grad_out, preferred_element_type=f32)
    d_gelu = jnp.einsum('bsd,fd->bsf', grad_out, down_w, preferred_element_type=f32)
    d_up_lin = gelu_pull(d_gelu)[0]
    d_up_b = d_up_lin.astype(bf16)
    d_up = jnp.einsum('bsd,bsf->df', norm_mid, d_up_b, preferred_element_type=f32)
    d_norm_mid = jnp.einsum('bsf,df->bsd', d_up_b, up_w, preferred_element_type=f32)
    d_resid_ln, d_gain2, d_bias2 = ln2_pull(d_norm_mid)
    d_resid = grad32 + d_resid_ln
    d_resid_b = d_resid.astype(bf16)
    d_outw = jnp.einsum('bsd,bse->de', attn_out, d_resid_b, preferred_element_type=f32)
    d_attn = jnp.einsum('bse,de->bsd', d_resid_b, out_w, preferred_element_type=f32).reshape(n_seq, seq_len, n_heads, head_dim)
    d_attn_b = d_attn.astype(bf16)
    delta = jnp.swapaxes(jnp.sum(d_attn * attn32, axis=-1), 1, 2)
    d_weights = jnp.einsum('bqhd,bkhd->bhqk', d_attn_b, v_val, preferred_element_type=f32)
    d_scores = (weights * (d_weights - delta[..., None])).astype(bf16)
    d_query = jnp.einsum('bhqk,bkhd->bqhd', d_scores, k_rot, preferred_element_type=f32)
    d_key = jnp.einsum('bhqk,bqhd->bkhd', d_scores, q_rot, preferred_element_type=f32)
    d_value = jnp.einsum('bhqk,bqhd->bkhd', weights_b, d_attn_b, preferred_element_type=f32)
    d_q_lin = rotate(d_query, cos_t, -sin_t) * head_dim ** -0.5
    d_k_lin = rotate(d_key, cos_t, -sin_t)
    d_qkv_lin = jnp.stack([d_q_lin, d_k_lin, d_value], axis=2)
    d_qkv_b = d_qkv_lin.astype(bf16)
    d_qkvw = jnp.einsum('bsd,bsthe->dthe', norm_in, d_qkv_b, preferred_element_type=f32)
    d_norm_in = jnp.einsum('bsthe,dthe->bsd', d_qkv_b, qkv_w, preferred_element_type=f32)
    d_embedded, d_gain1, d_bias1 = ln1_pull(d_norm_in)
    d_embedded = d_embedded + d_resid
    d_table = jnp.einsum('bsv,bsd->vd', one_hot, (d_embedded * keep_scale).astype(bf16), preferred_element_type=f32)
    d_bqkv = jnp.sum(d_qkv_lin, axis=(0, 1)).reshape(3, model_dim)
    d_tail = jnp.stack([jnp.sum(d_resid, axis=(0, 1)), d_gain2, d_bias2, jnp.sum(grad32, axis=(0, 1))])
    d_vecs = jnp.concatenate([jnp.stack([d_gain1, d_bias1]), d_bqkv, d_tail], axis=0)
    g_all = jnp.concatenate([
        d_qkvw.reshape(model_dim, 15, 128).transpose(1, 0, 2),
        d_outw.reshape(model_dim, 5, 128).transpose(1, 0, 2),
        d_up.reshape(model_dim, 20, 128).transpose(1, 0, 2),
        d_down.reshape(4, model_dim, 5, 128).transpose(0, 2, 1, 3).reshape(20, model_dim, 128),
    ], axis=0)
    return layer_out, d_table, d_vecs, g_all, jnp.sum(d_up_lin, axis=(0, 1))


def solution(mesh):
    chips = mesh.shape['fsdp']

    def local_step(tokens, lengths, embed_table, layer_vecs, w_qkv, w_out, w_up, b_up, w_down, grad_out):
        f32 = jnp.float32
        cp = lax.axis_index('cp')
        chip = lax.axis_index('fsdp')
        n_seq, seq_loc = tokens.shape
        half = n_seq // 2
        rows = w_qkv.shape[0]
        vocab, width = embed_table.shape
        w_loc = jnp.concatenate([
            w_qkv.reshape(rows, 15, 128).transpose(1, 0, 2),
            w_out.reshape(rows, 5, 128).transpose(1, 0, 2),
            w_up.reshape(rows, chips, 4, NB).transpose(2, 1, 3, 0).reshape(20, 128, rows).transpose(0, 2, 1),
            w_down.reshape(4, NB, 5, 128).transpose(0, 2, 1, 3).reshape(20, NB, 128),
        ], axis=0)
        s_loc = jnp.pad(jnp.concatenate([layer_vecs.reshape(-1), b_up]), (0, 1024 - 130)).reshape(8, 128)
        w_all, s_all, g_oth, t_oth = gather_all(w_loc, s_loc, grad_out, tokens)
        s_flat = s_all.reshape(chips, 1024)
        vecs_all = s_flat[:, :90].reshape(chips, 9, NB).transpose(1, 0, 2).reshape(9, width)
        up_b = s_flat[:, 90:130].reshape(chips, 4, NB).transpose(1, 0, 2).reshape(-1)
        start = half * cp
        tok_full = jnp.concatenate([lax.dynamic_slice_in_dim(tokens, start, half, 0), t_oth], axis=1)
        grad_full = jnp.concatenate([lax.dynamic_slice_in_dim(grad_out, start, half, 0), g_oth], axis=1)
        len_own = lax.dynamic_slice_in_dim(lengths, start, half, 0)
        positions = jnp.concatenate([cp * seq_loc + jnp.arange(seq_loc), (1 - cp) * seq_loc + jnp.arange(seq_loc)])
        layer_out, d_table, d_vecs, g_all, d_bup = layer_compute(tok_full, len_own, positions, embed_table, vecs_all, w_all, up_b, grad_full)
        small = jnp.concatenate([d_table.reshape(-1), d_vecs.reshape(-1), d_bup])
        small = jnp.pad(small, (0, 2 * SMALL_ROWS * 128 - small.shape[0])).reshape(2, SMALL_ROWS, 128)
        y_own, y_oth = layer_out[:, :seq_loc], layer_out[:, seq_loc:]
        g_red, s_red, y_recv = reduce_all(g_all.reshape(60, SIDE, SIDE, SIDE, NB, 128), small, y_oth)
        out_full = jnp.where(cp == 0, jnp.concatenate([y_own, y_recv], axis=0), jnp.concatenate([y_recv, y_own], axis=0))
        s_flat = s_red.reshape(-1)
        n_tab = vocab * width
        d_embed = s_flat[:n_tab].reshape(vocab, width)
        d_v = lax.dynamic_slice(s_flat[n_tab:n_tab + 9 * width].reshape(9, width), (0, chip * NB), (9, NB))
        d_b = s_flat[n_tab + 9 * width:n_tab + 9 * width + 2560].reshape(4, chips, NB)
        d_b = lax.dynamic_slice(d_b, (0, chip, 0), (4, 1, NB)).reshape(-1)
        d_qkv = g_red[:15].transpose(1, 0, 2).reshape(w_qkv.shape)
        d_wout = g_red[15:20].transpose(1, 0, 2).reshape(w_out.shape)
        d_wup = g_red[20:40].transpose(0, 2, 1).reshape(4, chips, NB, rows).transpose(3, 1, 0, 2).reshape(w_up.shape)
        d_wdown = g_red[40:60].reshape(4, 5, NB, 128).transpose(0, 2, 1, 3).reshape(w_down.shape)
        return out_full, d_embed, d_v, d_qkv, d_wout, d_wup, d_b, d_wdown

    in_specs = (P('fsdp', 'cp'), P('fsdp'), P(), P(None, 'fsdp'), P('fsdp', None, None, None), P('fsdp', None), P('fsdp', None), P('fsdp'), P('fsdp', None), P('fsdp', 'cp', None))
    out_specs = (P('fsdp', 'cp', None), P(), P(None, 'fsdp'), P('fsdp', None, None, None), P('fsdp', None), P('fsdp', None), P('fsdp'), P('fsdp', None))
    return jax.shard_map(local_step, mesh=mesh, in_specs=in_specs, out_specs=out_specs, check_vma=False)
```

```python
import functools

import jax
import jax.numpy as jnp
from jax import lax
from jax.experimental import pallas as pl
from jax.experimental.pallas import tpu as pltpu
from jax.sharding import PartitionSpec as P

MASK_ID = 32
LN_EPS = 1e-5
ROPE_BASE = 10000.0
TRAIN_RATIO = 0.15 * 0.8
NEG_BIG = -1e30
SIDE = 4
COLORS = 3
NB = 10
HALF = 5
SMALL_ROWS = 120
MESH_ID = pl.DeviceIdType.MESH
ANY = pl.BlockSpec(memory_space=pl.ANY)

GATHER_ORDER = ((2, 1, 0), (1, 0, 2), (0, 2, 1))
REDUCE_ORDER = ((0, 1, 2), (1, 2, 0), (2, 0, 1))


def my_coords():
    chip = lax.axis_index('fsdp')
    return [chip // 16, lax.rem(chip // 4, 4), lax.rem(chip, 4)]


def moved(coords, dim, by):
    out = list(coords)
    out[dim] = lax.rem(coords[dim] + by + SIDE, SIDE)
    return out


def chip_id(coords):
    return {'fsdp': coords[0] * 16 + coords[1] * 4 + coords[2]}


def entry_barrier(coords, cp):
    barrier = pltpu.get_barrier_semaphore()
    for dim in range(3):
        for by in (1, 2, 3):
            pl.semaphore_signal(barrier, inc=1, device_id=chip_id(moved(coords, dim, by)), device_id_type=MESH_ID)
    pl.semaphore_signal(barrier, inc=1, device_id={'cp': 1 - cp}, device_id_type=MESH_ID)
    pl.semaphore_wait(barrier, 10)


def push(src, dst, send_sem, recv_sem, target):
    return pltpu.make_async_remote_copy(src_ref=src, dst_ref=dst, send_sem=send_sem, recv_sem=recv_sem, device_id=target, device_id_type=MESH_ID)


def gather_kernel(w_loc, s_loc, g_own, t_own, w_all, s_all, g_oth, t_oth, ssem, rsem, fsend, frecv, s_ssem, s_rsem, psend, precv, lsem):
    cp = lax.axis_index('cp')
    me = my_coords()
    mate = {'cp': 1 - cp}
    own_w = pltpu.make_async_copy(w_loc, w_all.at[:, me[0], me[1], me[2]], lsem.at[0])
    own_s = pltpu.make_async_copy(s_loc, s_all.at[me[0], me[1], me[2]], lsem.at[1])
    own_w.start()
    own_s.start()
    entry_barrier(me, cp)
    swap_g = push(g_own.at[pl.ds(8 * (1 - cp), 8)], g_oth, psend.at[0], precv.at[0], mate)
    swap_t = push(t_own.at[pl.ds(8 * (1 - cp), 8)], t_oth, psend.at[1], precv.at[1], mate)
    swap_t.start()

    def region(ref, first, count, dims, at):
        index = [slice(None) if d in dims else at[d] for d in range(3)]
        return ref.at[(pl.ds(first, count), *index)]

    def small_region(dims, at):
        index = [slice(None) if d in dims else at[d] for d in range(3)]
        return s_all.at[tuple(index)]

    forwards = []
    pending = []
    own_s.wait()
    own_w.wait()
    for phase in range(3):
        firsts = {}
        for color in range(COLORS):
            dim = GATHER_ORDER[color][phase]
            done = GATHER_ORDER[color][:phase]
            base = cp * (COLORS * NB) + color * NB
            mine = region(w_all, base, NB, done, me)
            right, left = chip_id(moved(me, dim, 1)), chip_id(moved(me, dim, 3))
            to_right = push(mine, mine, ssem.at[color, phase, 0], rsem.at[color, phase, 0], right)
            to_left = push(mine, mine, ssem.at[color, phase, 1], rsem.at[color, phase, 1], left)
            to_right.start()
            to_left.start()
            firsts[color] = (to_right, to_left)
            pending += [to_right, to_left]
            if color == 0:
                s_mine = small_region(done, me)
                s_right = push(s_mine, s_mine, s_ssem.at[phase, 0], s_rsem.at[phase, 0], right)
                s_left = push(s_mine, s_mine, s_ssem.at[phase, 1], s_rsem.at[phase, 1], left)
                s_right.start()
                s_left.start()
                pending += [s_right, s_left]
        seconds = {}
        for color in range(COLORS):
            dim = GATHER_ORDER[color][phase]
            done = GATHER_ORDER[color][:phase]
            base = cp * (COLORS * NB) + color * NB
            right, left = chip_id(moved(me, dim, 1)), chip_id(moved(me, dim, 3))
            from_left, from_right = moved(me, dim, 3), moved(me, dim, 1)
            to_right, to_left = firsts[color]
            to_right.wait_recv()
            part = region(w_all, base, HALF, done, from_left)
            on_right = push(part, part, ssem.at[color, phase, 2], rsem.at[color, phase, 2], right)
            on_right.start()
            whole_l = region(w_all, base, NB, done, from_left)
            fwd_l = push(whole_l, whole_l, fsend.at[color, phase, 0], frecv.at[color, phase, 0], mate)
            fwd_l.start()
            to_left.wait_recv()
            part = region(w_all, base + HALF, HALF, done, from_right)
            on_left = push(part, part, ssem.at[color, phase, 3], rsem.at[color, phase, 3], left)
            on_left.start()
            whole_r = region(w_all, base, NB, done, from_right)
            fwd_r = push(whole_r, whole_r, fsend.at[color, phase, 1], frecv.at[color, phase, 1], mate)
            fwd_r.start()
            seconds[color] = (on_right, on_left)
            pending += [on_right, on_left]
            forwards += [fwd_l, fwd_r]
            if color == 0:
                s_right.wait_recv()
                s_left.wait_recv()
                s_part = small_region(done, from_left)
                s_on = push(s_part, s_part, s_ssem.at[phase, 2], s_rsem.at[phase, 2], right)
                s_on.start()
                pending.append(s_on)
        for color in range(COLORS):
            dim = GATHER_ORDER[color][phase]
            done = GATHER_ORDER[color][:phase]
            base = cp * (COLORS * NB) + color * NB
            on_right, on_left = seconds[color]
            on_right.wait_recv()
            on_left.wait_recv()
            far = region(w_all, base, NB, done, moved(me, dim, 2))
            fwd_f = push(far, far, fsend.at[color, phase, 2], frecv.at[color, phase, 2], mate)
            fwd_f.start()
            forwards.append(fwd_f)
            if color == 0:
                s_on.wait_recv()
        if phase == 0:
            swap_g.start()
    for copy in forwards:
        copy.wait_recv()
    swap_g.wait()
    swap_t.wait()
    for copy in pending + forwards:
        copy.wait_send()


def gather_all(w_loc, s_loc, grad_out, tokens):
    bf16, f32 = jnp.bfloat16, jnp.float32
    blocks = w_loc.shape[0]
    seqs, pos, width = grad_out.shape
    dma = pltpu.SemaphoreType.DMA
    return pl.pallas_call(
        gather_kernel,
        out_shape=(
            jax.ShapeDtypeStruct((blocks, SIDE, SIDE, SIDE, NB, 128), bf16),
            jax.ShapeDtypeStruct((SIDE, SIDE, SIDE, 8, 128), f32),
            jax.ShapeDtypeStruct((seqs // 2, pos, width), bf16),
            jax.ShapeDtypeStruct((seqs // 2, pos), jnp.int32),
        ),
        in_specs=[ANY] * 4,
        out_specs=(ANY,) * 4,
        scratch_shapes=[dma((3, 3, 4)), dma((3, 3, 4)), dma((3, 3, 3)), dma((3, 3, 3)), dma((3, 3)), dma((3, 3)), dma((2,)), dma((2,)), dma((2,))],
        compiler_params=pltpu.CompilerParams(collective_id=0, has_side_effects=True),
        name='gather_weights',
    )(w_loc, s_loc, grad_out, tokens)


def reduce_kernel(g_all, small, y_oth, g_out, s_out, y_recv, held, pair, ra0, rb0, ra1, rb1, ra2, rb2, s_pair, s_slots, s_acc,
                  lsem, psend, precv, ssem, rsem, s_ssem, s_rsem, osend, orecv, msem):
    cp = lax.axis_index('cp')
    me = my_coords()
    mate = {'cp': 1 - cp}
    per = COLORS * NB
    loads = []
    for color in range(COLORS):
        load = pltpu.make_async_copy(g_all.at[pl.ds(cp * per + color * NB, NB)], held.at[pl.ds(color * NB, NB)], lsem.at[color])
        load.start()
        loads.append(load)
    s_load = pltpu.make_async_copy(small, s_acc, lsem.at[3])
    s_load.start()
    entry_barrier(me, cp)
    sends = []
    s_swap = push(small, s_pair, psend.at[3], precv.at[3], mate)
    s_swap.start()
    swaps = []
    for color in range(COLORS):
        swap = push(g_all.at[pl.ds((1 - cp) * per + color * NB, NB)], pair.at[pl.ds(color * NB, NB)], psend.at[color], precv.at[color], mate)
        swap.start()
        swaps.append(swap)
    y_swap = push(y_oth, y_recv, psend.at[4], precv.at[4], mate)
    y_swap.start()

    bufs = ((ra0, rb0), (ra1, rb1), (ra2, rb2))

    def index_of(dims, at):
        return [slice(None) if d in dims else at[d] for d in range(3)]

    def region(first, count, dims, at):
        return held.at[(pl.ds(first, count), *index_of(dims, at))]

    def start_phase(color, phase):
        dim = REDUCE_ORDER[color][phase]
        rest = REDUCE_ORDER[color][phase + 1:]
        base = color * NB
        ra, rb = bufs[phase]
        right, left = moved(me, dim, 1), moved(me, dim, 3)
        far = moved(me, dim, 2)
        out = [
            push(region(base, HALF, rest, far), ra.at[color, 0], ssem.at[color, phase, 0], rsem.at[color, phase, 0], chip_id(right)),
            push(region(base + HALF, HALF, rest, far), ra.at[color, 1], ssem.at[color, phase, 1], rsem.at[color, phase, 1], chip_id(left)),
            push(region(base + HALF, HALF, rest, right), rb.at[color, 0, pl.ds(HALF, HALF)], ssem.at[color, phase, 2], rsem.at[color, phase, 2], chip_id(right)),
            push(region(base, HALF, rest, left), rb.at[color, 1, pl.ds(0, HALF)], ssem.at[color, phase, 3], rsem.at[color, phase, 3], chip_id(left)),
        ]
        for copy in out:
            copy.start()
        sends.extend(out)
        return out

    def middle(color, phase, copies):
        dim = REDUCE_ORDER[color][phase]
        rest = REDUCE_ORDER[color][phase + 1:]
        base = color * NB
        ra, rb = bufs[phase]
        right, left = moved(me, dim, 1), moved(me, dim, 3)
        copies[0].wait_recv()
        to_r = index_of(rest, right)

        @pl.loop(0, HALF)
        def _(b):
            held[(base + b, *to_r)] += ra[color, 0, b]

        fwd_r = push(region(base, HALF, rest, right), rb.at[color, 0, pl.ds(0, HALF)], ssem.at[color, phase, 4], rsem.at[color, phase, 4], chip_id(right))
        fwd_r.start()
        copies[1].wait_recv()
        to_l = index_of(rest, left)

        @pl.loop(0, HALF)
        def _(b):
            held[(base + HALF + b, *to_l)] += ra[color, 1, b]

        fwd_l = push(region(base + HALF, HALF, rest, left), rb.at[color, 1, pl.ds(HALF, HALF)], ssem.at[color, phase, 5], rsem.at[color, phase, 5], chip_id(left))
        fwd_l.start()
        sends.extend([fwd_r, fwd_l])
        return [fwd_r, fwd_l]

    def finish(color, phase, copies, late):
        rest = REDUCE_ORDER[color][phase + 1:]
        base = color * NB
        ra, rb = bufs[phase]
        copies[2].wait_recv()
        copies[3].wait_recv()
        late[0].wait_recv()
        late[1].wait_recv()
        here = index_of(rest, me)

        @pl.loop(0, NB)
        def _(b):
            held[(base + b, *here)] += rb[color, 0, b] + rb[color, 1, b]

    s_copies = []

    def small_start(phase):
        dim = REDUCE_ORDER[0][phase]
        out = []
        for by in (1, 2, 3):
            out.append(push(s_acc.at[cp], s_slots.at[phase, by - 1], s_ssem.at[phase, by - 1], s_rsem.at[phase, by - 1], chip_id(moved(me, dim, by))))
        for copy in out:
            copy.start()
        return out

    def small_finish(phase, copies):
        dim = REDUCE_ORDER[0][phase]
        for copy in copies:
            copy.wait()
        mine = me[dim]
        total = None
        own = s_acc[cp]
        got = [own] + [s_slots[phase, by] for by in range(3)]
        for coord in range(SIDE):
            gap = lax.rem(mine - coord + SIDE, SIDE)
            value = jnp.where(gap == 0, got[0], jnp.where(gap == 1, got[1], jnp.where(gap == 2, got[2], got[3])))
            total = value if total is None else total + value
        s_acc[cp] = total

    s_load.wait()
    s_swap.wait()
    s_acc[...] = s_acc[...] + s_pair[...]
    s_out_copies = small_start(0)
    started = []
    for color in range(COLORS):
        loads[color].wait()
        swaps[color].wait_recv()

        @pl.loop(0, NB)
        def _(b):
            for z in range(SIDE):
                held[color * NB + b, z] += pair[color * NB + b, z]

        started.append(start_phase(color, 0))
    for phase in range(3):
        late = [middle(color, phase, started[color]) for color in range(COLORS)]
        nxt = []
        for color in range(COLORS):
            finish(color, phase, started[color], late[color])
            if phase < 2:
                nxt.append(start_phase(color, phase + 1))
        small_finish(phase, s_out_copies)
        if phase < 2:
            s_out_copies = small_start(phase + 1)
        started = nxt
    mine = held.at[:, me[0], me[1], me[2]]
    out_far = push(mine, g_out.at[pl.ds(cp * per, per)], osend.at[0], orecv.at[0], mate)
    out_far.start()
    s_far = push(s_acc.at[cp], s_out.at[cp], osend.at[1], orecv.at[1], mate)
    s_far.start()
    out_own = pltpu.make_async_copy(mine, g_out.at[pl.ds(cp * per, per)], msem.at[0])
    out_own.start()
    s_own = pltpu.make_async_copy(s_acc.at[cp], s_out.at[cp], msem.at[1])
    s_own.start()
    for copy in sends:
        copy.wait_send()
    for copy in swaps:
        copy.wait_send()
    y_swap.wait()
    out_own.wait()
    s_own.wait()
    out_far.wait()
    s_far.wait()


def reduce_all(g_all, small, y_oth):
    f32 = jnp.float32
    blocks = g_all.shape[0]
    dma = pltpu.SemaphoreType.DMA
    vm = pltpu.VMEM
    return pl.pallas_call(
        reduce_kernel,
        out_shape=(
            jax.ShapeDtypeStruct((blocks, NB, 128), f32),
            jax.ShapeDtypeStruct(small.shape, f32),
            jax.ShapeDtypeStruct(y_oth.shape, y_oth.dtype),
        ),
        in_specs=[ANY] * 3,
        out_specs=(ANY,) * 3,
        scratch_shapes=[
            vm((blocks // 2, SIDE, SIDE, SIDE, NB, 128), f32),
            vm((blocks // 2, SIDE, SIDE, SIDE, NB, 128), f32),
            vm((COLORS, 2, HALF, SIDE, SIDE, NB, 128), f32),
            vm((COLORS, 2, NB, SIDE, SIDE, NB, 128), f32),
            vm((COLORS, 2, HALF, SIDE, NB, 128), f32),
            vm((COLORS, 2, NB, SIDE, NB, 128), f32),
            vm((COLORS, 2, HALF, NB, 128), f32),
            vm((COLORS, 2, NB, NB, 128), f32),
            vm(small.shape, f32),
            vm((3, 3) + small.shape[1:], f32),
            vm(small.shape, f32),
            dma((4,)), dma((5,)), dma((5,)), dma((3, 3, 6)), dma((3, 3, 6)), dma((3, 3)), dma((3, 3)), dma((2,)), dma((2,)), dma((2,)),
        ],
        compiler_params=pltpu.CompilerParams(collective_id=1, has_side_effects=True, vmem_limit_bytes=62 * 1024 * 1024),
        name='reduce_grads',
    )(g_all, small, y_oth)


SEQS = 8
STEP_SEQS = 2
STEPS = SEQS // STEP_SEQS
SEQ = 256
TOK = STEP_SEQS * SEQ
TILES = 5
HEADS_PER = 4
HEAD = 32
LANES = 128
F32 = jnp.float32
BF16 = jnp.bfloat16


def mm(lhs, rhs):
    return lax.dot_general(lhs, rhs, (((1,), (0,)), ((), ())), preferred_element_type=F32)


def mm_t(lhs, rhs):
    return lax.dot_general(lhs, rhs, (((1,), (1,)), ((), ())), preferred_element_type=F32)


def fold8(value):
    return jnp.sum(value.reshape(value.shape[0] // 8, 8, value.shape[1]), axis=0)


def wide(ref, first, count):
    return jnp.concatenate([ref[first + j] for j in range(count)], axis=1)


def add_blocks(ref, first, value):
    for j in range(value.shape[1] // LANES):
        ref[first + j] += value[:, j * LANES:(j + 1) * LANES]


def norm_stats(value):
    mean = jnp.mean(value, axis=-1, keepdims=True)
    cent = value - mean
    var = jnp.mean(cent * cent, axis=-1, keepdims=True)
    rstd = lax.rsqrt(var + LN_EPS)
    return cent * rstd, rstd


def norm_back(d_out, gain, xhat, rstd):
    d_hat = d_out * gain
    m1 = jnp.mean(d_hat, axis=-1, keepdims=True)
    m2 = jnp.mean(d_hat * xhat, axis=-1, keepdims=True)
    return rstd * (d_hat - m1 - xhat * m2)


def gelu_pair(u):
    z = u * (0.5 ** 0.5)
    t = 1.0 / (1.0 + 0.3275911 * jnp.abs(z))
    poly = t * (0.127414796 + t * (-0.142248368 + t * (0.710706871 + t * (-0.7265760135 + t * 0.5307027145))))
    ex = jnp.exp(-z * z)
    tail = poly * ex
    cdf = jnp.where(u >= 0, 1.0 - tail, tail)
    return u * cdf, cdf + u * (ex * 0.3989422804014327)


def unturn(z, cos, sin, groups):
    parts = z.reshape(groups, 2, HEAD // 2, z.shape[1])
    lo, up = parts[:, 0], parts[:, 1]
    out = jnp.stack([lo * cos + up * sin, up * cos - lo * sin], axis=1)
    return out.reshape(z.shape)


def turn(z, cos, sin, groups):
    return unturn(z, cos, -sin, groups)


def layer_kernel(tok_ref, keep_ref, mask_ref, emb_ref, vec_ref, bqkv_ref, bup_ref, cos_ref, sin_ref, cosn_ref, sinn_ref,
                 w_hbm, g_own, g_oth,
                 y_own, y_oth, grads, dtab, dsum, dbq, dbkv, dbup,
                 w, wt, acc, gbuf, e_s, ht, qt, kt, vt, qn, kn, vn, pt, ot32, otb, x1, nm, nmt, y_s, dnm, dot_s, dqkv,
                 wsem, gsem, osem):
    step = pl.program_id(0)
    cp = lax.axis_index('cp')
    chips = SIDE ** 3

    @pl.when(step == 0)
    def _():
        own = pltpu.make_async_copy(g_own.at[pl.ds(cp * SEQS, SEQS)], gbuf.at[:, 0], gsem.at[0])
        oth = pltpu.make_async_copy(g_oth, gbuf.at[:, 1], gsem.at[1])

        @pl.loop(0, chips)
        def _(i):
            pltpu.make_async_copy(w_hbm.at[:, i], w.at[:, pl.ds(i * NB, NB), :], wsem).start()

        own.start()
        oth.start()

        @pl.loop(0, 60)
        def _(i):
            acc[i] = jnp.zeros((640, LANES), F32)

        dtab[...] = jnp.zeros_like(dtab)
        dsum[...] = jnp.zeros_like(dsum)
        dbq[...] = jnp.zeros_like(dbq)
        dbkv[...] = jnp.zeros_like(dbkv)
        dbup[...] = jnp.zeros_like(dbup)

        @pl.loop(0, chips)
        def _(i):
            pltpu.make_async_copy(w_hbm.at[:, i], w.at[:, pl.ds(i * NB, NB), :], wsem).wait()

        own.wait()
        oth.wait()

        @pl.loop(0, 15)
        def _(n):
            wt[n] = w[n].T

    def grad_rows():
        return gbuf[pl.ds(step * STEP_SEQS, STEP_SEQS)].reshape(TOK, 640)

    vocab = lax.broadcasted_iota(jnp.int32, (64, TOK), 0)
    one_hot = jnp.where(vocab == tok_ref[0], 1.0, 0.0).astype(BF16)
    e_s[...] = lax.dot_general(one_hot, emb_ref[...], (((0,), (0,)), ((), ())), preferred_element_type=F32)

    @pl.loop(0, TOK // 128)
    def _(r):
        rows = pl.ds(pl.multiple_of(r * 128, 128), 128)
        keep = jnp.concatenate([keep_ref[rows]] * TILES, axis=1)
        emb = e_s[rows] * keep
        e_s[rows] = emb
        xhat, _ = norm_stats(emb)
        nm[rows] = (xhat * vec_ref[0:1] + vec_ref[1:2]).astype(BF16)

    ht[...] = nm[...].T

    cos, sin = cos_ref[...], sin_ref[...]
    for kind, (t_ref, n_ref) in enumerate(((qt, qn), (kt, kn), (vt, vn))):
        z = mm(wt[kind * TILES:(kind + 1) * TILES].reshape(640, 640), ht[...])
        bias = bqkv_ref[kind * 640:(kind + 1) * 640]
        z = z + jnp.concatenate([bias] * (TOK // LANES), axis=1)
        if kind == 0:
            z = z * HEAD ** -0.5
        if kind < 2:
            z = turn(z, cos, sin, 20)
        zb = z.astype(BF16)
        for s in range(STEP_SEQS):
            for t in range(TILES):
                piece = zb[t * LANES:(t + 1) * LANES, s * SEQ:(s + 1) * SEQ]
                t_ref[s, t] = piece
                n_ref[s, t] = piece.T

    lane_head = lax.broadcasted_iota(jnp.int32, (1, LANES), 1) // HEAD
    pick = [jnp.where(lane_head == h, 1.0, 0.0).astype(BF16) for h in range(HEADS_PER)]

    @pl.loop(0, STEP_SEQS)
    def _(s):
        rows = pl.ds(pl.multiple_of(s * SEQ, SEQ), SEQ)

        @pl.loop(0, TILES)
        def _(t):
            bias = mask_ref[rows]
            bias = jnp.concatenate([bias, bias], axis=1)
            q_t, k_n, v_t = qt[s, t], kn[s, t], vt[s, t]
            outs = []
            for h in range(HEADS_PER):
                score = mm(k_n * pick[h], q_t) + bias
                top = jnp.max(score, axis=0, keepdims=True)
                p = jnp.exp(score - top)
                p = p * (1.0 / jnp.sum(p, axis=0, keepdims=True))
                pb = p.astype(BF16)
                pt[s, t * HEADS_PER + h] = pb
                outs.append(mm(v_t[h * HEAD:(h + 1) * HEAD], pb))
            out = jnp.concatenate(outs, axis=0)
            ot32[s, t] = out
            outb = out.astype(BF16)
            otb[t, :, rows] = outb
            dqkv[t, rows] = outb.T

    w_out = wide(w, 15, TILES)
    x1[...] = e_s[...] + mm(wide(dqkv, 0, TILES), w_out) + vec_ref[5:6]

    @pl.loop(0, TOK // 128)
    def _(r):
        rows = pl.ds(pl.multiple_of(r * 128, 128), 128)
        xhat, _ = norm_stats(x1[rows])
        nm[rows] = (xhat * vec_ref[6:7] + vec_ref[7:8]).astype(BF16)

    nmt[...] = nm[...].T
    y_s[...] = jnp.zeros_like(y_s)
    dnm[...] = jnp.zeros_like(dnm)

    @pl.loop(0, 4)
    def _(c):
        g = grad_rows()
        w_up = wide(w, 20 + TILES * c, TILES)
        u = mm(nm[...], w_up) + bup_ref[c]
        a, slope = gelu_pair(u)
        ab = a.astype(BF16)
        w_down = wide(w, 40 + TILES * c, TILES)
        du = mm_t(g, w_down) * slope
        dbup[c] += fold8(du)
        dub = du.astype(BF16)
        y_s[...] += mm(ab, w_down)
        dnm[...] += mm_t(dub, w_up)
        add_blocks(acc, 40 + TILES * c, mm(ab.T, g))
        add_blocks(acc, 20 + TILES * c, mm(nmt[...], dub))

    @pl.loop(0, TOK // 128)
    def _(r):
        rows = pl.ds(pl.multiple_of(r * 128, 128), 128)
        x = x1[rows]
        out = (x + y_s[rows] + vec_ref[8:9]).astype(BF16)
        seq = r // 2

        @pl.when(lax.rem(r, 2) == 0)
        def _():
            y_own[seq] = out

        @pl.when(lax.rem(r, 2) == 1)
        def _():
            y_oth[seq] = out

        xhat, rstd = norm_stats(x)
        d_n = dnm[rows]
        g32 = gbuf[step * STEP_SEQS + seq, lax.rem(r, 2)].astype(F32)
        dsum[3] += fold8(d_n * xhat)
        dsum[4] += fold8(d_n)
        d_r = g32 + norm_back(d_n, vec_ref[6:7], xhat, rstd)
        dsum[2] += fold8(d_r)
        dsum[5] += fold8(g32)
        y_s[rows] = d_r
        nm[rows] = d_r.astype(BF16)

    d_rb = nm[...]
    add_blocks(acc, 15, mm(otb[...].reshape(640, TOK), d_rb))
    d_o = mm(wide(w, 15, TILES), d_rb.T)
    for t in range(TILES):
        dot_s[t] = d_o[t * LANES:(t + 1) * LANES]

    @pl.loop(0, STEP_SEQS)
    def _(s):
        rows = pl.ds(pl.multiple_of(s * SEQ, SEQ), SEQ)

        @pl.loop(0, TILES)
        def _(t):
            d_ot = dot_s[t, :, rows]
            d_otb = d_ot.astype(BF16)
            d_on = d_otb.T
            prod = d_ot * ot32[s, t]
            k_t, v_n, q_n = kt[s, t], vn[s, t], qn[s, t]
            dqs = []
            dk, dv = None, None
            for h in range(HEADS_PER):
                lanes = slice(h * HEAD, (h + 1) * HEAD)
                pb = pt[s, t * HEADS_PER + h]
                delta = jnp.sum(prod[lanes], axis=0, keepdims=True)
                d_p = mm(v_n * pick[h], d_otb)
                d_sb = (pb.astype(F32) * (d_p - delta)).astype(BF16)
                dqs.append(mm(k_t[lanes], d_sb))
                dk_h = mm(d_sb, q_n * pick[h])
                dv_h = mm(pb, d_on * pick[h])
                dk = dk_h if dk is None else dk + dk_h
                dv = dv_h if dv is None else dv + dv_h
            dq = unturn(jnp.concatenate(dqs, axis=0), cos[:, :SEQ], sin[:, :SEQ], HEADS_PER) * HEAD ** -0.5
            dbq[t] += dq[:, :LANES] + dq[:, LANES:]
            dqkv[t, rows] = dq.astype(BF16).T
            low = lax.rem(lax.broadcasted_iota(jnp.int32, (SEQ, LANES), 1), HEAD) < HEAD // 2
            other = jnp.where(low, pltpu.roll(dk, LANES - HEAD // 2, 1), pltpu.roll(dk, HEAD // 2, 1))
            dk = dk * cosn_ref[...] + other * sinn_ref[...]
            dbkv[0, t] += fold8(dk)
            dbkv[1, t] += fold8(dv)
            dqkv[TILES + t, rows] = dk.astype(BF16)
            dqkv[2 * TILES + t, rows] = dv.astype(BF16)

    for kind in range(3):
        add_blocks(acc, kind * TILES, mm(ht[...], wide(dqkv, kind * TILES, TILES)))
    dnm[...] = mm(wide(dqkv, 0, 15), wt[...].reshape(1920, 640))

    @pl.loop(0, TOK // 128)
    def _(r):
        rows = pl.ds(pl.multiple_of(r * 128, 128), 128)
        xhat, rstd = norm_stats(e_s[rows])
        d_n = dnm[rows]
        dsum[0] += fold8(d_n * xhat)
        dsum[1] += fold8(d_n)
        keep = jnp.concatenate([keep_ref[rows]] * TILES, axis=1)
        nm[rows] = ((norm_back(d_n, vec_ref[0:1], xhat, rstd) + y_s[rows]) * keep).astype(BF16)

    dtab[...] += mm(one_hot, nm[...])

    @pl.when(step == STEPS - 1)
    def _():
        @pl.loop(0, chips)
        def _(i):
            pltpu.make_async_copy(acc.at[:, pl.ds(i * NB, NB), :], grads.at[:, i], osem).start()

        @pl.loop(0, chips)
        def _(i):
            pltpu.make_async_copy(acc.at[:, pl.ds(i * NB, NB), :], grads.at[:, i], osem).wait()


def layer_call(tok, keep, mask, emb, vecs, bqkv, bup, cos, sin, cosn, sinn, w_hbm, g_own, g_oth):
    vm = pltpu.VMEM
    dma = pltpu.SemaphoreType.DMA

    def whole(shape):
        return pl.BlockSpec(shape, lambda i: (0,) * len(shape))

    pair = pl.BlockSpec((STEP_SEQS, 128, 640), lambda i: (i, 0, 0))
    out_shape = (
        jax.ShapeDtypeStruct((SEQS, 128, 640), BF16),
        jax.ShapeDtypeStruct((SEQS, 128, 640), BF16),
        jax.ShapeDtypeStruct((60, 64, NB, LANES), F32),
        jax.ShapeDtypeStruct((64, 640), F32),
        jax.ShapeDtypeStruct((6, 8, 640), F32),
        jax.ShapeDtypeStruct((TILES, LANES, LANES), F32),
        jax.ShapeDtypeStruct((2, TILES, 8, LANES), F32),
        jax.ShapeDtypeStruct((4, 8, 640), F32),
    )
    out_specs = (pair, pair, ANY) + tuple(whole(o.shape) for o in out_shape[3:])
    in_specs = [
        pl.BlockSpec((1, 1, TOK), lambda i: (i, 0, 0)),
        pl.BlockSpec((TOK, LANES), lambda i: (i, 0)),
        pl.BlockSpec((TOK, LANES), lambda i: (i, 0)),
    ] + [whole(a.shape) for a in (emb, vecs, bqkv, bup, cos, sin, cosn, sinn)] + [ANY] * 3
    halves = (STEP_SEQS, TILES, LANES, SEQ)
    flipped = (STEP_SEQS, TILES, SEQ, LANES)
    scratch = [
        vm((60, 640, LANES), BF16), vm((15, LANES, 640), BF16), vm((60, 640, LANES), F32), vm((SEQS, 2, 128, 640), BF16),
        vm((TOK, 640), F32), vm((640, TOK), BF16),
        vm(halves, BF16), vm(halves, BF16), vm(halves, BF16), vm(flipped, BF16), vm(flipped, BF16), vm(flipped, BF16),
        vm((STEP_SEQS, 20, SEQ, SEQ), BF16), vm(halves, F32), vm((TILES, LANES, TOK), BF16),
        vm((TOK, 640), F32), vm((TOK, 640), BF16), vm((640, TOK), BF16), vm((TOK, 640), F32), vm((TOK, 640), F32),
        vm((TILES, LANES, TOK), F32), vm((15, TOK, LANES), BF16),
        dma, dma((2,)), dma,
    ]
    return pl.pallas_call(
        layer_kernel,
        grid=(STEPS,),
        out_shape=out_shape,
        in_specs=in_specs,
        out_specs=out_specs,
        scratch_shapes=scratch,
        compiler_params=pltpu.CompilerParams(dimension_semantics=('arbitrary',), vmem_limit_bytes=67043328),
        name='layer',
    )(tok, keep, mask, emb, vecs, bqkv, bup, cos, sin, cosn, sinn, w_hbm, g_own, g_oth)


def prepare(tokens, lengths, positions, embed_table, vecs_all):
    n_seq, seq_len = tokens.shape
    is_mask = tokens == MASK_ID
    tok_valid = positions[None, :] < lengths[:, None]
    mask_count = jnp.sum(is_mask.astype(jnp.int32), axis=1)
    drop_scale = (1.0 - TRAIN_RATIO) / (1.0 - mask_count.astype(F32) / lengths.astype(F32))
    keep = jnp.where(is_mask | jnp.logical_not(tok_valid), 0.0, drop_scale[:, None])
    keep = jnp.broadcast_to(keep.reshape(-1, 1), (n_seq * seq_len, LANES))
    mask = jnp.broadcast_to(jnp.where(tok_valid, 0.0, NEG_BIG).reshape(-1, 1), (n_seq * seq_len, LANES)).astype(F32)
    emb = jnp.pad(embed_table, ((0, 64 - embed_table.shape[0]), (0, 0)))
    bqkv = jnp.broadcast_to(vecs_all[2:5].reshape(-1, 1), (1920, LANES))
    inv_freq = 1.0 / (ROPE_BASE ** (jnp.arange(0, HEAD, 2, dtype=F32) / HEAD))
    angles = positions.astype(F32)[:, None] * inv_freq[None, :]
    cos, sin = jnp.cos(angles), jnp.sin(angles)
    cos_t, sin_t = jnp.tile(cos.T, (1, STEP_SEQS)), jnp.tile(sin.T, (1, STEP_SEQS))
    cos_n = jnp.tile(cos, (1, 8))
    sin_n = jnp.tile(jnp.concatenate([sin, -sin], axis=1), (1, 4))
    return tokens.reshape(STEPS, 1, TOK), keep, mask, emb, bqkv, cos_t, sin_t, cos_n, sin_n


def solution(mesh):
    chips = mesh.shape['fsdp']

    def local_step(tokens, lengths, embed_table, layer_vecs, w_qkv, w_out, w_up, b_up, w_down, grad_out):
        f32 = jnp.float32
        cp = lax.axis_index('cp')
        chip = lax.axis_index('fsdp')
        n_seq, seq_loc = tokens.shape
        half = n_seq // 2
        rows = w_qkv.shape[0]
        vocab, width = embed_table.shape
        w_loc = jnp.concatenate([
            w_qkv.reshape(rows, 15, 128).transpose(1, 0, 2),
            w_out.reshape(rows, 5, 128).transpose(1, 0, 2),
            w_up.reshape(rows, chips, 4, NB).transpose(2, 1, 3, 0).reshape(20, 128, rows).transpose(0, 2, 1),
            w_down.reshape(4, NB, 5, 128).transpose(0, 2, 1, 3).reshape(20, NB, 128),
        ], axis=0)
        s_loc = jnp.pad(jnp.concatenate([layer_vecs.reshape(-1), b_up]), (0, 1024 - 130)).reshape(8, 128)
        w_all, s_all, g_oth, t_oth = gather_all(w_loc, s_loc, grad_out, tokens)
        s_flat = s_all.reshape(chips, 1024)
        vecs_all = s_flat[:, :90].reshape(chips, 9, NB).transpose(1, 0, 2).reshape(9, width)
        up_b = s_flat[:, 90:130].reshape(chips, 4, NB).transpose(1, 0, 2).reshape(-1)
        start = half * cp
        tok_full = jnp.concatenate([lax.dynamic_slice_in_dim(tokens, start, half, 0), t_oth], axis=1)
        len_own = lax.dynamic_slice_in_dim(lengths, start, half, 0)
        positions = jnp.concatenate([cp * seq_loc + jnp.arange(seq_loc), (1 - cp) * seq_loc + jnp.arange(seq_loc)])
        tok, keep, mask, emb, bqkv, cos, sin, cosn, sinn = prepare(tok_full, len_own, positions, embed_table, vecs_all)
        y_own, y_oth, g_all, dtab, dsum, dbq, dbkv, dbup = layer_call(
            tok, keep, mask, emb, vecs_all, bqkv, up_b.reshape(4, 1, 640), cos, sin, cosn, sinn, w_all.reshape(60, chips, NB, 128), grad_out, g_oth)
        rowsum = jnp.sum(dsum, axis=1)
        d_bq = jnp.sum(dbq, axis=2).reshape(1, width)
        d_bkv = jnp.sum(dbkv, axis=2).reshape(2, width)
        small = jnp.concatenate([dtab[:vocab].reshape(-1), rowsum[:2].reshape(-1), d_bq.reshape(-1), d_bkv.reshape(-1), rowsum[2:].reshape(-1), jnp.sum(dbup, axis=1).reshape(-1)])
        small = jnp.pad(small, (0, 2 * SMALL_ROWS * 128 - small.shape[0])).reshape(2, SMALL_ROWS, 128)
        g_red, s_red, y_recv = reduce_all(g_all.reshape(60, SIDE, SIDE, SIDE, NB, 128), small, y_oth)
        out_full = jnp.where(cp == 0, jnp.concatenate([y_own, y_recv], axis=0), jnp.concatenate([y_recv, y_own], axis=0))
        s_flat = s_red.reshape(-1)
        n_tab = vocab * width
        d_embed = s_flat[:n_tab].reshape(vocab, width)
        d_v = lax.dynamic_slice(s_flat[n_tab:n_tab + 9 * width].reshape(9, width), (0, chip * NB), (9, NB))
        d_b = s_flat[n_tab + 9 * width:n_tab + 9 * width + 2560].reshape(4, chips, NB)
        d_b = lax.dynamic_slice(d_b, (0, chip, 0), (4, 1, NB)).reshape(-1)
        d_qkv = g_red[:15].transpose(1, 0, 2).reshape(w_qkv.shape)
        d_wout = g_red[15:20].transpose(1, 0, 2).reshape(w_out.shape)
        d_wup = g_red[20:40].transpose(0, 2, 1).reshape(4, chips, NB, rows).transpose(3, 1, 0, 2).reshape(w_up.shape)
        d_wdown = g_red[40:60].reshape(4, 5, NB, 128).transpose(0, 2, 1, 3).reshape(w_down.shape)
        return out_full, d_embed, d_v, d_qkv, d_wout, d_wup, d_b, d_wdown

    in_specs = (P('fsdp', 'cp'), P('fsdp'), P(), P(None, 'fsdp'), P('fsdp', None, None, None), P('fsdp', None), P('fsdp', None), P('fsdp'), P('fsdp', None), P('fsdp', 'cp', None))
    out_specs = (P('fsdp', 'cp', None), P(), P(None, 'fsdp'), P('fsdp', None, None, None), P('fsdp', None), P('fsdp', None), P('fsdp'), P('fsdp', None))
    return jax.shard_map(local_step, mesh=mesh, in_specs=in_specs, out_specs=out_specs, check_vma=False)
```

```python
import functools

import jax
import jax.numpy as jnp
from jax import lax
from jax.experimental import pallas as pl
from jax.experimental.pallas import tpu as pltpu
from jax.sharding import PartitionSpec as P

MASK_ID = 32
LN_EPS = 1e-5
ROPE_BASE = 10000.0
TRAIN_RATIO = 0.15 * 0.8
NEG_BIG = -1e30
SIDE = 4
COLORS = 3
NB = 10
HALF = 5
SMALL_ROWS = 120
MESH_ID = pl.DeviceIdType.MESH
ANY = pl.BlockSpec(memory_space=pl.ANY)

GATHER_ORDER = ((2, 1, 0), (1, 0, 2), (0, 2, 1))
REDUCE_ORDER = ((0, 1, 2), (1, 2, 0), (2, 0, 1))


def my_coords():
    chip = lax.axis_index('fsdp')
    return [chip // 16, lax.rem(chip // 4, 4), lax.rem(chip, 4)]


def moved(coords, dim, by):
    out = list(coords)
    out[dim] = lax.rem(coords[dim] + by + SIDE, SIDE)
    return out


def chip_id(coords):
    return {'fsdp': coords[0] * 16 + coords[1] * 4 + coords[2]}


def entry_barrier(coords, cp):
    barrier = pltpu.get_barrier_semaphore()
    for dim in range(3):
        for by in (1, 2, 3):
            pl.semaphore_signal(barrier, inc=1, device_id=chip_id(moved(coords, dim, by)), device_id_type=MESH_ID)
    pl.semaphore_signal(barrier, inc=1, device_id={'cp': 1 - cp}, device_id_type=MESH_ID)
    pl.semaphore_wait(barrier, 10)


def push(src, dst, send_sem, recv_sem, target):
    return pltpu.make_async_remote_copy(src_ref=src, dst_ref=dst, send_sem=send_sem, recv_sem=recv_sem, device_id=target, device_id_type=MESH_ID)


def gather_kernel(w_loc, s_loc, g_own, t_own, w_all, s_all, g_oth, t_oth, ssem, rsem, fsend, frecv, s_ssem, s_rsem, psend, precv, lsem):
    cp = lax.axis_index('cp')
    me = my_coords()
    mate = {'cp': 1 - cp}
    own_w = pltpu.make_async_copy(w_loc, w_all.at[:, me[0], me[1], me[2]], lsem.at[0])
    own_s = pltpu.make_async_copy(s_loc, s_all.at[me[0], me[1], me[2]], lsem.at[1])
    own_w.start()
    own_s.start()
    entry_barrier(me, cp)
    swap_g = push(g_own.at[pl.ds(8 * (1 - cp), 8)], g_oth, psend.at[0], precv.at[0], mate)
    swap_t = push(t_own.at[pl.ds(8 * (1 - cp), 8)], t_oth, psend.at[1], precv.at[1], mate)
    swap_t.start()

    def region(ref, first, count, dims, at):
        index = [slice(None) if d in dims else at[d] for d in range(3)]
        return ref.at[(pl.ds(first, count), *index)]

    def small_region(dims, at):
        index = [slice(None) if d in dims else at[d] for d in range(3)]
        return s_all.at[tuple(index)]

    forwards = []
    pending = []
    own_s.wait()
    own_w.wait()
    for phase in range(3):
        firsts = {}
        for color in range(COLORS):
            dim = GATHER_ORDER[color][phase]
            done = GATHER_ORDER[color][:phase]
            base = cp * (COLORS * NB) + color * NB
            mine = region(w_all, base, NB, done, me)
            right, left = chip_id(moved(me, dim, 1)), chip_id(moved(me, dim, 3))
            to_right = push(mine, mine, ssem.at[color, phase, 0], rsem.at[color, phase, 0], right)
            to_left = push(mine, mine, ssem.at[color, phase, 1], rsem.at[color, phase, 1], left)
            to_right.start()
            to_left.start()
            firsts[color] = (to_right, to_left)
            pending += [to_right, to_left]
            if color == 0:
                s_mine = small_region(done, me)
                s_right = push(s_mine, s_mine, s_ssem.at[phase, 0], s_rsem.at[phase, 0], right)
                s_left = push(s_mine, s_mine, s_ssem.at[phase, 1], s_rsem.at[phase, 1], left)
                s_right.start()
                s_left.start()
                pending += [s_right, s_left]
        seconds = {}
        for color in range(COLORS):
            dim = GATHER_ORDER[color][phase]
            done = GATHER_ORDER[color][:phase]
            base = cp * (COLORS * NB) + color * NB
            right, left = chip_id(moved(me, dim, 1)), chip_id(moved(me, dim, 3))
            from_left, from_right = moved(me, dim, 3), moved(me, dim, 1)
            to_right, to_left = firsts[color]
            to_right.wait_recv()
            part = region(w_all, base, HALF, done, from_left)
            on_right = push(part, part, ssem.at[color, phase, 2], rsem.at[color, phase, 2], right)
            on_right.start()
            whole_l = region(w_all, base, NB, done, from_left)
            fwd_l = push(whole_l, whole_l, fsend.at[color, phase, 0], frecv.at[color, phase, 0], mate)
            fwd_l.start()
            to_left.wait_recv()
            part = region(w_all, base + HALF, HALF, done, from_right)
            on_left = push(part, part, ssem.at[color, phase, 3], rsem.at[color, phase, 3], left)
            on_left.start()
            whole_r = region(w_all, base, NB, done, from_right)
            fwd_r = push(whole_r, whole_r, fsend.at[color, phase, 1], frecv.at[color, phase, 1], mate)
            fwd_r.start()
            seconds[color] = (on_right, on_left)
            pending += [on_right, on_left]
            forwards += [fwd_l, fwd_r]
            if color == 0:
                s_right.wait_recv()
                s_left.wait_recv()
                s_part = small_region(done, from_left)
                s_on = push(s_part, s_part, s_ssem.at[phase, 2], s_rsem.at[phase, 2], right)
                s_on.start()
                pending.append(s_on)
        for color in range(COLORS):
            dim = GATHER_ORDER[color][phase]
            done = GATHER_ORDER[color][:phase]
            base = cp * (COLORS * NB) + color * NB
            on_right, on_left = seconds[color]
            on_right.wait_recv()
            on_left.wait_recv()
            far = region(w_all, base, NB, done, moved(me, dim, 2))
            fwd_f = push(far, far, fsend.at[color, phase, 2], frecv.at[color, phase, 2], mate)
            fwd_f.start()
            forwards.append(fwd_f)
            if color == 0:
                s_on.wait_recv()
        if phase == 0:
            swap_g.start()
    for copy in forwards:
        copy.wait_recv()
    swap_g.wait()
    swap_t.wait()
    for copy in pending + forwards:
        copy.wait_send()


def gather_all(w_loc, s_loc, grad_out, tokens):
    bf16, f32 = jnp.bfloat16, jnp.float32
    blocks = w_loc.shape[0]
    seqs, pos, width = grad_out.shape
    dma = pltpu.SemaphoreType.DMA
    return pl.pallas_call(
        gather_kernel,
        out_shape=(
            jax.ShapeDtypeStruct((blocks, SIDE, SIDE, SIDE, NB, 128), bf16),
            jax.ShapeDtypeStruct((SIDE, SIDE, SIDE, 8, 128), f32),
            jax.ShapeDtypeStruct((seqs // 2, pos, width), bf16),
            jax.ShapeDtypeStruct((seqs // 2, pos), jnp.int32),
        ),
        in_specs=[ANY] * 4,
        out_specs=(ANY,) * 4,
        scratch_shapes=[dma((3, 3, 4)), dma((3, 3, 4)), dma((3, 3, 3)), dma((3, 3, 3)), dma((3, 3)), dma((3, 3)), dma((2,)), dma((2,)), dma((2,))],
        compiler_params=pltpu.CompilerParams(collective_id=0, has_side_effects=True),
        name='gather_weights',
    )(w_loc, s_loc, grad_out, tokens)


def reduce_kernel(g_all, small, y_oth, g_out, s_out, y_recv, held, pair, ra0, rb0, ra1, rb1, ra2, rb2, s_pair, s_slots, s_acc,
                  lsem, psend, precv, ssem, rsem, s_ssem, s_rsem, osend, orecv, msem):
    cp = lax.axis_index('cp')
    me = my_coords()
    mate = {'cp': 1 - cp}
    per = COLORS * NB
    loads = []
    for color in range(COLORS):
        load = pltpu.make_async_copy(g_all.at[pl.ds(cp * per + color * NB, NB)], held.at[pl.ds(color * NB, NB)], lsem.at[color])
        load.start()
        loads.append(load)
    s_load = pltpu.make_async_copy(small, s_acc, lsem.at[3])
    s_load.start()
    entry_barrier(me, cp)
    sends = []
    s_swap = push(small, s_pair, psend.at[3], precv.at[3], mate)
    s_swap.start()
    swaps = []
    for color in range(COLORS):
        swap = push(g_all.at[pl.ds((1 - cp) * per + color * NB, NB)], pair.at[pl.ds(color * NB, NB)], psend.at[color], precv.at[color], mate)
        swap.start()
        swaps.append(swap)
    y_swap = push(y_oth, y_recv, psend.at[4], precv.at[4], mate)
    y_swap.start()

    bufs = ((ra0, rb0), (ra1, rb1), (ra2, rb2))

    def index_of(dims, at):
        return [slice(None) if d in dims else at[d] for d in range(3)]

    def region(first, count, dims, at):
        return held.at[(pl.ds(first, count), *index_of(dims, at))]

    def start_phase(color, phase):
        dim = REDUCE_ORDER[color][phase]
        rest = REDUCE_ORDER[color][phase + 1:]
        base = color * NB
        ra, rb = bufs[phase]
        right, left = moved(me, dim, 1), moved(me, dim, 3)
        far = moved(me, dim, 2)
        out = [
            push(region(base, HALF, rest, far), ra.at[color, 0], ssem.at[color, phase, 0], rsem.at[color, phase, 0], chip_id(right)),
            push(region(base + HALF, HALF, rest, far), ra.at[color, 1], ssem.at[color, phase, 1], rsem.at[color, phase, 1], chip_id(left)),
            push(region(base + HALF, HALF, rest, right), rb.at[color, 0, pl.ds(HALF, HALF)], ssem.at[color, phase, 2], rsem.at[color, phase, 2], chip_id(right)),
            push(region(base, HALF, rest, left), rb.at[color, 1, pl.ds(0, HALF)], ssem.at[color, phase, 3], rsem.at[color, phase, 3], chip_id(left)),
        ]
        for copy in out:
            copy.start()
        sends.extend(out)
        return out

    def middle(color, phase, copies):
        dim = REDUCE_ORDER[color][phase]
        rest = REDUCE_ORDER[color][phase + 1:]
        base = color * NB
        ra, rb = bufs[phase]
        right, left = moved(me, dim, 1), moved(me, dim, 3)
        copies[0].wait_recv()
        to_r = index_of(rest, right)

        @pl.loop(0, HALF)
        def _(b):
            held[(base + b, *to_r)] += ra[color, 0, b]

        fwd_r = push(region(base, HALF, rest, right), rb.at[color, 0, pl.ds(0, HALF)], ssem.at[color, phase, 4], rsem.at[color, phase, 4], chip_id(right))
        fwd_r.start()
        copies[1].wait_recv()
        to_l = index_of(rest, left)

        @pl.loop(0, HALF)
        def _(b):
            held[(base + HALF + b, *to_l)] += ra[color, 1, b]

        fwd_l = push(region(base + HALF, HALF, rest, left), rb.at[color, 1, pl.ds(HALF, HALF)], ssem.at[color, phase, 5], rsem.at[color, phase, 5], chip_id(left))
        fwd_l.start()
        sends.extend([fwd_r, fwd_l])
        return [fwd_r, fwd_l]

    def finish(color, phase, copies, late):
        rest = REDUCE_ORDER[color][phase + 1:]
        base = color * NB
        ra, rb = bufs[phase]
        copies[2].wait_recv()
        copies[3].wait_recv()
        late[0].wait_recv()
        late[1].wait_recv()
        here = index_of(rest, me)

        @pl.loop(0, NB)
        def _(b):
            held[(base + b, *here)] += rb[color, 0, b] + rb[color, 1, b]

    s_copies = []

    def small_start(phase):
        dim = REDUCE_ORDER[0][phase]
        out = []
        for by in (1, 2, 3):
            out.append(push(s_acc.at[cp], s_slots.at[phase, by - 1], s_ssem.at[phase, by - 1], s_rsem.at[phase, by - 1], chip_id(moved(me, dim, by))))
        for copy in out:
            copy.start()
        return out

    def small_finish(phase, copies):
        dim = REDUCE_ORDER[0][phase]
        for copy in copies:
            copy.wait()
        mine = me[dim]
        total = None
        own = s_acc[cp]
        got = [own] + [s_slots[phase, by] for by in range(3)]
        for coord in range(SIDE):
            gap = lax.rem(mine - coord + SIDE, SIDE)
            value = jnp.where(gap == 0, got[0], jnp.where(gap == 1, got[1], jnp.where(gap == 2, got[2], got[3])))
            total = value if total is None else total + value
        s_acc[cp] = total

    s_load.wait()
    s_swap.wait()
    s_acc[...] = s_acc[...] + s_pair[...]
    s_out_copies = small_start(0)
    started = []
    for color in range(COLORS):
        loads[color].wait()
        swaps[color].wait_recv()

        @pl.loop(0, NB)
        def _(b):
            for z in range(SIDE):
                held[color * NB + b, z] += pair[color * NB + b, z]

        started.append(start_phase(color, 0))
    for phase in range(3):
        late = [middle(color, phase, started[color]) for color in range(COLORS)]
        nxt = []
        for color in range(COLORS):
            finish(color, phase, started[color], late[color])
            if phase < 2:
                nxt.append(start_phase(color, phase + 1))
        small_finish(phase, s_out_copies)
        if phase < 2:
            s_out_copies = small_start(phase + 1)
        started = nxt
    mine = held.at[:, me[0], me[1], me[2]]
    out_far = push(mine, g_out.at[pl.ds(cp * per, per)], osend.at[0], orecv.at[0], mate)
    out_far.start()
    s_far = push(s_acc.at[cp], s_out.at[cp], osend.at[1], orecv.at[1], mate)
    s_far.start()
    out_own = pltpu.make_async_copy(mine, g_out.at[pl.ds(cp * per, per)], msem.at[0])
    out_own.start()
    s_own = pltpu.make_async_copy(s_acc.at[cp], s_out.at[cp], msem.at[1])
    s_own.start()
    for copy in sends:
        copy.wait_send()
    for copy in swaps:
        copy.wait_send()
    y_swap.wait()
    out_own.wait()
    s_own.wait()
    out_far.wait()
    s_far.wait()


def reduce_all(g_all, small, y_oth):
    f32 = jnp.float32
    blocks = g_all.shape[0]
    dma = pltpu.SemaphoreType.DMA
    vm = pltpu.VMEM
    return pl.pallas_call(
        reduce_kernel,
        out_shape=(
            jax.ShapeDtypeStruct((blocks, NB, 128), f32),
            jax.ShapeDtypeStruct(small.shape, f32),
            jax.ShapeDtypeStruct(y_oth.shape, y_oth.dtype),
        ),
        in_specs=[ANY] * 3,
        out_specs=(ANY,) * 3,
        scratch_shapes=[
            vm((blocks // 2, SIDE, SIDE, SIDE, NB, 128), f32),
            vm((blocks // 2, SIDE, SIDE, SIDE, NB, 128), f32),
            vm((COLORS, 2, HALF, SIDE, SIDE, NB, 128), f32),
            vm((COLORS, 2, NB, SIDE, SIDE, NB, 128), f32),
            vm((COLORS, 2, HALF, SIDE, NB, 128), f32),
            vm((COLORS, 2, NB, SIDE, NB, 128), f32),
            vm((COLORS, 2, HALF, NB, 128), f32),
            vm((COLORS, 2, NB, NB, 128), f32),
            vm(small.shape, f32),
            vm((3, 3) + small.shape[1:], f32),
            vm(small.shape, f32),
            dma((4,)), dma((5,)), dma((5,)), dma((3, 3, 6)), dma((3, 3, 6)), dma((3, 3)), dma((3, 3)), dma((2,)), dma((2,)), dma((2,)),
        ],
        compiler_params=pltpu.CompilerParams(collective_id=1, has_side_effects=True, vmem_limit_bytes=62 * 1024 * 1024),
        name='reduce_grads',
    )(g_all, small, y_oth)


SEQS = 8
STEP_SEQS = 2
STEPS = SEQS // STEP_SEQS
SEQ = 256
TOK = STEP_SEQS * SEQ
TILES = 5
HEADS_PER = 4
HEAD = 32
LANES = 128
F32 = jnp.float32
BF16 = jnp.bfloat16


def mm(lhs, rhs):
    return lax.dot_general(lhs, rhs, (((1,), (0,)), ((), ())), preferred_element_type=F32)


def mm_t(lhs, rhs):
    return lax.dot_general(lhs, rhs, (((1,), (1,)), ((), ())), preferred_element_type=F32)


def fold8(value):
    return jnp.sum(value.reshape(value.shape[0] // 8, 8, value.shape[1]), axis=0)


def wide(ref, first, count):
    return jnp.concatenate([ref[first + j] for j in range(count)], axis=1)


def add_blocks(ref, first, value):
    for j in range(value.shape[1] // LANES):
        ref[first + j] += value[:, j * LANES:(j + 1) * LANES]


def norm_stats(value):
    mean = jnp.mean(value, axis=-1, keepdims=True)
    cent = value - mean
    var = jnp.mean(cent * cent, axis=-1, keepdims=True)
    rstd = lax.rsqrt(var + LN_EPS)
    return cent * rstd, rstd


def norm_back(d_out, gain, xhat, rstd):
    d_hat = d_out * gain
    m1 = jnp.mean(d_hat, axis=-1, keepdims=True)
    m2 = jnp.mean(d_hat * xhat, axis=-1, keepdims=True)
    return rstd * (d_hat - m1 - xhat * m2)


def gelu_pair(u):
    z = u * (0.5 ** 0.5)
    t = 1.0 / (1.0 + 0.3275911 * jnp.abs(z))
    poly = t * (0.127414796 + t * (-0.142248368 + t * (0.710706871 + t * (-0.7265760135 + t * 0.5307027145))))
    ex = jnp.exp(-z * z)
    tail = poly * ex
    cdf = jnp.where(u >= 0, 1.0 - tail, tail)
    return u * cdf, cdf + u * (ex * 0.3989422804014327)


def unturn(z, cos, sin, groups):
    parts = z.reshape(groups, 2, HEAD // 2, z.shape[1])
    lo, up = parts[:, 0], parts[:, 1]
    out = jnp.stack([lo * cos + up * sin, up * cos - lo * sin], axis=1)
    return out.reshape(z.shape)


def turn(z, cos, sin, groups):
    return unturn(z, cos, -sin, groups)


def layer_kernel(tok_ref, keep_ref, mask_ref, emb_ref, vec_ref, bqkv_ref, bup_ref, cos_ref, sin_ref, cosn_ref, sinn_ref,
                 w_hbm, g_own, g_oth,
                 y_own, y_oth, grads, dtab, dsum, dbq, dbkv, dbup,
                 w, wt, acc, gbuf, e_s, ht, qt, kt, vt, qn, kn, vn, pt, ot32, otb, x1, nm, nmt, y_s, dnm, dot_s, dqkv,
                 wsem, gsem, osem):
    step = pl.program_id(0)
    cp = lax.axis_index('cp')
    chips = SIDE ** 3

    @pl.when(step == 0)
    def _():
        own = pltpu.make_async_copy(g_own.at[pl.ds(cp * SEQS, SEQS)], gbuf.at[:, 0], gsem.at[0])
        oth = pltpu.make_async_copy(g_oth, gbuf.at[:, 1], gsem.at[1])

        @pl.loop(0, chips)
        def _(i):
            pltpu.make_async_copy(w_hbm.at[:, i], w.at[:, pl.ds(i * NB, NB), :], wsem).start()

        own.start()
        oth.start()

        @pl.loop(0, 60)
        def _(i):
            acc[i] = jnp.zeros((640, LANES), F32)

        dtab[...] = jnp.zeros_like(dtab)
        dsum[...] = jnp.zeros_like(dsum)
        dbq[...] = jnp.zeros_like(dbq)
        dbkv[...] = jnp.zeros_like(dbkv)
        dbup[...] = jnp.zeros_like(dbup)

        @pl.loop(0, chips)
        def _(i):
            pltpu.make_async_copy(w_hbm.at[:, i], w.at[:, pl.ds(i * NB, NB), :], wsem).wait()

        own.wait()
        oth.wait()

        @pl.loop(0, 15)
        def _(n):
            wt[n] = w[n].T

    def grad_rows():
        return gbuf[pl.ds(step * STEP_SEQS, STEP_SEQS)].reshape(TOK, 640)

    vocab = lax.broadcasted_iota(jnp.int32, (64, TOK), 0)
    one_hot = jnp.where(vocab == tok_ref[0], 1.0, 0.0).astype(BF16)
    e_s[...] = lax.dot_general(one_hot, emb_ref[...], (((0,), (0,)), ((), ())), preferred_element_type=F32)

    @pl.loop(0, TOK // 128)
    def _(r):
        rows = pl.ds(pl.multiple_of(r * 128, 128), 128)
        keep = jnp.concatenate([keep_ref[rows]] * TILES, axis=1)
        emb = e_s[rows] * keep
        e_s[rows] = emb
        xhat, _ = norm_stats(emb)
        nm[rows] = (xhat * vec_ref[0:1] + vec_ref[1:2]).astype(BF16)

    ht[...] = nm[...].T

    cos, sin = cos_ref[...], sin_ref[...]
    for kind, (t_ref, n_ref) in enumerate(((qt, qn), (kt, kn), (vt, vn))):
        z = mm(wt[kind * TILES:(kind + 1) * TILES].reshape(640, 640), ht[...])
        bias = bqkv_ref[kind * 640:(kind + 1) * 640]
        z = z + jnp.concatenate([bias] * (TOK // LANES), axis=1)
        if kind == 0:
            z = z * HEAD ** -0.5
        if kind < 2:
            z = turn(z, cos, sin, 20)
        zb = z.astype(BF16)
        for s in range(STEP_SEQS):
            for t in range(TILES):
                piece = zb[t * LANES:(t + 1) * LANES, s * SEQ:(s + 1) * SEQ]
                t_ref[s, t] = piece
                n_ref[s, t] = piece.T

    lane_head = lax.broadcasted_iota(jnp.int32, (1, LANES), 1) // HEAD
    pick = [jnp.where(lane_head == h, 1.0, 0.0).astype(BF16) for h in range(HEADS_PER)]

    def stack(tile):
        return jnp.concatenate([tile * pick[h] for h in range(HEADS_PER)], axis=0)

    def spot(h):
        return slice((h % 2) * SEQ, (h % 2 + 1) * SEQ), (h // 2) * SEQ

    def stage(buf, value):
        for h in range(HEADS_PER):
            down, along = spot(h)
            buf[down, along:along + SEQ] = value[h * SEQ:(h + 1) * SEQ]

    @pl.loop(0, STEP_SEQS)
    def _(s):
        rows = pl.ds(pl.multiple_of(s * SEQ, SEQ), SEQ)
        bufs = (y_s, dnm)

        def scores(t):
            stage(bufs[t % 2], mm(stack(kn[s, t]), qt[s, t]))

        scores(0)
        for t in range(TILES):
            if t + 1 < TILES:
                scores(t + 1)
            bias = mask_ref[rows]
            for h in range(HEADS_PER):
                down, along = spot(h)
                for c in range(0, SEQ, LANES):
                    score = bufs[t % 2][down, along + c:along + c + LANES] + bias
                    p = jnp.exp(score - jnp.max(score, axis=0, keepdims=True))
                    p = p * (1.0 / jnp.sum(p, axis=0, keepdims=True))
                    pt[s, t * HEADS_PER + h, :, c:c + LANES] = p.astype(BF16)
            v_t = vt[s, t]
            out = jnp.concatenate([mm(v_t[h * HEAD:(h + 1) * HEAD], pt[s, t * HEADS_PER + h]) for h in range(HEADS_PER)], axis=0)
            ot32[s, t] = out
            outb = out.astype(BF16)
            otb[t, :, rows] = outb
            dqkv[t, rows] = outb.T

    w_out = wide(w, 15, TILES)
    x1[...] = e_s[...] + mm(wide(dqkv, 0, TILES), w_out) + vec_ref[5:6]

    @pl.loop(0, TOK // 128)
    def _(r):
        rows = pl.ds(pl.multiple_of(r * 128, 128), 128)
        xhat, _ = norm_stats(x1[rows])
        nm[rows] = (xhat * vec_ref[6:7] + vec_ref[7:8]).astype(BF16)

    nmt[...] = nm[...].T
    y_s[...] = jnp.zeros_like(y_s)
    dnm[...] = jnp.zeros_like(dnm)

    @pl.loop(0, 4)
    def _(c):
        g = grad_rows()
        w_up = wide(w, 20 + TILES * c, TILES)
        u = mm(nm[...], w_up) + bup_ref[c]
        a, slope = gelu_pair(u)
        ab = a.astype(BF16)
        w_down = wide(w, 40 + TILES * c, TILES)
        du = mm_t(g, w_down) * slope
        dbup[c] += fold8(du)
        dub = du.astype(BF16)
        y_s[...] += mm(ab, w_down)
        dnm[...] += mm_t(dub, w_up)
        add_blocks(acc, 40 + TILES * c, mm(ab.T, g))
        add_blocks(acc, 20 + TILES * c, mm(nmt[...], dub))

    @pl.loop(0, TOK // 128)
    def _(r):
        rows = pl.ds(pl.multiple_of(r * 128, 128), 128)
        x = x1[rows]
        out = (x + y_s[rows] + vec_ref[8:9]).astype(BF16)
        seq = r // 2

        @pl.when(lax.rem(r, 2) == 0)
        def _():
            y_own[seq] = out

        @pl.when(lax.rem(r, 2) == 1)
        def _():
            y_oth[seq] = out

        xhat, rstd = norm_stats(x)
        d_n = dnm[rows]
        g32 = gbuf[step * STEP_SEQS + seq, lax.rem(r, 2)].astype(F32)
        dsum[3] += fold8(d_n * xhat)
        dsum[4] += fold8(d_n)
        d_r = g32 + norm_back(d_n, vec_ref[6:7], xhat, rstd)
        dsum[2] += fold8(d_r)
        dsum[5] += fold8(g32)
        y_s[rows] = d_r
        nm[rows] = d_r.astype(BF16)

    d_rb = nm[...]
    add_blocks(acc, 15, mm(otb[...].reshape(640, TOK), d_rb))
    d_o = mm(wide(w, 15, TILES), d_rb.T)
    for t in range(TILES):
        dot_s[t] = d_o[t * LANES:(t + 1) * LANES]

    @pl.loop(0, STEP_SEQS)
    def _(s):
        rows = pl.ds(pl.multiple_of(s * SEQ, SEQ), SEQ)
        bufs = (x1, dnm)
        outs = (nm, nmt)

        def slopes(t):
            stage(bufs[t % 2], mm(stack(vn[s, t]), dot_s[t, :, rows].astype(BF16)))

        slopes(0)
        for t in range(TILES):
            if t + 1 < TILES:
                slopes(t + 1)
            d_ot = dot_s[t, :, rows]
            prod = d_ot * ot32[s, t]
            ds_ref = outs[t % 2]
            for h in range(HEADS_PER):
                down, along = spot(h)
                delta = jnp.sum(prod[h * HEAD:(h + 1) * HEAD], axis=0, keepdims=True)
                for c in range(0, SEQ, LANES):
                    d_p = bufs[t % 2][down, along + c:along + c + LANES]
                    p = pt[s, t * HEADS_PER + h, :, c:c + LANES].astype(F32)
                    ds_ref[down, along + c:along + c + LANES] = (p * (d_p - delta[:, c:c + LANES])).astype(BF16)
            k_t, q_n = kt[s, t], qn[s, t]
            dqs = []
            for h in range(HEADS_PER):
                down, along = spot(h)
                dqs.append(mm(k_t[h * HEAD:(h + 1) * HEAD], ds_ref[down, along:along + SEQ]))
            dq = unturn(jnp.concatenate(dqs, axis=0), cos[:, :SEQ], sin[:, :SEQ], HEADS_PER) * HEAD ** -0.5
            dbq[t] += dq[:, :LANES] + dq[:, LANES:]
            dqkv[t, rows] = dq.astype(BF16).T
            dk = mm(ds_ref[:SEQ, :2 * SEQ], jnp.concatenate([q_n * pick[0], q_n * pick[2]], axis=0))
            dk = dk + mm(ds_ref[SEQ:2 * SEQ, :2 * SEQ], jnp.concatenate([q_n * pick[1], q_n * pick[3]], axis=0))
            p_wide = jnp.concatenate([pt[s, t * HEADS_PER + h] for h in range(HEADS_PER)], axis=1)
            dv = mm(p_wide, stack(d_ot.astype(BF16).T))
            low = lax.rem(lax.broadcasted_iota(jnp.int32, (SEQ, LANES), 1), HEAD) < HEAD // 2
            other = jnp.where(low, pltpu.roll(dk, LANES - HEAD // 2, 1), pltpu.roll(dk, HEAD // 2, 1))
            dk = dk * cosn_ref[...] + other * sinn_ref[...]
            dbkv[0, t] += fold8(dk)
            dbkv[1, t] += fold8(dv)
            dqkv[TILES + t, rows] = dk.astype(BF16)
            dqkv[2 * TILES + t, rows] = dv.astype(BF16)

    for kind in range(3):
        add_blocks(acc, kind * TILES, mm(ht[...], wide(dqkv, kind * TILES, TILES)))
    dnm[...] = mm(wide(dqkv, 0, 15), wt[...].reshape(1920, 640))

    @pl.loop(0, TOK // 128)
    def _(r):
        rows = pl.ds(pl.multiple_of(r * 128, 128), 128)
        xhat, rstd = norm_stats(e_s[rows])
        d_n = dnm[rows]
        dsum[0] += fold8(d_n * xhat)
        dsum[1] += fold8(d_n)
        keep = jnp.concatenate([keep_ref[rows]] * TILES, axis=1)
        nm[rows] = ((norm_back(d_n, vec_ref[0:1], xhat, rstd) + y_s[rows]) * keep).astype(BF16)

    dtab[...] += mm(one_hot, nm[...])

    @pl.when(step == STEPS - 1)
    def _():
        @pl.loop(0, chips)
        def _(i):
            pltpu.make_async_copy(acc.at[:, pl.ds(i * NB, NB), :], grads.at[:, i], osem).start()

        @pl.loop(0, chips)
        def _(i):
            pltpu.make_async_copy(acc.at[:, pl.ds(i * NB, NB), :], grads.at[:, i], osem).wait()


def layer_call(tok, keep, mask, emb, vecs, bqkv, bup, cos, sin, cosn, sinn, w_hbm, g_own, g_oth):
    vm = pltpu.VMEM
    dma = pltpu.SemaphoreType.DMA

    def whole(shape):
        return pl.BlockSpec(shape, lambda i: (0,) * len(shape))

    pair = pl.BlockSpec((STEP_SEQS, 128, 640), lambda i: (i, 0, 0))
    out_shape = (
        jax.ShapeDtypeStruct((SEQS, 128, 640), BF16),
        jax.ShapeDtypeStruct((SEQS, 128, 640), BF16),
        jax.ShapeDtypeStruct((60, 64, NB, LANES), F32),
        jax.ShapeDtypeStruct((64, 640), F32),
        jax.ShapeDtypeStruct((6, 8, 640), F32),
        jax.ShapeDtypeStruct((TILES, LANES, LANES), F32),
        jax.ShapeDtypeStruct((2, TILES, 8, LANES), F32),
        jax.ShapeDtypeStruct((4, 8, 640), F32),
    )
    out_specs = (pair, pair, ANY) + tuple(whole(o.shape) for o in out_shape[3:])
    in_specs = [
        pl.BlockSpec((1, 1, TOK), lambda i: (i, 0, 0)),
        pl.BlockSpec((TOK, LANES), lambda i: (i, 0)),
        pl.BlockSpec((TOK, LANES), lambda i: (i, 0)),
    ] + [whole(a.shape) for a in (emb, vecs, bqkv, bup, cos, sin, cosn, sinn)] + [ANY] * 3
    halves = (STEP_SEQS, TILES, LANES, SEQ)
    flipped = (STEP_SEQS, TILES, SEQ, LANES)
    scratch = [
        vm((60, 640, LANES), BF16), vm((15, LANES, 640), BF16), vm((60, 640, LANES), F32), vm((SEQS, 2, 128, 640), BF16),
        vm((TOK, 640), F32), vm((640, TOK), BF16),
        vm(halves, BF16), vm(halves, BF16), vm(halves, BF16), vm(flipped, BF16), vm(flipped, BF16), vm(flipped, BF16),
        vm((STEP_SEQS, 20, SEQ, SEQ), BF16), vm(halves, F32), vm((TILES, LANES, TOK), BF16),
        vm((TOK, 640), F32), vm((TOK, 640), BF16), vm((640, TOK), BF16), vm((TOK, 640), F32), vm((TOK, 640), F32),
        vm((TILES, LANES, TOK), F32), vm((15, TOK, LANES), BF16),
        dma, dma((2,)), dma,
    ]
    return pl.pallas_call(
        layer_kernel,
        grid=(STEPS,),
        out_shape=out_shape,
        in_specs=in_specs,
        out_specs=out_specs,
        scratch_shapes=scratch,
        compiler_params=pltpu.CompilerParams(dimension_semantics=('arbitrary',), vmem_limit_bytes=67043328),
        name='layer',
    )(tok, keep, mask, emb, vecs, bqkv, bup, cos, sin, cosn, sinn, w_hbm, g_own, g_oth)


def prepare(tokens, lengths, positions, embed_table, vecs_all):
    n_seq, seq_len = tokens.shape
    is_mask = tokens == MASK_ID
    tok_valid = positions[None, :] < lengths[:, None]
    mask_count = jnp.sum(is_mask.astype(jnp.int32), axis=1)
    drop_scale = (1.0 - TRAIN_RATIO) / (1.0 - mask_count.astype(F32) / lengths.astype(F32))
    keep = jnp.where(is_mask | jnp.logical_not(tok_valid), 0.0, drop_scale[:, None])
    keep = jnp.broadcast_to(keep.reshape(-1, 1), (n_seq * seq_len, LANES))
    mask = jnp.broadcast_to(jnp.where(tok_valid, 0.0, NEG_BIG).reshape(-1, 1), (n_seq * seq_len, LANES)).astype(F32)
    emb = jnp.pad(embed_table, ((0, 64 - embed_table.shape[0]), (0, 0)))
    bqkv = jnp.broadcast_to(vecs_all[2:5].reshape(-1, 1), (1920, LANES))
    inv_freq = 1.0 / (ROPE_BASE ** (jnp.arange(0, HEAD, 2, dtype=F32) / HEAD))
    angles = positions.astype(F32)[:, None] * inv_freq[None, :]
    cos, sin = jnp.cos(angles), jnp.sin(angles)
    cos_t, sin_t = jnp.tile(cos.T, (1, STEP_SEQS)), jnp.tile(sin.T, (1, STEP_SEQS))
    cos_n = jnp.tile(cos, (1, 8))
    sin_n = jnp.tile(jnp.concatenate([sin, -sin], axis=1), (1, 4))
    return tokens.reshape(STEPS, 1, TOK), keep, mask, emb, bqkv, cos_t, sin_t, cos_n, sin_n


def solution(mesh):
    chips = mesh.shape['fsdp']

    def local_step(tokens, lengths, embed_table, layer_vecs, w_qkv, w_out, w_up, b_up, w_down, grad_out):
        f32 = jnp.float32
        cp = lax.axis_index('cp')
        chip = lax.axis_index('fsdp')
        n_seq, seq_loc = tokens.shape
        half = n_seq // 2
        rows = w_qkv.shape[0]
        vocab, width = embed_table.shape
        w_loc = jnp.concatenate([
            w_qkv.reshape(rows, 15, 128).transpose(1, 0, 2),
            w_out.reshape(rows, 5, 128).transpose(1, 0, 2),
            w_up.reshape(rows, chips, 4, NB).transpose(2, 1, 3, 0).reshape(20, 128, rows).transpose(0, 2, 1),
            w_down.reshape(4, NB, 5, 128).transpose(0, 2, 1, 3).reshape(20, NB, 128),
        ], axis=0)
        s_loc = jnp.pad(jnp.concatenate([layer_vecs.reshape(-1), b_up]), (0, 1024 - 130)).reshape(8, 128)
        w_all, s_all, g_oth, t_oth = gather_all(w_loc, s_loc, grad_out, tokens)
        s_flat = s_all.reshape(chips, 1024)
        vecs_all = s_flat[:, :90].reshape(chips, 9, NB).transpose(1, 0, 2).reshape(9, width)
        up_b = s_flat[:, 90:130].reshape(chips, 4, NB).transpose(1, 0, 2).reshape(-1)
        start = half * cp
        tok_full = jnp.concatenate([lax.dynamic_slice_in_dim(tokens, start, half, 0), t_oth], axis=1)
        len_own = lax.dynamic_slice_in_dim(lengths, start, half, 0)
        positions = jnp.concatenate([cp * seq_loc + jnp.arange(seq_loc), (1 - cp) * seq_loc + jnp.arange(seq_loc)])
        tok, keep, mask, emb, bqkv, cos, sin, cosn, sinn = prepare(tok_full, len_own, positions, embed_table, vecs_all)
        y_own, y_oth, g_all, dtab, dsum, dbq, dbkv, dbup = layer_call(
            tok, keep, mask, emb, vecs_all, bqkv, up_b.reshape(4, 1, 640), cos, sin, cosn, sinn, w_all.reshape(60, chips, NB, 128), grad_out, g_oth)
        rowsum = jnp.sum(dsum, axis=1)
        d_bq = jnp.sum(dbq, axis=2).reshape(1, width)
        d_bkv = jnp.sum(dbkv, axis=2).reshape(2, width)
        small = jnp.concatenate([dtab[:vocab].reshape(-1), rowsum[:2].reshape(-1), d_bq.reshape(-1), d_bkv.reshape(-1), rowsum[2:].reshape(-1), jnp.sum(dbup, axis=1).reshape(-1)])
        small = jnp.pad(small, (0, 2 * SMALL_ROWS * 128 - small.shape[0])).reshape(2, SMALL_ROWS, 128)
        g_red, s_red, y_recv = reduce_all(g_all.reshape(60, SIDE, SIDE, SIDE, NB, 128), small, y_oth)
        out_full = jnp.where(cp == 0, jnp.concatenate([y_own, y_recv], axis=0), jnp.concatenate([y_recv, y_own], axis=0))
        s_flat = s_red.reshape(-1)
        n_tab = vocab * width
        d_embed = s_flat[:n_tab].reshape(vocab, width)
        d_v = lax.dynamic_slice(s_flat[n_tab:n_tab + 9 * width].reshape(9, width), (0, chip * NB), (9, NB))
        d_b = s_flat[n_tab + 9 * width:n_tab + 9 * width + 2560].reshape(4, chips, NB)
        d_b = lax.dynamic_slice(d_b, (0, chip, 0), (4, 1, NB)).reshape(-1)
        d_qkv = g_red[:15].transpose(1, 0, 2).reshape(w_qkv.shape)
        d_wout = g_red[15:20].transpose(1, 0, 2).reshape(w_out.shape)
        d_wup = g_red[20:40].transpose(0, 2, 1).reshape(4, chips, NB, rows).transpose(3, 1, 0, 2).reshape(w_up.shape)
        d_wdown = g_red[40:60].reshape(4, 5, NB, 128).transpose(0, 2, 1, 3).reshape(w_down.shape)
        return out_full, d_embed, d_v, d_qkv, d_wout, d_wup, d_b, d_wdown

    in_specs = (P('fsdp', 'cp'), P('fsdp'), P(), P(None, 'fsdp'), P('fsdp', None, None, None), P('fsdp', None), P('fsdp', None), P('fsdp'), P('fsdp', None), P('fsdp', 'cp', None))
    out_specs = (P('fsdp', 'cp', None), P(), P(None, 'fsdp'), P('fsdp', None, None, None), P('fsdp', None), P('fsdp', None), P('fsdp'), P('fsdp', None))
    return jax.shard_map(local_step, mesh=mesh, in_specs=in_specs, out_specs=out_specs, check_vma=False)
```

```python
import functools

import jax
import jax.numpy as jnp
from jax import lax
from jax.experimental import pallas as pl
from jax.experimental.pallas import tpu as pltpu
from jax.sharding import PartitionSpec as P

MASK_ID = 32
LN_EPS = 1e-5
ROPE_BASE = 10000.0
TRAIN_RATIO = 0.15 * 0.8
NEG_BIG = -1e30
SIDE = 4
COLORS = 3
NB = 10
GROUP = 5
PER = 6
SMALL_ROWS = 120
QUARTERS = (2, 1, 3, 0)
MESH_ID = pl.DeviceIdType.MESH
ANY = pl.BlockSpec(memory_space=pl.ANY)

GATHER_ORDER = ((2, 1, 0), (1, 0, 2), (0, 2, 1))
REDUCE_ORDER = ((0, 1, 2), (1, 2, 0), (2, 0, 1))


def my_coords():
    chip = lax.axis_index('fsdp')
    return [chip // 16, lax.rem(chip // 4, 4), lax.rem(chip, 4)]


def moved(coords, dim, by):
    out = list(coords)
    out[dim] = lax.rem(coords[dim] + by + SIDE, SIDE)
    return out


def chip_id(coords):
    return {'fsdp': coords[0] * 16 + coords[1] * 4 + coords[2]}


def entry_barrier(coords, cp):
    barrier = pltpu.get_barrier_semaphore()
    for dim in range(3):
        for by in (1, 2, 3):
            pl.semaphore_signal(barrier, inc=1, device_id=chip_id(moved(coords, dim, by)), device_id_type=MESH_ID)
    pl.semaphore_signal(barrier, inc=1, device_id={'cp': 1 - cp}, device_id_type=MESH_ID)
    pl.semaphore_wait(barrier, 10)


def push(src, dst, send_sem, recv_sem, target):
    return pltpu.make_async_remote_copy(src_ref=src, dst_ref=dst, send_sem=send_sem, recv_sem=recv_sem, device_id=target, device_id_type=MESH_ID)


def gather_kernel(w_loc, s_loc, g_own, t_own, w_out, s_out, g_oth, t_oth, w_all, s_all, ssem, rsem, fsend, frecv, s_ssem, s_rsem, psend, precv, lsem, osem, xsem):
    cp = lax.axis_index('cp')
    me = my_coords()
    mate = {'cp': 1 - cp}
    own_w = pltpu.make_async_copy(w_loc, w_all.at[me[0], me[1], me[2]], lsem.at[0])
    own_s = pltpu.make_async_copy(s_loc, s_all.at[me[0], me[1], me[2]], lsem.at[1])
    own_w.start()
    own_s.start()
    entry_barrier(me, cp)
    swap_g = push(g_own.at[pl.ds(8 * (1 - cp), 8)], g_oth, psend.at[0], precv.at[0], mate)
    swap_t = push(t_own.at[pl.ds(8 * (1 - cp), 8)], t_oth, psend.at[1], precv.at[1], mate)
    swap_t.start()

    def region(ref, first, count, dims, at):
        index = [slice(None) if d in dims else at[d] for d in range(3)]
        return ref.at[(*index, pl.ds(first, count))]

    def small_region(dims, at):
        index = [slice(None) if d in dims else at[d] for d in range(3)]
        return s_all.at[tuple(index)]

    forwards = []
    pending = []
    stores = []
    arrivals = {}

    def store(first, count, dims, at, sem):
        index = [slice(None) if d in dims else at[d] for d in range(3)]
        index = (*index, pl.ds(first, count))
        copy = pltpu.make_async_copy(w_all.at[index], w_out.at[index], sem)
        copy.start()
        stores.append(copy)

    own_s.wait()
    own_w.wait()
    store(0, 2 * PER, (), me, lsem.at[2])
    for phase in range(3):
        firsts = {}
        for color in range(COLORS):
            dim = GATHER_ORDER[color][phase]
            done = GATHER_ORDER[color][:phase]
            base = cp * PER + color * 2
            mine = region(w_all, base, 2, done, me)
            right, left = chip_id(moved(me, dim, 1)), chip_id(moved(me, dim, 3))
            to_right = push(mine, mine, ssem.at[color, phase, 0], rsem.at[color, phase, 0], right)
            to_left = push(mine, mine, ssem.at[color, phase, 1], rsem.at[color, phase, 1], left)
            to_right.start()
            to_left.start()
            firsts[color] = (to_right, to_left)
            pending += [to_right, to_left]
            if color == 0:
                s_mine = small_region(done, me)
                s_right = push(s_mine, s_mine, s_ssem.at[phase, 0], s_rsem.at[phase, 0], right)
                s_left = push(s_mine, s_mine, s_ssem.at[phase, 1], s_rsem.at[phase, 1], left)
                s_right.start()
                s_left.start()
                pending += [s_right, s_left]
        seconds = {}
        for color in range(COLORS):
            dim = GATHER_ORDER[color][phase]
            done = GATHER_ORDER[color][:phase]
            base = cp * PER + color * 2
            right, left = chip_id(moved(me, dim, 1)), chip_id(moved(me, dim, 3))
            from_left, from_right = moved(me, dim, 3), moved(me, dim, 1)
            to_right, to_left = firsts[color]
            to_right.wait_recv()
            part = region(w_all, base, 1, done, from_left)
            on_right = push(part, part, ssem.at[color, phase, 2], rsem.at[color, phase, 2], right)
            on_right.start()
            whole_l = region(w_all, base, 2, done, from_left)
            fwd_l = push(whole_l, whole_l, fsend.at[color, phase, 0], frecv.at[color, phase, 0], mate)
            fwd_l.start()
            store(base, 2, done, from_left, osem.at[color, phase, 0])
            to_left.wait_recv()
            part = region(w_all, base + 1, 1, done, from_right)
            on_left = push(part, part, ssem.at[color, phase, 3], rsem.at[color, phase, 3], left)
            on_left.start()
            whole_r = region(w_all, base, 2, done, from_right)
            fwd_r = push(whole_r, whole_r, fsend.at[color, phase, 1], frecv.at[color, phase, 1], mate)
            fwd_r.start()
            store(base, 2, done, from_right, osem.at[color, phase, 1])
            seconds[color] = (on_right, on_left)
            pending += [on_right, on_left]
            forwards += [fwd_l, fwd_r]
            arrivals[color, phase] = [(fwd_l, done, from_left, 0), (fwd_r, done, from_right, 1)]
            if color == 0:
                s_right.wait_recv()
                s_left.wait_recv()
                s_part = small_region(done, from_left)
                s_on = push(s_part, s_part, s_ssem.at[phase, 2], s_rsem.at[phase, 2], right)
                s_on.start()
                pending.append(s_on)
        for color in range(COLORS):
            dim = GATHER_ORDER[color][phase]
            done = GATHER_ORDER[color][:phase]
            base = cp * PER + color * 2
            on_right, on_left = seconds[color]
            on_right.wait_recv()
            on_left.wait_recv()
            far = region(w_all, base, 2, done, moved(me, dim, 2))
            fwd_f = push(far, far, fsend.at[color, phase, 2], frecv.at[color, phase, 2], mate)
            fwd_f.start()
            store(base, 2, done, moved(me, dim, 2), osem.at[color, phase, 2])
            forwards.append(fwd_f)
            arrivals[color, phase].append((fwd_f, done, moved(me, dim, 2), 2))
            if color == 0:
                s_on.wait_recv()
        if phase == 0:
            swap_g.start()
    s_store = pltpu.make_async_copy(s_all, s_out, lsem.at[3])
    s_store.start()
    for phase in range(3):
        for color in range(COLORS):
            for copy, done, at, slot in arrivals[color, phase]:
                copy.wait_recv()
                store((1 - cp) * PER + color * 2, 2, done, at, xsem.at[color, phase, slot])
    s_store.wait()
    for copy in stores:
        copy.wait()
    swap_g.wait()
    swap_t.wait()
    for copy in pending + forwards:
        copy.wait_send()


def gather_all(w_loc, s_loc, grad_out, tokens):
    bf16, f32 = jnp.bfloat16, jnp.float32
    seqs, pos, width = grad_out.shape
    dma = pltpu.SemaphoreType.DMA
    return pl.pallas_call(
        gather_kernel,
        out_shape=(
            jax.ShapeDtypeStruct((SIDE, SIDE, SIDE, *w_loc.shape), bf16),
            jax.ShapeDtypeStruct((SIDE, SIDE, SIDE, 8, 128), f32),
            jax.ShapeDtypeStruct((seqs // 2, pos, width), bf16),
            jax.ShapeDtypeStruct((seqs // 2, pos), jnp.int32),
        ),
        in_specs=[ANY] * 4,
        out_specs=(ANY,) * 4,
        scratch_shapes=[
            pltpu.VMEM((SIDE, SIDE, SIDE, *w_loc.shape), bf16), pltpu.VMEM((SIDE, SIDE, SIDE, 8, 128), f32),
            dma((3, 3, 4)), dma((3, 3, 4)), dma((3, 3, 3)), dma((3, 3, 3)), dma((3, 3)), dma((3, 3)), dma((2,)), dma((2,)), dma((4,)), dma((3, 3, 3)), dma((3, 3, 3)),
        ],
        compiler_params=pltpu.CompilerParams(collective_id=0, has_side_effects=True, vmem_limit_bytes=40 * 1024 * 1024),
        name='gather_weights',
    )(w_loc, s_loc, grad_out, tokens)


def reduce_kernel(g_all, small, y_oth, g_out, s_out, y_recv, held, pair, ra0, rb0, ra1, rb1, ra2, rb2, s_pair, s_slots, s_acc,
                  lsem, psend, precv, ssem, rsem, s_ssem, s_rsem, osend, orecv, msem):
    cp = lax.axis_index('cp')
    me = my_coords()
    mate = {'cp': 1 - cp}
    per = PER
    loads = {}

    def quarter(ref, first, color, by):
        dim = REDUCE_ORDER[color][0]
        index = [slice(None)] * 3
        index[dim] = moved(me, dim, by)[dim]
        return ref.at[(*index, pl.ds(first + color * 2, 2))]

    for by in QUARTERS:
        for color in range(COLORS):
            load = pltpu.make_async_copy(quarter(g_all, cp * per, color, by), quarter(held, 0, color, by), lsem.at[color, by])
            load.start()
            loads[color, by] = load
    s_load = pltpu.make_async_copy(small, s_acc, msem.at[2])
    s_load.start()
    entry_barrier(me, cp)
    sends = []
    s_swap = push(small, s_pair, osend.at[2], orecv.at[2], mate)
    s_swap.start()
    swaps = {}
    for by in QUARTERS:
        for color in range(COLORS):
            swap = push(quarter(g_all, (1 - cp) * per, color, by), quarter(pair, 0, color, by), psend.at[color, by], precv.at[color, by], mate)
            swap.start()
            swaps[color, by] = swap
    y_swap = push(y_oth, y_recv, osend.at[3], orecv.at[3], mate)
    y_swap.start()

    bufs = ((ra0, rb0), (ra1, rb1), (ra2, rb2))

    def index_of(dims, at):
        return [slice(None) if d in dims else at[d] for d in range(3)]

    def region(first, count, dims, at):
        return held.at[(*index_of(dims, at), pl.ds(first, count))]

    def side(rb, color, way, rest, half):
        return rb.at[(color, way, *[slice(None)] * len(rest), pl.ds(half, 1))]

    def accumulate(rest, at, first, count, *sources):
        where = index_of(rest, at)
        units = slice(first, first + count)

        def add(lead):
            total = held[(*where, units)]
            for ref, color, way in sources:
                total = total + ref[(color, way, *lead)]
            held[(*where, units)] = total

        if rest:
            dim = min(rest)

            @pl.loop(0, SIDE)
            def _(v):
                where[dim] = v
                add((v,))
        else:
            add(())

    def start_phase(color, phase, part=None):
        dim = REDUCE_ORDER[color][phase]
        rest = REDUCE_ORDER[color][phase + 1:]
        base = color * 2
        ra, rb = bufs[phase]
        right, left = moved(me, dim, 1), moved(me, dim, 3)
        far = moved(me, dim, 2)
        out = [
            push(region(base, 1, rest, far), ra.at[color, 0], ssem.at[color, phase, 0], rsem.at[color, phase, 0], chip_id(right)),
            push(region(base + 1, 1, rest, far), ra.at[color, 1], ssem.at[color, phase, 1], rsem.at[color, phase, 1], chip_id(left)),
            push(region(base + 1, 1, rest, right), side(rb, color, 0, rest, 1), ssem.at[color, phase, 2], rsem.at[color, phase, 2], chip_id(right)),
            push(region(base, 1, rest, left), side(rb, color, 1, rest, 0), ssem.at[color, phase, 3], rsem.at[color, phase, 3], chip_id(left)),
        ]
        if part is not None:
            out = {2: out[:2], 1: out[2:3], 3: out[3:]}[part]
        for copy in out:
            copy.start()
        sends.extend(out)
        return out

    def middle(color, phase, copies):
        dim = REDUCE_ORDER[color][phase]
        rest = REDUCE_ORDER[color][phase + 1:]
        base = color * 2
        ra, rb = bufs[phase]
        right, left = moved(me, dim, 1), moved(me, dim, 3)
        copies[0].wait_recv()
        accumulate(rest, right, base, 1, (ra, color, 0))

        fwd_r = push(region(base, 1, rest, right), side(rb, color, 0, rest, 0), ssem.at[color, phase, 4], rsem.at[color, phase, 4], chip_id(right))
        fwd_r.start()
        copies[1].wait_recv()
        accumulate(rest, left, base + 1, 1, (ra, color, 1))

        fwd_l = push(region(base + 1, 1, rest, left), side(rb, color, 1, rest, 1), ssem.at[color, phase, 5], rsem.at[color, phase, 5], chip_id(left))
        fwd_l.start()
        sends.extend([fwd_r, fwd_l])
        return [fwd_r, fwd_l]

    def finish(color, phase, copies, late):
        rest = REDUCE_ORDER[color][phase + 1:]
        base = color * 2
        ra, rb = bufs[phase]
        copies[2].wait_recv()
        copies[3].wait_recv()
        late[0].wait_recv()
        late[1].wait_recv()
        accumulate(rest, me, base, 2, (rb, color, 0), (rb, color, 1))

    s_copies = []

    def small_start(phase):
        dim = REDUCE_ORDER[0][phase]
        out = []
        for by in (1, 2, 3):
            out.append(push(s_acc.at[cp], s_slots.at[phase, by - 1], s_ssem.at[phase, by - 1], s_rsem.at[phase, by - 1], chip_id(moved(me, dim, by))))
        for copy in out:
            copy.start()
        return out

    def small_finish(phase, copies):
        dim = REDUCE_ORDER[0][phase]
        for copy in copies:
            copy.wait()
        mine = me[dim]
        total = None
        own = s_acc[cp]
        got = [own] + [s_slots[phase, by] for by in range(3)]
        for coord in range(SIDE):
            gap = lax.rem(mine - coord + SIDE, SIDE)
            value = jnp.where(gap == 0, got[0], jnp.where(gap == 1, got[1], jnp.where(gap == 2, got[2], got[3])))
            total = value if total is None else total + value
        s_acc[cp] = total

    s_load.wait()
    s_swap.wait()
    s_acc[...] = s_acc[...] + s_pair[...]
    s_out_copies = small_start(0)
    started = [[] for _ in range(COLORS)]
    for by in QUARTERS:
        for color in range(COLORS):
            loads[color, by].wait()
            swaps[color, by].wait_recv()
            dim = REDUCE_ORDER[color][0]
            part = [slice(None)] * 3
            part[dim] = moved(me, dim, by)[dim]
            other = (dim + 1) % 3

            @pl.loop(0, SIDE)
            def _(v):
                part[other] = v
                at = (*part, slice(color * 2, color * 2 + 2))
                held[at] += pair[at]

            if by:
                started[color] += start_phase(color, 0, by)
    for phase in range(3):
        late = [middle(color, phase, started[color]) for color in range(COLORS)]
        nxt = []
        for color in range(COLORS):
            finish(color, phase, started[color], late[color])
            if phase < 2:
                nxt.append(start_phase(color, phase + 1))
        small_finish(phase, s_out_copies)
        if phase < 2:
            s_out_copies = small_start(phase + 1)
        started = nxt
    mine = held.at[me[0], me[1], me[2]]
    out_far = push(mine, g_out.at[pl.ds(cp * per, per)], osend.at[0], orecv.at[0], mate)
    out_far.start()
    s_far = push(s_acc.at[cp], s_out.at[cp], osend.at[1], orecv.at[1], mate)
    s_far.start()
    out_own = pltpu.make_async_copy(mine, g_out.at[pl.ds(cp * per, per)], msem.at[0])
    out_own.start()
    s_own = pltpu.make_async_copy(s_acc.at[cp], s_out.at[cp], msem.at[1])
    s_own.start()
    for copy in sends:
        copy.wait_send()
    for copy in swaps.values():
        copy.wait_send()
    y_swap.wait()
    out_own.wait()
    s_own.wait()
    out_far.wait()
    s_far.wait()


def reduce_all(g_all, small, y_oth):
    f32 = jnp.float32
    units, rows = g_all.shape[3:5]
    dma = pltpu.SemaphoreType.DMA
    vm = pltpu.VMEM
    return pl.pallas_call(
        reduce_kernel,
        out_shape=(
            jax.ShapeDtypeStruct((units, rows, 128), f32),
            jax.ShapeDtypeStruct(small.shape, f32),
            jax.ShapeDtypeStruct(y_oth.shape, y_oth.dtype),
        ),
        in_specs=[ANY] * 3,
        out_specs=(ANY,) * 3,
        scratch_shapes=[
            vm((SIDE, SIDE, SIDE, PER, rows, 128), f32),
            vm((SIDE, SIDE, SIDE, PER, rows, 128), f32),
            vm((COLORS, 2, SIDE, SIDE, 1, rows, 128), f32),
            vm((COLORS, 2, SIDE, SIDE, 2, rows, 128), f32),
            vm((COLORS, 2, SIDE, 1, rows, 128), f32),
            vm((COLORS, 2, SIDE, 2, rows, 128), f32),
            vm((COLORS, 2, 1, rows, 128), f32),
            vm((COLORS, 2, 2, rows, 128), f32),
            vm(small.shape, f32),
            vm((3, 3) + small.shape[1:], f32),
            vm(small.shape, f32),
            dma((3, 4)), dma((3, 4)), dma((3, 4)), dma((3, 3, 6)), dma((3, 3, 6)), dma((3, 3)), dma((3, 3)), dma((4,)), dma((4,)), dma((3,)),
        ],
        compiler_params=pltpu.CompilerParams(collective_id=1, has_side_effects=True, vmem_limit_bytes=62 * 1024 * 1024),
        name='reduce_grads',
    )(g_all, small, y_oth)


SEQS = 8
STEP_SEQS = 2
STEPS = SEQS // STEP_SEQS
SEQ = 256
TOK = STEP_SEQS * SEQ
TILES = 5
HEADS_PER = 4
HEAD = 32
LANES = 128
F32 = jnp.float32
BF16 = jnp.bfloat16


def mm(lhs, rhs):
    return lax.dot_general(lhs, rhs, (((1,), (0,)), ((), ())), preferred_element_type=F32)


def mm_t(lhs, rhs):
    return lax.dot_general(lhs, rhs, (((1,), (1,)), ((), ())), preferred_element_type=F32)


def fold8(value):
    return jnp.sum(value.reshape(value.shape[0] // 8, 8, value.shape[1]), axis=0)


def wide(ref, group):
    return jnp.concatenate([ref[group, j] for j in range(GROUP)], axis=1)


def flat(ref, first, count):
    return jnp.concatenate([ref[first + j] for j in range(count)], axis=1)


def add_blocks(ref, group, value):
    for j in range(GROUP):
        ref[group, j] += value[:, j * LANES:(j + 1) * LANES]


def norm_stats(value):
    mean = jnp.mean(value, axis=-1, keepdims=True)
    cent = value - mean
    var = jnp.mean(cent * cent, axis=-1, keepdims=True)
    rstd = lax.rsqrt(var + LN_EPS)
    return cent * rstd, rstd


def norm_back(d_out, gain, xhat, rstd):
    d_hat = d_out * gain
    m1 = jnp.mean(d_hat, axis=-1, keepdims=True)
    m2 = jnp.mean(d_hat * xhat, axis=-1, keepdims=True)
    return rstd * (d_hat - m1 - xhat * m2)


def gelu_pair(u):
    z = u * (0.5 ** 0.5)
    t = 1.0 / (1.0 + 0.3275911 * jnp.abs(z))
    poly = t * (0.127414796 + t * (-0.142248368 + t * (0.710706871 + t * (-0.7265760135 + t * 0.5307027145))))
    ex = jnp.exp(-z * z)
    tail = poly * ex
    cdf = jnp.where(u >= 0, 1.0 - tail, tail)
    return u * cdf, cdf + u * (ex * 0.3989422804014327)


def unturn(z, cos, sin, groups):
    parts = z.reshape(groups, 2, HEAD // 2, z.shape[1])
    lo, up = parts[:, 0], parts[:, 1]
    out = jnp.stack([lo * cos + up * sin, up * cos - lo * sin], axis=1)
    return out.reshape(z.shape)


def turn(z, cos, sin, groups):
    return unturn(z, cos, -sin, groups)


def layer_kernel(tok_ref, keep_ref, mask_ref, emb_ref, vec_ref, bqkv_ref, bup_ref, cos_ref, sin_ref, cosn_ref, sinn_ref,
                 w_hbm, g_own, g_oth,
                 y_own, y_oth, grads, dtab, dsum, dbq, dbkv, dbup,
                 w, wt, acc, gbuf, e_s, ht, qt, kt, vt, qn, kn, vn, pt, ot32, otb, x1, nm, nmt, y_s, dnm, dot_s, dqkv,
                 wsem, gsem, osem):
    step = pl.program_id(0)
    cp = lax.axis_index('cp')
    chips = SIDE ** 3

    @pl.when(step == 0)
    def _():
        own = pltpu.make_async_copy(g_own.at[pl.ds(cp * SEQS, SEQS)], gbuf.at[:, 0], gsem.at[0])
        oth = pltpu.make_async_copy(g_oth, gbuf.at[:, 1], gsem.at[1])

        @pl.loop(0, chips)
        def _(i):
            for r in range(GROUP):
                pltpu.make_async_copy(w_hbm.at[i, :, pl.ds(r * NB, NB)], w.at[:, r, pl.ds(i * NB, NB)], wsem).start()

        own.start()
        oth.start()

        @pl.loop(0, 2 * PER)
        def _(i):
            for r in range(GROUP):
                acc[i, r] = jnp.zeros((640, LANES), F32)

        dtab[...] = jnp.zeros_like(dtab)
        dsum[...] = jnp.zeros_like(dsum)
        dbq[...] = jnp.zeros_like(dbq)
        dbkv[...] = jnp.zeros_like(dbkv)
        dbup[...] = jnp.zeros_like(dbup)

        @pl.loop(0, chips)
        def _(i):
            for r in range(GROUP):
                pltpu.make_async_copy(w_hbm.at[i, :, pl.ds(r * NB, NB)], w.at[:, r, pl.ds(i * NB, NB)], wsem).wait()

        own.wait()
        oth.wait()

        @pl.loop(0, 3)
        def _(n):
            for r in range(GROUP):
                wt[n * GROUP + r] = w[n, r].T

    def grad_rows():
        return gbuf[pl.ds(step * STEP_SEQS, STEP_SEQS)].reshape(TOK, 640)

    vocab = lax.broadcasted_iota(jnp.int32, (64, TOK), 0)
    one_hot = jnp.where(vocab == tok_ref[0], 1.0, 0.0).astype(BF16)
    e_s[...] = lax.dot_general(one_hot, emb_ref[...], (((0,), (0,)), ((), ())), preferred_element_type=F32)

    @pl.loop(0, TOK // 128)
    def _(r):
        rows = pl.ds(pl.multiple_of(r * 128, 128), 128)
        keep = jnp.concatenate([keep_ref[rows]] * TILES, axis=1)
        emb = e_s[rows] * keep
        e_s[rows] = emb
        xhat, _ = norm_stats(emb)
        nm[rows] = (xhat * vec_ref[0:1] + vec_ref[1:2]).astype(BF16)

    ht[...] = nm[...].T

    cos, sin = cos_ref[...], sin_ref[...]
    for kind, (t_ref, n_ref) in enumerate(((qt, qn), (kt, kn), (vt, vn))):
        z = mm(wt[kind * TILES:(kind + 1) * TILES].reshape(640, 640), ht[...])
        bias = bqkv_ref[kind * 640:(kind + 1) * 640]
        z = z + jnp.concatenate([bias] * (TOK // LANES), axis=1)
        if kind == 0:
            z = z * HEAD ** -0.5
        if kind < 2:
            z = turn(z, cos, sin, 20)
        zb = z.astype(BF16)
        for s in range(STEP_SEQS):
            for t in range(TILES):
                piece = zb[t * LANES:(t + 1) * LANES, s * SEQ:(s + 1) * SEQ]
                t_ref[s, t] = piece
                n_ref[s, t] = piece.T

    lane_head = lax.broadcasted_iota(jnp.int32, (1, LANES), 1) // HEAD
    pick = [jnp.where(lane_head == h, 1.0, 0.0).astype(BF16) for h in range(HEADS_PER)]

    def stack(tile):
        return jnp.concatenate([tile * pick[h] for h in range(HEADS_PER)], axis=0)

    def spot(h):
        return slice((h % 2) * SEQ, (h % 2 + 1) * SEQ), (h // 2) * SEQ

    def stage(buf, value):
        for h in range(HEADS_PER):
            down, along = spot(h)
            buf[down, along:along + SEQ] = value[h * SEQ:(h + 1) * SEQ]

    @pl.loop(0, STEP_SEQS)
    def _(s):
        rows = pl.ds(pl.multiple_of(s * SEQ, SEQ), SEQ)
        bufs = (y_s, dnm)

        def scores(t):
            stage(bufs[t % 2], mm(stack(kn[s, t]), qt[s, t]))

        scores(0)
        for t in range(TILES):
            if t + 1 < TILES:
                scores(t + 1)
            bias = mask_ref[rows]
            for h in range(HEADS_PER):
                down, along = spot(h)
                for c in range(0, SEQ, LANES):
                    score = bufs[t % 2][down, along + c:along + c + LANES] + bias
                    p = jnp.exp(score - jnp.max(score, axis=0, keepdims=True))
                    p = p * (1.0 / jnp.sum(p, axis=0, keepdims=True))
                    pt[s, t * HEADS_PER + h, :, c:c + LANES] = p.astype(BF16)
            v_t = vt[s, t]
            out = jnp.concatenate([mm(v_t[h * HEAD:(h + 1) * HEAD], pt[s, t * HEADS_PER + h]) for h in range(HEADS_PER)], axis=0)
            ot32[s, t] = out
            outb = out.astype(BF16)
            otb[t, :, rows] = outb
            dqkv[t, rows] = outb.T

    w_out = wide(w, 3)
    x1[...] = e_s[...] + mm(flat(dqkv, 0, TILES), w_out) + vec_ref[5:6]

    @pl.loop(0, TOK // 128)
    def _(r):
        rows = pl.ds(pl.multiple_of(r * 128, 128), 128)
        xhat, _ = norm_stats(x1[rows])
        nm[rows] = (xhat * vec_ref[6:7] + vec_ref[7:8]).astype(BF16)

    nmt[...] = nm[...].T
    y_s[...] = jnp.zeros_like(y_s)
    dnm[...] = jnp.zeros_like(dnm)

    @pl.loop(0, 4)
    def _(c):
        g = grad_rows()
        w_up = wide(w, 4 + c)
        u = mm(nm[...], w_up) + bup_ref[c]
        a, slope = gelu_pair(u)
        ab = a.astype(BF16)
        w_down = wide(w, 8 + c)
        du = mm_t(g, w_down) * slope
        dbup[c] += fold8(du)
        dub = du.astype(BF16)
        y_s[...] += mm(ab, w_down)
        dnm[...] += mm_t(dub, w_up)
        add_blocks(acc, 8 + c, mm(ab.T, g))
        add_blocks(acc, 4 + c, mm(nmt[...], dub))

    @pl.loop(0, TOK // 128)
    def _(r):
        rows = pl.ds(pl.multiple_of(r * 128, 128), 128)
        x = x1[rows]
        out = (x + y_s[rows] + vec_ref[8:9]).astype(BF16)
        seq = r // 2

        @pl.when(lax.rem(r, 2) == 0)
        def _():
            y_own[seq] = out

        @pl.when(lax.rem(r, 2) == 1)
        def _():
            y_oth[seq] = out

        xhat, rstd = norm_stats(x)
        d_n = dnm[rows]
        g32 = gbuf[step * STEP_SEQS + seq, lax.rem(r, 2)].astype(F32)
        dsum[3] += fold8(d_n * xhat)
        dsum[4] += fold8(d_n)
        d_r = g32 + norm_back(d_n, vec_ref[6:7], xhat, rstd)
        dsum[2] += fold8(d_r)
        dsum[5] += fold8(g32)
        y_s[rows] = d_r
        nm[rows] = d_r.astype(BF16)

    d_rb = nm[...]
    add_blocks(acc, 3, mm(otb[...].reshape(640, TOK), d_rb))
    d_o = mm(wide(w, 3), d_rb.T)
    for t in range(TILES):
        dot_s[t] = d_o[t * LANES:(t + 1) * LANES]

    @pl.loop(0, STEP_SEQS)
    def _(s):
        rows = pl.ds(pl.multiple_of(s * SEQ, SEQ), SEQ)
        bufs = (x1, dnm)
        outs = (nm, nmt)

        def slopes(t):
            stage(bufs[t % 2], mm(stack(vn[s, t]), dot_s[t, :, rows].astype(BF16)))

        slopes(0)
        for t in range(TILES):
            if t + 1 < TILES:
                slopes(t + 1)
            d_ot = dot_s[t, :, rows]
            prod = d_ot * ot32[s, t]
            ds_ref = outs[t % 2]
            for h in range(HEADS_PER):
                down, along = spot(h)
                delta = jnp.sum(prod[h * HEAD:(h + 1) * HEAD], axis=0, keepdims=True)
                for c in range(0, SEQ, LANES):
                    d_p = bufs[t % 2][down, along + c:along + c + LANES]
                    p = pt[s, t * HEADS_PER + h, :, c:c + LANES].astype(F32)
                    ds_ref[down, along + c:along + c + LANES] = (p * (d_p - delta[:, c:c + LANES])).astype(BF16)
            k_t, q_n = kt[s, t], qn[s, t]
            dqs = []
            for h in range(HEADS_PER):
                down, along = spot(h)
                dqs.append(mm(k_t[h * HEAD:(h + 1) * HEAD], ds_ref[down, along:along + SEQ]))
            dq = unturn(jnp.concatenate(dqs, axis=0), cos[:, :SEQ], sin[:, :SEQ], HEADS_PER) * HEAD ** -0.5
            dbq[t] += dq[:, :LANES] + dq[:, LANES:]
            dqkv[t, rows] = dq.astype(BF16).T
            dk = mm(ds_ref[:SEQ, :2 * SEQ], jnp.concatenate([q_n * pick[0], q_n * pick[2]], axis=0))
            dk = dk + mm(ds_ref[SEQ:2 * SEQ, :2 * SEQ], jnp.concatenate([q_n * pick[1], q_n * pick[3]], axis=0))
            p_wide = jnp.concatenate([pt[s, t * HEADS_PER + h] for h in range(HEADS_PER)], axis=1)
            dv = mm(p_wide, stack(d_ot.astype(BF16).T))
            low = lax.rem(lax.broadcasted_iota(jnp.int32, (SEQ, LANES), 1), HEAD) < HEAD // 2
            other = jnp.where(low, pltpu.roll(dk, LANES - HEAD // 2, 1), pltpu.roll(dk, HEAD // 2, 1))
            dk = dk * cosn_ref[...] + other * sinn_ref[...]
            dbkv[0, t] += fold8(dk)
            dbkv[1, t] += fold8(dv)
            dqkv[TILES + t, rows] = dk.astype(BF16)
            dqkv[2 * TILES + t, rows] = dv.astype(BF16)

    for kind in range(3):
        add_blocks(acc, kind, mm(ht[...], flat(dqkv, kind * TILES, TILES)))
    dnm[...] = mm(flat(dqkv, 0, 15), wt[...].reshape(1920, 640))

    @pl.loop(0, TOK // 128)
    def _(r):
        rows = pl.ds(pl.multiple_of(r * 128, 128), 128)
        xhat, rstd = norm_stats(e_s[rows])
        d_n = dnm[rows]
        dsum[0] += fold8(d_n * xhat)
        dsum[1] += fold8(d_n)
        keep = jnp.concatenate([keep_ref[rows]] * TILES, axis=1)
        nm[rows] = ((norm_back(d_n, vec_ref[0:1], xhat, rstd) + y_s[rows]) * keep).astype(BF16)

    dtab[...] += mm(one_hot, nm[...])

    @pl.when(step == STEPS - 1)
    def _():
        @pl.loop(0, chips)
        def _(i):
            for r in range(GROUP):
                pltpu.make_async_copy(acc.at[:, r, pl.ds(i * NB, NB)], grads.at[i, :, pl.ds(r * NB, NB)], osem).start()

        @pl.loop(0, chips)
        def _(i):
            for r in range(GROUP):
                pltpu.make_async_copy(acc.at[:, r, pl.ds(i * NB, NB)], grads.at[i, :, pl.ds(r * NB, NB)], osem).wait()


def layer_call(tok, keep, mask, emb, vecs, bqkv, bup, cos, sin, cosn, sinn, w_hbm, g_own, g_oth):
    vm = pltpu.VMEM
    dma = pltpu.SemaphoreType.DMA

    def whole(shape):
        return pl.BlockSpec(shape, lambda i: (0,) * len(shape))

    pair = pl.BlockSpec((STEP_SEQS, 128, 640), lambda i: (i, 0, 0))
    out_shape = (
        jax.ShapeDtypeStruct((SEQS, 128, 640), BF16),
        jax.ShapeDtypeStruct((SEQS, 128, 640), BF16),
        jax.ShapeDtypeStruct((64, 2 * PER, GROUP * NB, LANES), F32),
        jax.ShapeDtypeStruct((64, 640), F32),
        jax.ShapeDtypeStruct((6, 8, 640), F32),
        jax.ShapeDtypeStruct((TILES, LANES, LANES), F32),
        jax.ShapeDtypeStruct((2, TILES, 8, LANES), F32),
        jax.ShapeDtypeStruct((4, 8, 640), F32),
    )
    out_specs = (pair, pair, ANY) + tuple(whole(o.shape) for o in out_shape[3:])
    in_specs = [
        pl.BlockSpec((1, 1, TOK), lambda i: (i, 0, 0)),
        pl.BlockSpec((TOK, LANES), lambda i: (i, 0)),
        pl.BlockSpec((TOK, LANES), lambda i: (i, 0)),
    ] + [whole(a.shape) for a in (emb, vecs, bqkv, bup, cos, sin, cosn, sinn)] + [ANY] * 3
    halves = (STEP_SEQS, TILES, LANES, SEQ)
    flipped = (STEP_SEQS, TILES, SEQ, LANES)
    scratch = [
        vm((2 * PER, GROUP, 640, LANES), BF16), vm((15, LANES, 640), BF16), vm((2 * PER, GROUP, 640, LANES), F32), vm((SEQS, 2, 128, 640), BF16),
        vm((TOK, 640), F32), vm((640, TOK), BF16),
        vm(halves, BF16), vm(halves, BF16), vm(halves, BF16), vm(flipped, BF16), vm(flipped, BF16), vm(flipped, BF16),
        vm((STEP_SEQS, 20, SEQ, SEQ), BF16), vm(halves, F32), vm((TILES, LANES, TOK), BF16),
        vm((TOK, 640), F32), vm((TOK, 640), BF16), vm((640, TOK), BF16), vm((TOK, 640), F32), vm((TOK, 640), F32),
        vm((TILES, LANES, TOK), F32), vm((15, TOK, LANES), BF16),
        dma, dma((2,)), dma,
    ]
    return pl.pallas_call(
        layer_kernel,
        grid=(STEPS,),
        out_shape=out_shape,
        in_specs=in_specs,
        out_specs=out_specs,
        scratch_shapes=scratch,
        compiler_params=pltpu.CompilerParams(dimension_semantics=('arbitrary',), vmem_limit_bytes=67043328),
        name='layer',
    )(tok, keep, mask, emb, vecs, bqkv, bup, cos, sin, cosn, sinn, w_hbm, g_own, g_oth)


def prepare(tokens, lengths, positions, embed_table, vecs_all):
    n_seq, seq_len = tokens.shape
    is_mask = tokens == MASK_ID
    tok_valid = positions[None, :] < lengths[:, None]
    mask_count = jnp.sum(is_mask.astype(jnp.int32), axis=1)
    drop_scale = (1.0 - TRAIN_RATIO) / (1.0 - mask_count.astype(F32) / lengths.astype(F32))
    keep = jnp.where(is_mask | jnp.logical_not(tok_valid), 0.0, drop_scale[:, None])
    keep = jnp.broadcast_to(keep.reshape(-1, 1), (n_seq * seq_len, LANES))
    mask = jnp.broadcast_to(jnp.where(tok_valid, 0.0, NEG_BIG).reshape(-1, 1), (n_seq * seq_len, LANES)).astype(F32)
    emb = jnp.pad(embed_table, ((0, 64 - embed_table.shape[0]), (0, 0)))
    bqkv = jnp.broadcast_to(vecs_all[2:5].reshape(-1, 1), (1920, LANES))
    inv_freq = 1.0 / (ROPE_BASE ** (jnp.arange(0, HEAD, 2, dtype=F32) / HEAD))
    angles = positions.astype(F32)[:, None] * inv_freq[None, :]
    cos, sin = jnp.cos(angles), jnp.sin(angles)
    cos_t, sin_t = jnp.tile(cos.T, (1, STEP_SEQS)), jnp.tile(sin.T, (1, STEP_SEQS))
    cos_n = jnp.tile(cos, (1, 8))
    sin_n = jnp.tile(jnp.concatenate([sin, -sin], axis=1), (1, 4))
    return tokens.reshape(STEPS, 1, TOK), keep, mask, emb, bqkv, cos_t, sin_t, cos_n, sin_n


def solution(mesh):
    chips = mesh.shape['fsdp']

    def local_step(tokens, lengths, embed_table, layer_vecs, w_qkv, w_out, w_up, b_up, w_down, grad_out):
        f32 = jnp.float32
        cp = lax.axis_index('cp')
        chip = lax.axis_index('fsdp')
        n_seq, seq_loc = tokens.shape
        half = n_seq // 2
        rows = w_qkv.shape[0]
        vocab, width = embed_table.shape
        w_loc = jnp.concatenate([
            w_qkv.reshape(rows, 15, 128).transpose(1, 0, 2),
            w_out.reshape(rows, 5, 128).transpose(1, 0, 2),
            w_up.reshape(rows, chips, 4, NB).transpose(2, 1, 3, 0).reshape(20, 128, rows).transpose(0, 2, 1),
            w_down.reshape(4, NB, 5, 128).transpose(0, 2, 1, 3).reshape(20, NB, 128),
        ], axis=0)
        s_loc = jnp.pad(jnp.concatenate([layer_vecs.reshape(-1), b_up]), (0, 1024 - 130)).reshape(8, 128)
        w_all, s_all, g_oth, t_oth = gather_all(w_loc.reshape(2 * PER, GROUP * NB, 128), s_loc, grad_out, tokens)
        s_flat = s_all.reshape(chips, 1024)
        vecs_all = s_flat[:, :90].reshape(chips, 9, NB).transpose(1, 0, 2).reshape(9, width)
        up_b = s_flat[:, 90:130].reshape(chips, 4, NB).transpose(1, 0, 2).reshape(-1)
        start = half * cp
        tok_full = jnp.concatenate([lax.dynamic_slice_in_dim(tokens, start, half, 0), t_oth], axis=1)
        len_own = lax.dynamic_slice_in_dim(lengths, start, half, 0)
        positions = jnp.concatenate([cp * seq_loc + jnp.arange(seq_loc), (1 - cp) * seq_loc + jnp.arange(seq_loc)])
        tok, keep, mask, emb, bqkv, cos, sin, cosn, sinn = prepare(tok_full, len_own, positions, embed_table, vecs_all)
        y_own, y_oth, g_all, dtab, dsum, dbq, dbkv, dbup = layer_call(
            tok, keep, mask, emb, vecs_all, bqkv, up_b.reshape(4, 1, 640), cos, sin, cosn, sinn, w_all.reshape(chips, 2 * PER, GROUP * NB, 128), grad_out, g_oth)
        rowsum = jnp.sum(dsum, axis=1)
        d_bq = jnp.sum(dbq, axis=2).reshape(1, width)
        d_bkv = jnp.sum(dbkv, axis=2).reshape(2, width)
        small = jnp.concatenate([dtab[:vocab].reshape(-1), rowsum[:2].reshape(-1), d_bq.reshape(-1), d_bkv.reshape(-1), rowsum[2:].reshape(-1), jnp.sum(dbup, axis=1).reshape(-1)])
        small = jnp.pad(small, (0, 2 * SMALL_ROWS * 128 - small.shape[0])).reshape(2, SMALL_ROWS, 128)
        g_red, s_red, y_recv = reduce_all(g_all.reshape(SIDE, SIDE, SIDE, 2 * PER, GROUP * NB, 128), small, y_oth)
        g_red = g_red.reshape(60, NB, 128)
        out_full = jnp.where(cp == 0, jnp.concatenate([y_own, y_recv], axis=0), jnp.concatenate([y_recv, y_own], axis=0))
        s_flat = s_red.reshape(-1)
        n_tab = vocab * width
        d_embed = s_flat[:n_tab].reshape(vocab, width)
        d_v = lax.dynamic_slice(s_flat[n_tab:n_tab + 9 * width].reshape(9, width), (0, chip * NB), (9, NB))
        d_b = s_flat[n_tab + 9 * width:n_tab + 9 * width + 2560].reshape(4, chips, NB)
        d_b = lax.dynamic_slice(d_b, (0, chip, 0), (4, 1, NB)).reshape(-1)
        d_qkv = g_red[:15].transpose(1, 0, 2).reshape(w_qkv.shape)
        d_wout = g_red[15:20].transpose(1, 0, 2).reshape(w_out.shape)
        d_wup = g_red[20:40].transpose(0, 2, 1).reshape(4, chips, NB, rows).transpose(3, 1, 0, 2).reshape(w_up.shape)
        d_wdown = g_red[40:60].reshape(4, 5, NB, 128).transpose(0, 2, 1, 3).reshape(w_down.shape)
        return out_full, d_embed, d_v, d_qkv, d_wout, d_wup, d_b, d_wdown

    in_specs = (P('fsdp', 'cp'), P('fsdp'), P(), P(None, 'fsdp'), P('fsdp', None, None, None), P('fsdp', None), P('fsdp', None), P('fsdp'), P('fsdp', None), P('fsdp', 'cp', None))
    out_specs = (P('fsdp', 'cp', None), P(), P(None, 'fsdp'), P('fsdp', None, None, None), P('fsdp', None), P('fsdp', None), P('fsdp'), P('fsdp', None))
    return jax.shard_map(local_step, mesh=mesh, in_specs=in_specs, out_specs=out_specs, check_vma=False)
```

```python
import functools

import jax
import jax.numpy as jnp
import numpy as np
from jax import lax
from jax.experimental import pallas as pl
from jax.experimental.pallas import tpu as pltpu
from jax.sharding import PartitionSpec as P

MASK_ID = 32
LN_EPS = 1e-5
ROPE_BASE = 10000.0
TRAIN_RATIO = 0.15 * 0.8
NEG_BIG = -1e30
SIDE = 4
COLORS = 3
NB = 10
GROUP = 5
PER = 6
SMALL_ROWS = 120
QUARTERS = (2, 1, 3, 0)
MESH_ID = pl.DeviceIdType.MESH
ANY = pl.BlockSpec(memory_space=pl.ANY)

GATHER_ORDER = ((2, 1, 0), (1, 0, 2), (0, 2, 1))
REDUCE_ORDER = ((0, 1, 2), (1, 2, 0), (2, 0, 1))


def my_coords():
    chip = lax.axis_index('fsdp')
    return [chip // 16, lax.rem(chip // 4, 4), lax.rem(chip, 4)]


def moved(coords, dim, by):
    out = list(coords)
    out[dim] = lax.rem(coords[dim] + by + SIDE, SIDE)
    return out


def chip_id(coords):
    return {'fsdp': coords[0] * 16 + coords[1] * 4 + coords[2]}


def entry_barrier(coords, cp):
    barrier = pltpu.get_barrier_semaphore()
    for dim in range(3):
        for by in (1, 2, 3):
            pl.semaphore_signal(barrier, inc=1, device_id=chip_id(moved(coords, dim, by)), device_id_type=MESH_ID)
    pl.semaphore_signal(barrier, inc=1, device_id={'cp': 1 - cp}, device_id_type=MESH_ID)
    pl.semaphore_wait(barrier, 10)


def push(src, dst, send_sem, recv_sem, target):
    return pltpu.make_async_remote_copy(src_ref=src, dst_ref=dst, send_sem=send_sem, recv_sem=recv_sem, device_id=target, device_id_type=MESH_ID)


def gather_kernel(w_loc, s_loc, g_own, t_own, w_out, s_out, g_oth, t_oth, w_all, s_all, ssem, rsem, fsend, frecv, s_ssem, s_rsem, psend, precv, lsem, osem, xsem):
    cp = lax.axis_index('cp')
    me = my_coords()
    mate = {'cp': 1 - cp}
    own_w = pltpu.make_async_copy(w_loc, w_all.at[me[0], me[1], me[2]], lsem.at[0])
    own_s = pltpu.make_async_copy(s_loc, s_all.at[me[0], me[1], me[2]], lsem.at[1])
    own_w.start()
    own_s.start()
    entry_barrier(me, cp)
    swap_g = push(g_own.at[pl.ds(8 * (1 - cp), 8)], g_oth, psend.at[0], precv.at[0], mate)
    swap_t = push(t_own.at[pl.ds(8 * (1 - cp), 8)], t_oth, psend.at[1], precv.at[1], mate)
    swap_t.start()

    def region(ref, first, count, dims, at):
        index = [slice(None) if d in dims else at[d] for d in range(3)]
        return ref.at[(*index, pl.ds(first, count))]

    def small_region(dims, at):
        index = [slice(None) if d in dims else at[d] for d in range(3)]
        return s_all.at[tuple(index)]

    forwards = []
    pending = []
    stores = []
    arrivals = {}

    def store(first, count, dims, at, sem):
        index = [slice(None) if d in dims else at[d] for d in range(3)]
        index = (*index, pl.ds(first, count))
        copy = pltpu.make_async_copy(w_all.at[index], w_out.at[index], sem)
        copy.start()
        stores.append(copy)

    own_s.wait()
    own_w.wait()
    store(0, 2 * PER, (), me, lsem.at[2])
    for phase in range(3):
        firsts = {}
        for color in range(COLORS):
            dim = GATHER_ORDER[color][phase]
            done = GATHER_ORDER[color][:phase]
            base = cp * PER + color * 2
            mine = region(w_all, base, 2, done, me)
            right, left = chip_id(moved(me, dim, 1)), chip_id(moved(me, dim, 3))
            to_right = push(mine, mine, ssem.at[color, phase, 0], rsem.at[color, phase, 0], right)
            to_left = push(mine, mine, ssem.at[color, phase, 1], rsem.at[color, phase, 1], left)
            to_right.start()
            to_left.start()
            firsts[color] = (to_right, to_left)
            pending += [to_right, to_left]
            if color == 0:
                s_mine = small_region(done, me)
                s_right = push(s_mine, s_mine, s_ssem.at[phase, 0], s_rsem.at[phase, 0], right)
                s_left = push(s_mine, s_mine, s_ssem.at[phase, 1], s_rsem.at[phase, 1], left)
                s_right.start()
                s_left.start()
                pending += [s_right, s_left]
        seconds = {}
        for color in range(COLORS):
            dim = GATHER_ORDER[color][phase]
            done = GATHER_ORDER[color][:phase]
            base = cp * PER + color * 2
            right, left = chip_id(moved(me, dim, 1)), chip_id(moved(me, dim, 3))
            from_left, from_right = moved(me, dim, 3), moved(me, dim, 1)
            to_right, to_left = firsts[color]
            to_right.wait_recv()
            part = region(w_all, base, 1, done, from_left)
            on_right = push(part, part, ssem.at[color, phase, 2], rsem.at[color, phase, 2], right)
            on_right.start()
            whole_l = region(w_all, base, 2, done, from_left)
            fwd_l = push(whole_l, whole_l, fsend.at[color, phase, 0], frecv.at[color, phase, 0], mate)
            fwd_l.start()
            store(base, 2, done, from_left, osem.at[color, phase, 0])
            to_left.wait_recv()
            part = region(w_all, base + 1, 1, done, from_right)
            on_left = push(part, part, ssem.at[color, phase, 3], rsem.at[color, phase, 3], left)
            on_left.start()
            whole_r = region(w_all, base, 2, done, from_right)
            fwd_r = push(whole_r, whole_r, fsend.at[color, phase, 1], frecv.at[color, phase, 1], mate)
            fwd_r.start()
            store(base, 2, done, from_right, osem.at[color, phase, 1])
            seconds[color] = (on_right, on_left)
            pending += [on_right, on_left]
            forwards += [fwd_l, fwd_r]
            arrivals[color, phase] = [(fwd_l, done, from_left, 0), (fwd_r, done, from_right, 1)]
            if color == 0:
                s_right.wait_recv()
                s_left.wait_recv()
                s_part = small_region(done, from_left)
                s_on = push(s_part, s_part, s_ssem.at[phase, 2], s_rsem.at[phase, 2], right)
                s_on.start()
                pending.append(s_on)
        for color in range(COLORS):
            dim = GATHER_ORDER[color][phase]
            done = GATHER_ORDER[color][:phase]
            base = cp * PER + color * 2
            on_right, on_left = seconds[color]
            on_right.wait_recv()
            on_left.wait_recv()
            far = region(w_all, base, 2, done, moved(me, dim, 2))
            fwd_f = push(far, far, fsend.at[color, phase, 2], frecv.at[color, phase, 2], mate)
            fwd_f.start()
            store(base, 2, done, moved(me, dim, 2), osem.at[color, phase, 2])
            forwards.append(fwd_f)
            arrivals[color, phase].append((fwd_f, done, moved(me, dim, 2), 2))
            if color == 0:
                s_on.wait_recv()
        if phase == 0:
            swap_g.start()
    s_store = pltpu.make_async_copy(s_all, s_out, lsem.at[3])
    s_store.start()
    for phase in range(3):
        for color in range(COLORS):
            for copy, done, at, slot in arrivals[color, phase]:
                copy.wait_recv()
                store((1 - cp) * PER + color * 2, 2, done, at, xsem.at[color, phase, slot])
    s_store.wait()
    for copy in stores:
        copy.wait()
    swap_g.wait()
    swap_t.wait()
    for copy in pending + forwards:
        copy.wait_send()


def gather_all(w_loc, s_loc, grad_out, tokens):
    bf16, f32 = jnp.bfloat16, jnp.float32
    seqs, pos, width = grad_out.shape
    dma = pltpu.SemaphoreType.DMA
    return pl.pallas_call(
        gather_kernel,
        out_shape=(
            jax.ShapeDtypeStruct((SIDE, SIDE, SIDE, *w_loc.shape), bf16),
            jax.ShapeDtypeStruct((SIDE, SIDE, SIDE, 8, 128), f32),
            jax.ShapeDtypeStruct((seqs // 2, pos, width), bf16),
            jax.ShapeDtypeStruct((seqs // 2, pos), jnp.int32),
        ),
        in_specs=[ANY] * 4,
        out_specs=(ANY,) * 4,
        scratch_shapes=[
            pltpu.VMEM((SIDE, SIDE, SIDE, *w_loc.shape), bf16), pltpu.VMEM((SIDE, SIDE, SIDE, 8, 128), f32),
            dma((3, 3, 4)), dma((3, 3, 4)), dma((3, 3, 3)), dma((3, 3, 3)), dma((3, 3)), dma((3, 3)), dma((2,)), dma((2,)), dma((4,)), dma((3, 3, 3)), dma((3, 3, 3)),
        ],
        compiler_params=pltpu.CompilerParams(collective_id=0, has_side_effects=True, vmem_limit_bytes=40 * 1024 * 1024),
        name='gather_weights',
    )(w_loc, s_loc, grad_out, tokens)


def reduce_kernel(g_all, small, y_own, y_oth, g_out, s_out, y_full, y_hold, held, pair, ra0, rb0, ra1, rb1, ra2, rb2, s_pair, s_slots, s_acc,
                  lsem, psend, precv, ssem, rsem, s_ssem, s_rsem, osend, orecv, msem):
    cp = lax.axis_index('cp')
    me = my_coords()
    mate = {'cp': 1 - cp}
    per = PER
    loads = {}

    def quarter(ref, first, color, by):
        dim = REDUCE_ORDER[color][0]
        index = [slice(None)] * 3
        index[dim] = moved(me, dim, by)[dim]
        return ref.at[(*index, pl.ds(first + color * 2, 2))]

    for by in QUARTERS:
        for color in range(COLORS):
            load = pltpu.make_async_copy(quarter(g_all, cp * per, color, by), quarter(held, 0, color, by), lsem.at[color, by])
            load.start()
            loads[color, by] = load
    s_load = pltpu.make_async_copy(small, s_acc, msem.at[2])
    s_load.start()
    entry_barrier(me, cp)
    sends = []
    s_swap = push(small, s_pair, osend.at[2], orecv.at[2], mate)
    s_swap.start()
    swaps = {}
    for by in QUARTERS:
        for color in range(COLORS):
            swap = push(quarter(g_all, (1 - cp) * per, color, by), quarter(pair, 0, color, by), psend.at[color, by], precv.at[color, by], mate)
            swap.start()
            swaps[color, by] = swap
    y_rows = y_full.at[pl.ds(y_own.shape[0] * cp, y_own.shape[0])]
    y_swap = push(y_oth, y_rows, osend.at[3], orecv.at[3], mate)
    y_swap.start()
    y_in = pltpu.make_async_copy(y_own, y_hold, msem.at[3])
    y_in.start()

    bufs = ((ra0, rb0), (ra1, rb1), (ra2, rb2))

    def index_of(dims, at):
        return [slice(None) if d in dims else at[d] for d in range(3)]

    def region(first, count, dims, at):
        return held.at[(*index_of(dims, at), pl.ds(first, count))]

    def side(rb, color, way, rest, half):
        return rb.at[(color, way, *[slice(None)] * len(rest), pl.ds(half, 1))]

    def accumulate(rest, at, first, count, *sources):
        where = index_of(rest, at)
        units = slice(first, first + count)

        def add(lead):
            total = held[(*where, units)]
            for ref, color, way in sources:
                total = total + ref[(color, way, *lead)]
            held[(*where, units)] = total

        if rest:
            dim = min(rest)

            @pl.loop(0, SIDE)
            def _(v):
                where[dim] = v
                add((v,))
        else:
            add(())

    def start_phase(color, phase, part=None):
        dim = REDUCE_ORDER[color][phase]
        rest = REDUCE_ORDER[color][phase + 1:]
        base = color * 2
        ra, rb = bufs[phase]
        right, left = moved(me, dim, 1), moved(me, dim, 3)
        far = moved(me, dim, 2)
        out = [
            push(region(base, 1, rest, far), ra.at[color, 0], ssem.at[color, phase, 0], rsem.at[color, phase, 0], chip_id(right)),
            push(region(base + 1, 1, rest, far), ra.at[color, 1], ssem.at[color, phase, 1], rsem.at[color, phase, 1], chip_id(left)),
            push(region(base + 1, 1, rest, right), side(rb, color, 0, rest, 1), ssem.at[color, phase, 2], rsem.at[color, phase, 2], chip_id(right)),
            push(region(base, 1, rest, left), side(rb, color, 1, rest, 0), ssem.at[color, phase, 3], rsem.at[color, phase, 3], chip_id(left)),
        ]
        if part is not None:
            out = {2: out[:2], 1: out[2:3], 3: out[3:]}[part]
        for copy in out:
            copy.start()
        sends.extend(out)
        return out

    def middle(color, phase, copies):
        dim = REDUCE_ORDER[color][phase]
        rest = REDUCE_ORDER[color][phase + 1:]
        base = color * 2
        ra, rb = bufs[phase]
        right, left = moved(me, dim, 1), moved(me, dim, 3)
        copies[0].wait_recv()
        accumulate(rest, right, base, 1, (ra, color, 0))

        fwd_r = push(region(base, 1, rest, right), side(rb, color, 0, rest, 0), ssem.at[color, phase, 4], rsem.at[color, phase, 4], chip_id(right))
        fwd_r.start()
        copies[1].wait_recv()
        accumulate(rest, left, base + 1, 1, (ra, color, 1))

        fwd_l = push(region(base + 1, 1, rest, left), side(rb, color, 1, rest, 1), ssem.at[color, phase, 5], rsem.at[color, phase, 5], chip_id(left))
        fwd_l.start()
        sends.extend([fwd_r, fwd_l])
        return [fwd_r, fwd_l]

    def finish(color, phase, copies, late):
        rest = REDUCE_ORDER[color][phase + 1:]
        base = color * 2
        ra, rb = bufs[phase]
        copies[2].wait_recv()
        copies[3].wait_recv()
        late[0].wait_recv()
        late[1].wait_recv()
        accumulate(rest, me, base, 2, (rb, color, 0), (rb, color, 1))

    s_copies = []

    def small_start(phase):
        dim = REDUCE_ORDER[0][phase]
        out = []
        for by in (1, 2, 3):
            out.append(push(s_acc.at[cp], s_slots.at[phase, by - 1], s_ssem.at[phase, by - 1], s_rsem.at[phase, by - 1], chip_id(moved(me, dim, by))))
        for copy in out:
            copy.start()
        return out

    def small_finish(phase, copies):
        dim = REDUCE_ORDER[0][phase]
        for copy in copies:
            copy.wait()
        mine = me[dim]
        total = None
        own = s_acc[cp]
        got = [own] + [s_slots[phase, by] for by in range(3)]
        for coord in range(SIDE):
            gap = lax.rem(mine - coord + SIDE, SIDE)
            value = jnp.where(gap == 0, got[0], jnp.where(gap == 1, got[1], jnp.where(gap == 2, got[2], got[3])))
            total = value if total is None else total + value
        s_acc[cp] = total

    y_in.wait()
    y_put = pltpu.make_async_copy(y_hold, y_rows, msem.at[4])
    y_put.start()
    s_load.wait()
    s_swap.wait()
    s_acc[...] = s_acc[...] + s_pair[...]
    s_out_copies = small_start(0)
    started = [[] for _ in range(COLORS)]
    for by in QUARTERS:
        for color in range(COLORS):
            loads[color, by].wait()
            swaps[color, by].wait_recv()
            dim = REDUCE_ORDER[color][0]
            part = [slice(None)] * 3
            part[dim] = moved(me, dim, by)[dim]
            other = (dim + 1) % 3

            @pl.loop(0, SIDE)
            def _(v):
                part[other] = v
                at = (*part, slice(color * 2, color * 2 + 2))
                held[at] += pair[at]

            if by:
                started[color] += start_phase(color, 0, by)
    for phase in range(3):
        late = [middle(color, phase, started[color]) for color in range(COLORS)]
        nxt = []
        for color in range(COLORS):
            finish(color, phase, started[color], late[color])
            if phase < 2:
                nxt.append(start_phase(color, phase + 1))
        small_finish(phase, s_out_copies)
        if phase < 2:
            s_out_copies = small_start(phase + 1)
        started = nxt
    mine = held.at[me[0], me[1], me[2]]
    out_far = push(mine, g_out.at[pl.ds(cp * per, per)], osend.at[0], orecv.at[0], mate)
    out_far.start()
    s_far = push(s_acc.at[cp], s_out.at[cp], osend.at[1], orecv.at[1], mate)
    s_far.start()
    out_own = pltpu.make_async_copy(mine, g_out.at[pl.ds(cp * per, per)], msem.at[0])
    out_own.start()
    s_own = pltpu.make_async_copy(s_acc.at[cp], s_out.at[cp], msem.at[1])
    s_own.start()
    for copy in sends:
        copy.wait_send()
    for copy in swaps.values():
        copy.wait_send()
    y_swap.wait()
    y_put.wait()
    out_own.wait()
    s_own.wait()
    out_far.wait()
    s_far.wait()


def reduce_all(g_all, small, y_own, y_oth):
    f32 = jnp.float32
    units, rows = g_all.shape[3:5]
    dma = pltpu.SemaphoreType.DMA
    vm = pltpu.VMEM
    return pl.pallas_call(
        reduce_kernel,
        out_shape=(
            jax.ShapeDtypeStruct((units, rows, 128), f32),
            jax.ShapeDtypeStruct(small.shape, f32),
            jax.ShapeDtypeStruct((2 * y_oth.shape[0], *y_oth.shape[1:]), y_oth.dtype),
        ),
        in_specs=[ANY] * 4,
        out_specs=(ANY,) * 3,
        scratch_shapes=[
            vm(y_own.shape, y_own.dtype),
            vm((SIDE, SIDE, SIDE, PER, rows, 128), f32),
            vm((SIDE, SIDE, SIDE, PER, rows, 128), f32),
            vm((COLORS, 2, SIDE, SIDE, 1, rows, 128), f32),
            vm((COLORS, 2, SIDE, SIDE, 2, rows, 128), f32),
            vm((COLORS, 2, SIDE, 1, rows, 128), f32),
            vm((COLORS, 2, SIDE, 2, rows, 128), f32),
            vm((COLORS, 2, 1, rows, 128), f32),
            vm((COLORS, 2, 2, rows, 128), f32),
            vm(small.shape, f32),
            vm((3, 3) + small.shape[1:], f32),
            vm(small.shape, f32),
            dma((3, 4)), dma((3, 4)), dma((3, 4)), dma((3, 3, 6)), dma((3, 3, 6)), dma((3, 3)), dma((3, 3)), dma((4,)), dma((4,)), dma((5,)),
        ],
        compiler_params=pltpu.CompilerParams(collective_id=1, has_side_effects=True, vmem_limit_bytes=62 * 1024 * 1024),
        name='reduce_grads',
    )(g_all, small, y_own, y_oth)


SEQS = 8
STEP_SEQS = 2
STEPS = SEQS // STEP_SEQS
SEQ = 256
TOK = STEP_SEQS * SEQ
TILES = 5
HEADS_PER = 4
HEAD = 32
LANES = 128
F32 = jnp.float32
BF16 = jnp.bfloat16


def mm(lhs, rhs):
    return lax.dot_general(lhs, rhs, (((1,), (0,)), ((), ())), preferred_element_type=F32)


def mm_t(lhs, rhs):
    return lax.dot_general(lhs, rhs, (((1,), (1,)), ((), ())), preferred_element_type=F32)


def fold8(value):
    return jnp.sum(value.reshape(value.shape[0] // 8, 8, value.shape[1]), axis=0)


def wide(ref, group):
    return jnp.concatenate([ref[group, j] for j in range(GROUP)], axis=1)


def flat(ref, first, count):
    return jnp.concatenate([ref[first + j] for j in range(count)], axis=1)


def add_blocks(ref, group, value):
    for j in range(GROUP):
        ref[group, j] += value[:, j * LANES:(j + 1) * LANES]


def norm_stats(value):
    mean = jnp.mean(value, axis=-1, keepdims=True)
    cent = value - mean
    var = jnp.mean(cent * cent, axis=-1, keepdims=True)
    rstd = lax.rsqrt(var + LN_EPS)
    return cent * rstd, rstd


def norm_back(d_out, gain, xhat, rstd):
    d_hat = d_out * gain
    m1 = jnp.mean(d_hat, axis=-1, keepdims=True)
    m2 = jnp.mean(d_hat * xhat, axis=-1, keepdims=True)
    return rstd * (d_hat - m1 - xhat * m2)


def gelu_pair(u):
    z = u * (0.5 ** 0.5)
    t = 1.0 / (1.0 + 0.3275911 * jnp.abs(z))
    poly = t * (0.127414796 + t * (-0.142248368 + t * (0.710706871 + t * (-0.7265760135 + t * 0.5307027145))))
    ex = jnp.exp(-z * z)
    tail = poly * ex
    cdf = jnp.where(u >= 0, 1.0 - tail, tail)
    return u * cdf, cdf + u * (ex * 0.3989422804014327)


def unturn(z, cos, sin, groups):
    parts = z.reshape(groups, 2, HEAD // 2, z.shape[1])
    lo, up = parts[:, 0], parts[:, 1]
    out = jnp.stack([lo * cos + up * sin, up * cos - lo * sin], axis=1)
    return out.reshape(z.shape)


def turn(z, cos, sin, groups):
    return unturn(z, cos, -sin, groups)


def layer_kernel(tok_ref, keep_in, mask_in, emb_ref, vec_ref, bup_ref, cos_ref, sin_ref, cosn_ref, sinn_ref,
                 w_hbm, g_own, g_oth,
                 y_own, y_oth, grads, dtab, dsum, dbq, dbkv, dbup,
                 w, wt, acc, gbuf, e_s, ht, qt, kt, vt, qn, kn, vn, pt, ot32, otb, x1, nm, nmt, y_s, dnm, dot_s, dqkv, keep_ref, mask_ref, bqkv_ref,
                 wsem, gsem, osem):
    step = pl.program_id(0)
    cp = lax.axis_index('cp')
    chips = SIDE ** 3

    def weights(act, first, count):
        @pl.loop(0, chips)
        def _(i):
            for r in range(GROUP):
                src = w_hbm.at[i, pl.ds(first, count), pl.ds(r * NB, NB)]
                dst = w.at[pl.ds(first, count), r, pl.ds(i * NB, NB)]
                getattr(pltpu.make_async_copy(src, dst, wsem.at[first // 4]), act)()

    def ship(act, first, count):
        @pl.loop(0, chips)
        def _(i):
            for r in range(GROUP):
                src = acc.at[pl.ds(first, count), r, pl.ds(i * NB, NB)]
                dst = grads.at[i, pl.ds(first, count), pl.ds(r * NB, NB)]
                getattr(pltpu.make_async_copy(src, dst, osem.at[first // 4]), act)()

    def grad_loads():
        own = pltpu.make_async_copy(g_own.at[pl.ds(cp * SEQS, SEQS)], gbuf.at[:, 0], gsem.at[0])
        oth = pltpu.make_async_copy(g_oth, gbuf.at[:, 1], gsem.at[1])
        return own, oth

    keep_ref[...] = jnp.broadcast_to(keep_in[0], (LANES, TOK)).T
    mask_ref[...] = jnp.broadcast_to(mask_in[0], (LANES, TOK)).T

    @pl.when(step == 0)
    def _():
        own, oth = grad_loads()
        weights('start', 0, 4)
        weights('start', 4, 8)

        own.start()
        oth.start()

        @pl.loop(0, 2 * PER)
        def _(i):
            for r in range(GROUP):
                acc[i, r] = jnp.zeros((640, LANES), F32)

        dtab[...] = jnp.zeros_like(dtab)
        dsum[...] = jnp.zeros_like(dsum)
        dbq[...] = jnp.zeros_like(dbq)
        dbkv[...] = jnp.zeros_like(dbkv)
        dbup[...] = jnp.zeros_like(dbup)

        for kind in range(3):
            for t in range(TILES):
                first = (kind * TILES + t) * LANES
                row = vec_ref[2 + kind:3 + kind, t * LANES:(t + 1) * LANES]
                bqkv_ref[first:first + LANES] = jnp.broadcast_to(row, (LANES, LANES)).T

        weights('wait', 0, 4)

        @pl.loop(0, 3)
        def _(n):
            for r in range(GROUP):
                wt[n * GROUP + r] = w[n, r].T

    def grad_rows():
        return gbuf[pl.ds(step * STEP_SEQS, STEP_SEQS)].reshape(TOK, 640)

    vocab = lax.broadcasted_iota(jnp.int32, (64, TOK), 0)
    one_hot = jnp.where(vocab == tok_ref[0], 1.0, 0.0).astype(BF16)
    e_s[...] = lax.dot_general(one_hot, emb_ref[...], (((0,), (0,)), ((), ())), preferred_element_type=F32)

    @pl.loop(0, TOK // 128, unroll=2)
    def _(r):
        rows = pl.ds(pl.multiple_of(r * 128, 128), 128)
        keep = jnp.concatenate([keep_ref[rows]] * TILES, axis=1)
        emb = e_s[rows] * keep
        e_s[rows] = emb
        xhat, _ = norm_stats(emb)
        nm[rows] = (xhat * vec_ref[0:1] + vec_ref[1:2]).astype(BF16)

    ht[...] = nm[...].T

    cos, sin = cos_ref[cp], sin_ref[cp]
    for kind, (t_ref, n_ref) in enumerate(((qt, qn), (kt, kn), (vt, vn))):
        z = mm(wt[kind * TILES:(kind + 1) * TILES].reshape(640, 640), ht[...])
        bias = bqkv_ref[kind * 640:(kind + 1) * 640]
        z = z + jnp.concatenate([bias] * (TOK // LANES), axis=1)
        if kind == 0:
            z = z * HEAD ** -0.5
        if kind < 2:
            z = turn(z, cos, sin, 20)
        zb = z.astype(BF16)
        for s in range(STEP_SEQS):
            for t in range(TILES):
                piece = zb[t * LANES:(t + 1) * LANES, s * SEQ:(s + 1) * SEQ]
                t_ref[s, t] = piece
                n_ref[s, t] = piece.T

    lane_head = lax.broadcasted_iota(jnp.int32, (1, LANES), 1) // HEAD
    pick = [jnp.where(lane_head == h, 1.0, 0.0).astype(BF16) for h in range(HEADS_PER)]

    def stack(tile):
        return jnp.concatenate([tile * pick[h] for h in range(HEADS_PER)], axis=0)

    def spot(h):
        return slice((h % 2) * SEQ, (h % 2 + 1) * SEQ), (h // 2) * SEQ

    def stage(buf, value):
        for h in range(HEADS_PER):
            down, along = spot(h)
            buf[down, along:along + SEQ] = value[h * SEQ:(h + 1) * SEQ]

    @pl.loop(0, STEP_SEQS)
    def _(s):
        rows = pl.ds(pl.multiple_of(s * SEQ, SEQ), SEQ)
        bufs = (y_s, dnm)

        def scores(t):
            stage(bufs[t % 2], mm(stack(kn[s, t]), qt[s, t]))

        scores(0)
        for t in range(TILES):
            if t + 1 < TILES:
                scores(t + 1)
            bias = mask_ref[rows]
            for h in range(HEADS_PER):
                down, along = spot(h)
                for c in range(0, SEQ, LANES):
                    score = bufs[t % 2][down, along + c:along + c + LANES] + bias
                    p = jnp.exp(score - jnp.max(score, axis=0, keepdims=True))
                    p = p * (1.0 / jnp.sum(p, axis=0, keepdims=True))
                    pt[s, t * HEADS_PER + h, :, c:c + LANES] = p.astype(BF16)
            v_t = vt[s, t]
            out = jnp.concatenate([mm(v_t[h * HEAD:(h + 1) * HEAD], pt[s, t * HEADS_PER + h]) for h in range(HEADS_PER)], axis=0)
            ot32[s, t] = out
            outb = out.astype(BF16)
            otb[t, :, rows] = outb
            dqkv[t, rows] = outb.T

    w_out = wide(w, 3)
    x1[...] = e_s[...] + mm(flat(dqkv, 0, TILES), w_out) + vec_ref[5:6]

    @pl.loop(0, TOK // 128, unroll=2)
    def _(r):
        rows = pl.ds(pl.multiple_of(r * 128, 128), 128)
        xhat, _ = norm_stats(x1[rows])
        nm[rows] = (xhat * vec_ref[6:7] + vec_ref[7:8]).astype(BF16)

    nmt[...] = nm[...].T
    y_s[...] = jnp.zeros_like(y_s)
    dnm[...] = jnp.zeros_like(dnm)

    @pl.when(step == 0)
    def _():
        weights('wait', 4, 8)
        for copy in grad_loads():
            copy.wait()

    @pl.loop(0, 4)
    def _(c):
        g = grad_rows()
        w_up = wide(w, 4 + c)
        u = mm(nm[...], w_up) + bup_ref[c]
        a, slope = gelu_pair(u)
        ab = a.astype(BF16)
        w_down = wide(w, 8 + c)
        du = mm_t(g, w_down) * slope
        dbup[c] += fold8(du)
        dub = du.astype(BF16)
        y_s[...] += mm(ab, w_down)
        dnm[...] += mm_t(dub, w_up)
        add_blocks(acc, 8 + c, mm(ab.T, g))
        add_blocks(acc, 4 + c, mm(nmt[...], dub))

    @pl.when(step == STEPS - 1)
    def _():
        ship('start', 4, 8)

    @pl.loop(0, STEP_SEQS)
    def _(seq):
        for part in range(2):
            rows = pl.ds(pl.multiple_of(seq * SEQ, SEQ) + part * 128, 128)
            x = x1[rows]
            out = (x + y_s[rows] + vec_ref[8:9]).astype(BF16)
            (y_own, y_oth)[part][seq] = out
            xhat, rstd = norm_stats(x)
            d_n = dnm[rows]
            g32 = gbuf[step * STEP_SEQS + seq, part].astype(F32)
            dsum[3] += fold8(d_n * xhat)
            dsum[4] += fold8(d_n)
            d_r = g32 + norm_back(d_n, vec_ref[6:7], xhat, rstd)
            dsum[2] += fold8(d_r)
            dsum[5] += fold8(g32)
            y_s[rows] = d_r
            nm[rows] = d_r.astype(BF16)

    d_rb = nm[...]
    add_blocks(acc, 3, mm(otb[...].reshape(640, TOK), d_rb))
    d_o = mm(wide(w, 3), d_rb.T)
    for t in range(TILES):
        dot_s[t] = d_o[t * LANES:(t + 1) * LANES]

    @pl.loop(0, STEP_SEQS)
    def _(s):
        rows = pl.ds(pl.multiple_of(s * SEQ, SEQ), SEQ)
        bufs = (x1, dnm)
        outs = (nm, nmt)

        def slopes(t):
            stage(bufs[t % 2], mm(stack(vn[s, t]), dot_s[t, :, rows].astype(BF16)))

        slopes(0)
        for t in range(TILES):
            if t + 1 < TILES:
                slopes(t + 1)
            d_ot = dot_s[t, :, rows]
            prod = d_ot * ot32[s, t]
            ds_ref = outs[t % 2]
            for h in range(HEADS_PER):
                down, along = spot(h)
                delta = jnp.sum(prod[h * HEAD:(h + 1) * HEAD], axis=0, keepdims=True)
                for c in range(0, SEQ, LANES):
                    d_p = bufs[t % 2][down, along + c:along + c + LANES]
                    p = pt[s, t * HEADS_PER + h, :, c:c + LANES].astype(F32)
                    ds_ref[down, along + c:along + c + LANES] = (p * (d_p - delta[:, c:c + LANES])).astype(BF16)
            k_t, q_n = kt[s, t], qn[s, t]
            dqs = []
            for h in range(HEADS_PER):
                down, along = spot(h)
                dqs.append(mm(k_t[h * HEAD:(h + 1) * HEAD], ds_ref[down, along:along + SEQ]))
            dq = unturn(jnp.concatenate(dqs, axis=0), cos[:, :SEQ], sin[:, :SEQ], HEADS_PER) * HEAD ** -0.5
            dbq[t] += dq[:, :LANES] + dq[:, LANES:]
            dqkv[t, rows] = dq.astype(BF16).T
            dk = mm(ds_ref[:SEQ, :2 * SEQ], jnp.concatenate([q_n * pick[0], q_n * pick[2]], axis=0))
            dk = dk + mm(ds_ref[SEQ:2 * SEQ, :2 * SEQ], jnp.concatenate([q_n * pick[1], q_n * pick[3]], axis=0))
            p_wide = jnp.concatenate([pt[s, t * HEADS_PER + h] for h in range(HEADS_PER)], axis=1)
            dv = mm(p_wide, stack(d_ot.astype(BF16).T))
            low = lax.rem(lax.broadcasted_iota(jnp.int32, (SEQ, LANES), 1), HEAD) < HEAD // 2
            other = jnp.where(low, pltpu.roll(dk, LANES - HEAD // 2, 1), pltpu.roll(dk, HEAD // 2, 1))
            dk = dk * cosn_ref[cp] + other * sinn_ref[cp]
            dbkv[0, t] += fold8(dk)
            dbkv[1, t] += fold8(dv)
            dqkv[TILES + t, rows] = dk.astype(BF16)
            dqkv[2 * TILES + t, rows] = dv.astype(BF16)

    for kind in range(3):
        add_blocks(acc, kind, mm(ht[...], flat(dqkv, kind * TILES, TILES)))
    dnm[...] = mm(flat(dqkv, 0, 15), wt[...].reshape(1920, 640))

    @pl.loop(0, TOK // 128, unroll=2)
    def _(r):
        rows = pl.ds(pl.multiple_of(r * 128, 128), 128)
        xhat, rstd = norm_stats(e_s[rows])
        d_n = dnm[rows]
        dsum[0] += fold8(d_n * xhat)
        dsum[1] += fold8(d_n)
        keep = jnp.concatenate([keep_ref[rows]] * TILES, axis=1)
        nm[rows] = ((norm_back(d_n, vec_ref[0:1], xhat, rstd) + y_s[rows]) * keep).astype(BF16)

    dtab[...] += mm(one_hot, nm[...])

    @pl.when(step == STEPS - 1)
    def _():
        ship('start', 0, 4)
        ship('wait', 4, 8)
        ship('wait', 0, 4)


def layer_call(tok, keep, mask, emb, vecs, bup, cos, sin, cosn, sinn, w_hbm, g_own, g_oth):
    vm = pltpu.VMEM
    dma = pltpu.SemaphoreType.DMA

    def whole(shape):
        return pl.BlockSpec(shape, lambda i: (0,) * len(shape))

    pair = pl.BlockSpec((STEP_SEQS, 128, 640), lambda i: (i, 0, 0))
    out_shape = (
        jax.ShapeDtypeStruct((SEQS, 128, 640), BF16),
        jax.ShapeDtypeStruct((SEQS, 128, 640), BF16),
        jax.ShapeDtypeStruct((64, 2 * PER, GROUP * NB, LANES), F32),
        jax.ShapeDtypeStruct((64, 640), F32),
        jax.ShapeDtypeStruct((6, 8, 640), F32),
        jax.ShapeDtypeStruct((TILES, LANES, LANES), F32),
        jax.ShapeDtypeStruct((2, TILES, 8, LANES), F32),
        jax.ShapeDtypeStruct((4, 8, 640), F32),
    )
    out_specs = (pair, pair, ANY) + tuple(whole(o.shape) for o in out_shape[3:])
    in_specs = [
        pl.BlockSpec((1, 1, TOK), lambda i: (i, 0, 0)),
        pl.BlockSpec((1, 1, TOK), lambda i: (i, 0, 0)),
        pl.BlockSpec((1, 1, TOK), lambda i: (i, 0, 0)),
    ] + [whole(a.shape) for a in (emb, vecs, bup, cos, sin, cosn, sinn)] + [ANY] * 3
    halves = (STEP_SEQS, TILES, LANES, SEQ)
    flipped = (STEP_SEQS, TILES, SEQ, LANES)
    scratch = [
        vm((2 * PER, GROUP, 640, LANES), BF16), vm((15, LANES, 640), BF16), vm((2 * PER, GROUP, 640, LANES), F32), vm((SEQS, 2, 128, 640), BF16),
        vm((TOK, 640), F32), vm((640, TOK), BF16),
        vm(halves, BF16), vm(halves, BF16), vm(halves, BF16), vm(flipped, BF16), vm(flipped, BF16), vm(flipped, BF16),
        vm((STEP_SEQS, 20, SEQ, SEQ), BF16), vm(halves, F32), vm((TILES, LANES, TOK), BF16),
        vm((TOK, 640), F32), vm((TOK, 640), BF16), vm((640, TOK), BF16), vm((TOK, 640), F32), vm((TOK, 640), F32),
        vm((TILES, LANES, TOK), F32), vm((15, TOK, LANES), BF16), vm((TOK, LANES), F32), vm((TOK, LANES), F32), vm((1920, LANES), F32),
        dma((2,)), dma((2,)), dma((2,)),
    ]
    return pl.pallas_call(
        layer_kernel,
        grid=(STEPS,),
        out_shape=out_shape,
        in_specs=in_specs,
        out_specs=out_specs,
        scratch_shapes=scratch,
        compiler_params=pltpu.CompilerParams(dimension_semantics=('arbitrary',), vmem_limit_bytes=67043328),
        name='layer',
    )(tok, keep, mask, emb, vecs, bup, cos, sin, cosn, sinn, w_hbm, g_own, g_oth)


def prepare(tokens, lengths, positions, embed_table, vecs_all):
    n_seq, seq_len = tokens.shape
    is_mask = tokens == MASK_ID
    tok_valid = positions[None, :] < lengths[:, None]
    mask_count = jnp.sum(is_mask.astype(jnp.int32), axis=1)
    drop_scale = (1.0 - TRAIN_RATIO) / (1.0 - mask_count.astype(F32) / lengths.astype(F32))
    keep = jnp.where(is_mask | jnp.logical_not(tok_valid), 0.0, drop_scale[:, None])
    mask = jnp.where(tok_valid, 0.0, NEG_BIG).astype(F32)
    emb = jnp.pad(embed_table, ((0, 64 - embed_table.shape[0]), (0, 0)))
    rows = [x.reshape(STEPS, 1, TOK) for x in (tokens, keep, mask)]
    return (*rows, emb, *rope_tables(seq_len // 2))


def rope_tables(half):
    inv_freq = (1.0 / (np.float32(ROPE_BASE) ** (np.arange(0, HEAD, 2, dtype=np.float32) / np.float32(HEAD)))).astype(np.float32)
    tables = []
    for cp in range(2):
        positions = np.concatenate([np.arange(half) + cp * half, np.arange(half) + (1 - cp) * half]).astype(np.float32)
        angles = (positions[:, None] * inv_freq[None, :]).astype(np.float64)
        cos, sin = np.cos(angles), np.sin(angles)
        tables.append((
            np.tile(cos.T, (1, STEP_SEQS)), np.tile(sin.T, (1, STEP_SEQS)),
            np.tile(cos, (1, 8)), np.tile(np.concatenate([sin, -sin], axis=1), (1, 4)),
        ))
    return tuple(jnp.asarray(np.stack(pair), F32) for pair in zip(*tables))


def solution(mesh):
    chips = mesh.shape['fsdp']

    def local_step(tokens, lengths, embed_table, layer_vecs, w_qkv, w_out, w_up, b_up, w_down, grad_out):
        f32 = jnp.float32
        cp = lax.axis_index('cp')
        chip = lax.axis_index('fsdp')
        n_seq, seq_loc = tokens.shape
        half = n_seq // 2
        rows = w_qkv.shape[0]
        vocab, width = embed_table.shape
        w_loc = jnp.concatenate([
            w_qkv.reshape(rows, 15, 128).transpose(1, 0, 2),
            w_out.reshape(rows, 5, 128).transpose(1, 0, 2),
            w_up.reshape(rows, chips, 4, NB).transpose(2, 1, 3, 0).reshape(20, 128, rows).transpose(0, 2, 1),
            w_down.reshape(4, NB, 5, 128).transpose(0, 2, 1, 3).reshape(20, NB, 128),
        ], axis=0)
        s_loc = jnp.pad(jnp.concatenate([layer_vecs.reshape(-1), b_up]), (0, 1024 - 130)).reshape(8, 128)
        w_all, s_all, g_oth, t_oth = gather_all(w_loc.reshape(2 * PER, GROUP * NB, 128), s_loc, grad_out, tokens)
        s_flat = s_all.reshape(chips, 1024)
        vecs_all = s_flat[:, :90].reshape(chips, 9, NB).transpose(1, 0, 2).reshape(9, width)
        up_b = s_flat[:, 90:130].reshape(chips, 4, NB).transpose(1, 0, 2).reshape(-1)
        start = half * cp
        tok_full = jnp.concatenate([lax.dynamic_slice_in_dim(tokens, start, half, 0), t_oth], axis=1)
        len_own = lax.dynamic_slice_in_dim(lengths, start, half, 0)
        positions = jnp.concatenate([cp * seq_loc + jnp.arange(seq_loc), (1 - cp) * seq_loc + jnp.arange(seq_loc)])
        tok, keep, mask, emb, cos, sin, cosn, sinn = prepare(tok_full, len_own, positions, embed_table, vecs_all)
        y_own, y_oth, g_all, dtab, dsum, dbq, dbkv, dbup = layer_call(
            tok, keep, mask, emb, vecs_all, up_b.reshape(4, 1, 640), cos, sin, cosn, sinn, w_all.reshape(chips, 2 * PER, GROUP * NB, 128), grad_out, g_oth)
        rowsum = jnp.sum(dsum, axis=1)
        d_bq = jnp.sum(dbq, axis=2).reshape(1, width)
        d_bkv = jnp.sum(dbkv, axis=2).reshape(2, width)
        small = jnp.concatenate([dtab[:vocab].reshape(-1), rowsum[:2].reshape(-1), d_bq.reshape(-1), d_bkv.reshape(-1), rowsum[2:].reshape(-1), jnp.sum(dbup, axis=1).reshape(-1)])
        small = jnp.pad(small, (0, 2 * SMALL_ROWS * 128 - small.shape[0])).reshape(2, SMALL_ROWS, 128)
        g_red, s_red, out_full = reduce_all(g_all.reshape(SIDE, SIDE, SIDE, 2 * PER, GROUP * NB, 128), small, y_own, y_oth)
        g_red = g_red.reshape(60, NB, 128)
        s_flat = s_red.reshape(-1)
        n_tab = vocab * width
        d_embed = s_flat[:n_tab].reshape(vocab, width)
        d_v = lax.dynamic_slice(s_flat[n_tab:n_tab + 9 * width].reshape(9, width), (0, chip * NB), (9, NB))
        d_b = s_flat[n_tab + 9 * width:n_tab + 9 * width + 2560].reshape(4, chips, NB)
        d_b = lax.dynamic_slice(d_b, (0, chip, 0), (4, 1, NB)).reshape(-1)
        d_qkv = g_red[:15].transpose(1, 0, 2).reshape(w_qkv.shape)
        d_wout = g_red[15:20].transpose(1, 0, 2).reshape(w_out.shape)
        d_wup = g_red[20:40].transpose(0, 2, 1).reshape(4, chips, NB, rows).transpose(3, 1, 0, 2).reshape(w_up.shape)
        d_wdown = g_red[40:60].reshape(4, 5, NB, 128).transpose(0, 2, 1, 3).reshape(w_down.shape)
        return out_full, d_embed, d_v, d_qkv, d_wout, d_wup, d_b, d_wdown

    in_specs = (P('fsdp', 'cp'), P('fsdp'), P(), P(None, 'fsdp'), P('fsdp', None, None, None), P('fsdp', None), P('fsdp', None), P('fsdp'), P('fsdp', None), P('fsdp', 'cp', None))
    out_specs = (P('fsdp', 'cp', None), P(), P(None, 'fsdp'), P('fsdp', None, None, None), P('fsdp', None), P('fsdp', None), P('fsdp'), P('fsdp', None))
    return jax.shard_map(local_step, mesh=mesh, in_specs=in_specs, out_specs=out_specs, check_vma=False)
```

```python
import functools

import jax
import jax.numpy as jnp
import numpy as np
from jax import lax
from jax.experimental import pallas as pl
from jax.experimental.pallas import tpu as pltpu
from jax.sharding import PartitionSpec as P

MASK_ID = 32
LN_EPS = 1e-5
ROPE_BASE = 10000.0
TRAIN_RATIO = 0.15 * 0.8
NEG_BIG = -1e30
SIDE = 4
COLORS = 3
NB = 10
GROUP = 5
PER = 6
SMALL_ROWS = 120
SMALL_BLOCK = 48
VOCAB = 33
QUARTERS = (2, 1, 3, 0)
MESH_ID = pl.DeviceIdType.MESH
ANY = pl.BlockSpec(memory_space=pl.ANY)

GATHER_ORDER = ((2, 1, 0), (1, 0, 2), (0, 2, 1))
REDUCE_ORDER = ((0, 1, 2), (1, 2, 0), (2, 0, 1))


def my_coords():
    chip = lax.axis_index('fsdp')
    return [chip // 16, lax.rem(chip // 4, 4), lax.rem(chip, 4)]


def moved(coords, dim, by):
    out = list(coords)
    out[dim] = lax.rem(coords[dim] + by + SIDE, SIDE)
    return out


def chip_id(coords):
    return {'fsdp': coords[0] * 16 + coords[1] * 4 + coords[2]}


def entry_barrier(coords, cp):
    barrier = pltpu.get_barrier_semaphore()
    for dim in range(3):
        for by in (1, 2, 3):
            pl.semaphore_signal(barrier, inc=1, device_id=chip_id(moved(coords, dim, by)), device_id_type=MESH_ID)
    pl.semaphore_signal(barrier, inc=1, device_id={'cp': 1 - cp}, device_id_type=MESH_ID)
    pl.semaphore_wait(barrier, 10)


def push(src, dst, send_sem, recv_sem, target):
    return pltpu.make_async_remote_copy(src_ref=src, dst_ref=dst, send_sem=send_sem, recv_sem=recv_sem, device_id=target, device_id_type=MESH_ID)


def gather_kernel(w_loc, s_loc, g_own, t_own, w_out, s_out, g_oth, t_oth, w_all, s_all, ssem, rsem, fsend, frecv, s_ssem, s_rsem, psend, precv, lsem, osem, xsem):
    cp = lax.axis_index('cp')
    me = my_coords()
    mate = {'cp': 1 - cp}
    own_w = pltpu.make_async_copy(w_loc, w_all.at[me[0], me[1], me[2]], lsem.at[0])
    own_s = pltpu.make_async_copy(s_loc, s_all.at[me[0], me[1], me[2]], lsem.at[1])
    own_w.start()
    own_s.start()
    entry_barrier(me, cp)
    swap_g = push(g_own.at[pl.ds(8 * (1 - cp), 8)], g_oth, psend.at[0], precv.at[0], mate)
    swap_t = push(t_own.at[pl.ds(8 * (1 - cp), 8)], t_oth, psend.at[1], precv.at[1], mate)
    swap_t.start()

    def region(ref, first, count, dims, at):
        index = [slice(None) if d in dims else at[d] for d in range(3)]
        return ref.at[(*index, pl.ds(first, count))]

    def small_region(dims, at):
        index = [slice(None) if d in dims else at[d] for d in range(3)]
        return s_all.at[tuple(index)]

    forwards = []
    pending = []
    stores = []
    arrivals = {}

    def store(first, count, dims, at, sem):
        index = [slice(None) if d in dims else at[d] for d in range(3)]
        index = (*index, pl.ds(first, count))
        copy = pltpu.make_async_copy(w_all.at[index], w_out.at[index], sem)
        copy.start()
        stores.append(copy)

    own_s.wait()
    own_w.wait()
    store(0, 2 * PER, (), me, lsem.at[2])
    for phase in range(3):
        firsts = {}
        for color in range(COLORS):
            dim = GATHER_ORDER[color][phase]
            done = GATHER_ORDER[color][:phase]
            base = cp * PER + color * 2
            mine = region(w_all, base, 2, done, me)
            right, left = chip_id(moved(me, dim, 1)), chip_id(moved(me, dim, 3))
            to_right = push(mine, mine, ssem.at[color, phase, 0], rsem.at[color, phase, 0], right)
            to_left = push(mine, mine, ssem.at[color, phase, 1], rsem.at[color, phase, 1], left)
            to_right.start()
            to_left.start()
            firsts[color] = (to_right, to_left)
            pending += [to_right, to_left]
            if color == 0:
                s_mine = small_region(done, me)
                s_right = push(s_mine, s_mine, s_ssem.at[phase, 0], s_rsem.at[phase, 0], right)
                s_left = push(s_mine, s_mine, s_ssem.at[phase, 1], s_rsem.at[phase, 1], left)
                s_right.start()
                s_left.start()
                pending += [s_right, s_left]
        seconds = {}
        for color in range(COLORS):
            dim = GATHER_ORDER[color][phase]
            done = GATHER_ORDER[color][:phase]
            base = cp * PER + color * 2
            right, left = chip_id(moved(me, dim, 1)), chip_id(moved(me, dim, 3))
            from_left, from_right = moved(me, dim, 3), moved(me, dim, 1)
            to_right, to_left = firsts[color]
            to_right.wait_recv()
            part = region(w_all, base, 1, done, from_left)
            on_right = push(part, part, ssem.at[color, phase, 2], rsem.at[color, phase, 2], right)
            on_right.start()
            whole_l = region(w_all, base, 2, done, from_left)
            fwd_l = push(whole_l, whole_l, fsend.at[color, phase, 0], frecv.at[color, phase, 0], mate)
            fwd_l.start()
            store(base, 2, done, from_left, osem.at[color, phase, 0])
            to_left.wait_recv()
            part = region(w_all, base + 1, 1, done, from_right)
            on_left = push(part, part, ssem.at[color, phase, 3], rsem.at[color, phase, 3], left)
            on_left.start()
            whole_r = region(w_all, base, 2, done, from_right)
            fwd_r = push(whole_r, whole_r, fsend.at[color, phase, 1], frecv.at[color, phase, 1], mate)
            fwd_r.start()
            store(base, 2, done, from_right, osem.at[color, phase, 1])
            seconds[color] = (on_right, on_left)
            pending += [on_right, on_left]
            forwards += [fwd_l, fwd_r]
            arrivals[color, phase] = [(fwd_l, done, from_left, 0), (fwd_r, done, from_right, 1)]
            if color == 0:
                s_right.wait_recv()
                s_left.wait_recv()
                s_part = small_region(done, from_left)
                s_on = push(s_part, s_part, s_ssem.at[phase, 2], s_rsem.at[phase, 2], right)
                s_on.start()
                pending.append(s_on)
        for color in range(COLORS):
            dim = GATHER_ORDER[color][phase]
            done = GATHER_ORDER[color][:phase]
            base = cp * PER + color * 2
            on_right, on_left = seconds[color]
            on_right.wait_recv()
            on_left.wait_recv()
            far = region(w_all, base, 2, done, moved(me, dim, 2))
            fwd_f = push(far, far, fsend.at[color, phase, 2], frecv.at[color, phase, 2], mate)
            fwd_f.start()
            store(base, 2, done, moved(me, dim, 2), osem.at[color, phase, 2])
            forwards.append(fwd_f)
            arrivals[color, phase].append((fwd_f, done, moved(me, dim, 2), 2))
            if color == 0:
                s_on.wait_recv()
        if phase == 0:
            swap_g.start()
    s_store = pltpu.make_async_copy(s_all, s_out, lsem.at[3])
    s_store.start()
    for phase in range(3):
        for color in range(COLORS):
            for copy, done, at, slot in arrivals[color, phase]:
                copy.wait_recv()
                store((1 - cp) * PER + color * 2, 2, done, at, xsem.at[color, phase, slot])
    s_store.wait()
    for copy in stores:
        copy.wait()
    swap_g.wait()
    swap_t.wait()
    for copy in pending + forwards:
        copy.wait_send()


def gather_all(w_loc, s_loc, grad_out, tokens):
    bf16, f32 = jnp.bfloat16, jnp.float32
    seqs, pos, width = grad_out.shape
    dma = pltpu.SemaphoreType.DMA
    return pl.pallas_call(
        gather_kernel,
        out_shape=(
            jax.ShapeDtypeStruct((SIDE, SIDE, SIDE, *w_loc.shape), bf16),
            jax.ShapeDtypeStruct((SIDE, SIDE, SIDE, 8, 128), f32),
            jax.ShapeDtypeStruct((seqs // 2, pos, width), bf16),
            jax.ShapeDtypeStruct((seqs // 2, pos), jnp.int32),
        ),
        in_specs=[ANY] * 4,
        out_specs=(ANY,) * 4,
        scratch_shapes=[
            pltpu.VMEM((SIDE, SIDE, SIDE, *w_loc.shape), bf16), pltpu.VMEM((SIDE, SIDE, SIDE, 8, 128), f32),
            dma((3, 3, 4)), dma((3, 3, 4)), dma((3, 3, 3)), dma((3, 3, 3)), dma((3, 3)), dma((3, 3)), dma((2,)), dma((2,)), dma((4,)), dma((3, 3, 3)), dma((3, 3, 3)),
        ],
        compiler_params=pltpu.CompilerParams(collective_id=0, has_side_effects=True, vmem_limit_bytes=40 * 1024 * 1024),
        name='gather_weights',
    )(w_loc, s_loc, grad_out, tokens)


def reduce_kernel(g_all, small, y_own, y_oth, g_out, s_out, y_full, y_hold, held, pair, ra0, rb0, ra1, rb1, ra2, rb2, s_pair, s_slots, s_acc,
                  lsem, psend, precv, ssem, rsem, s_ssem, s_rsem, osend, orecv, msem):
    cp = lax.axis_index('cp')
    me = my_coords()
    mate = {'cp': 1 - cp}
    per = PER
    loads = {}

    def quarter(ref, first, color, by):
        dim = REDUCE_ORDER[color][0]
        index = [slice(None)] * 3
        index[dim] = moved(me, dim, by)[dim]
        return ref.at[(*index, pl.ds(first + color * 2, 2))]

    for by in QUARTERS:
        for color in range(COLORS):
            load = pltpu.make_async_copy(quarter(g_all, cp * per, color, by), quarter(held, 0, color, by), lsem.at[color, by])
            load.start()
            loads[color, by] = load
    s_load = pltpu.make_async_copy(small, s_acc, msem.at[2])
    s_load.start()
    entry_barrier(me, cp)
    sends = []
    s_swap = push(small, s_pair, osend.at[2], orecv.at[2], mate)
    s_swap.start()
    swaps = {}
    for by in QUARTERS:
        for color in range(COLORS):
            swap = push(quarter(g_all, (1 - cp) * per, color, by), quarter(pair, 0, color, by), psend.at[color, by], precv.at[color, by], mate)
            swap.start()
            swaps[color, by] = swap
    y_rows = y_full.at[pl.ds(y_own.shape[0] * cp, y_own.shape[0])]
    y_swap = push(y_oth, y_rows, osend.at[3], orecv.at[3], mate)
    y_swap.start()
    y_in = pltpu.make_async_copy(y_own, y_hold, msem.at[3])
    y_in.start()

    bufs = ((ra0, rb0), (ra1, rb1), (ra2, rb2))

    def index_of(dims, at):
        return [slice(None) if d in dims else at[d] for d in range(3)]

    def region(first, count, dims, at):
        return held.at[(*index_of(dims, at), pl.ds(first, count))]

    def side(rb, color, way, rest, half):
        return rb.at[(color, way, *[slice(None)] * len(rest), pl.ds(half, 1))]

    def accumulate(rest, at, first, count, *sources):
        where = index_of(rest, at)
        units = slice(first, first + count)

        def add(lead):
            total = held[(*where, units)]
            for ref, color, way in sources:
                total = total + ref[(color, way, *lead)]
            held[(*where, units)] = total

        if rest:
            dim = min(rest)

            @pl.loop(0, SIDE)
            def _(v):
                where[dim] = v
                add((v,))
        else:
            add(())

    def start_phase(color, phase, part=None):
        dim = REDUCE_ORDER[color][phase]
        rest = REDUCE_ORDER[color][phase + 1:]
        base = color * 2
        ra, rb = bufs[phase]
        right, left = moved(me, dim, 1), moved(me, dim, 3)
        far = moved(me, dim, 2)
        out = [
            push(region(base, 1, rest, far), ra.at[color, 0], ssem.at[color, phase, 0], rsem.at[color, phase, 0], chip_id(right)),
            push(region(base + 1, 1, rest, far), ra.at[color, 1], ssem.at[color, phase, 1], rsem.at[color, phase, 1], chip_id(left)),
            push(region(base + 1, 1, rest, right), side(rb, color, 0, rest, 1), ssem.at[color, phase, 2], rsem.at[color, phase, 2], chip_id(right)),
            push(region(base, 1, rest, left), side(rb, color, 1, rest, 0), ssem.at[color, phase, 3], rsem.at[color, phase, 3], chip_id(left)),
        ]
        if part is not None:
            out = {2: out[:2], 1: out[2:3], 3: out[3:]}[part]
        for copy in out:
            copy.start()
        sends.extend(out)
        return out

    def middle(color, phase, copies):
        dim = REDUCE_ORDER[color][phase]
        rest = REDUCE_ORDER[color][phase + 1:]
        base = color * 2
        ra, rb = bufs[phase]
        right, left = moved(me, dim, 1), moved(me, dim, 3)
        copies[0].wait_recv()
        accumulate(rest, right, base, 1, (ra, color, 0))

        fwd_r = push(region(base, 1, rest, right), side(rb, color, 0, rest, 0), ssem.at[color, phase, 4], rsem.at[color, phase, 4], chip_id(right))
        fwd_r.start()
        copies[1].wait_recv()
        accumulate(rest, left, base + 1, 1, (ra, color, 1))

        fwd_l = push(region(base + 1, 1, rest, left), side(rb, color, 1, rest, 1), ssem.at[color, phase, 5], rsem.at[color, phase, 5], chip_id(left))
        fwd_l.start()
        sends.extend([fwd_r, fwd_l])
        return [fwd_r, fwd_l]

    def finish(color, phase, copies, late):
        rest = REDUCE_ORDER[color][phase + 1:]
        base = color * 2
        ra, rb = bufs[phase]
        copies[2].wait_recv()
        copies[3].wait_recv()
        late[0].wait_recv()
        late[1].wait_recv()
        accumulate(rest, me, base, 2, (rb, color, 0), (rb, color, 1))

    s_copies = []

    def small_start(phase):
        dim = REDUCE_ORDER[0][phase]
        out = []
        for by in (1, 2, 3):
            out.append(push(s_acc.at[cp], s_slots.at[phase, by - 1], s_ssem.at[phase, by - 1], s_rsem.at[phase, by - 1], chip_id(moved(me, dim, by))))
        for copy in out:
            copy.start()
        return out

    def small_finish(phase, copies):
        dim = REDUCE_ORDER[0][phase]
        for copy in copies:
            copy.wait()
        mine = me[dim]
        total = None
        own = s_acc[cp]
        got = [own] + [s_slots[phase, by] for by in range(3)]
        for coord in range(SIDE):
            gap = lax.rem(mine - coord + SIDE, SIDE)
            value = jnp.where(gap == 0, got[0], jnp.where(gap == 1, got[1], jnp.where(gap == 2, got[2], got[3])))
            total = value if total is None else total + value
        s_acc[cp] = total

    y_in.wait()
    y_put = pltpu.make_async_copy(y_hold, y_rows, msem.at[4])
    y_put.start()
    s_load.wait()
    s_swap.wait()
    s_acc[...] = s_acc[...] + s_pair[...]
    s_out_copies = small_start(0)
    started = [[] for _ in range(COLORS)]
    for by in QUARTERS:
        for color in range(COLORS):
            loads[color, by].wait()
            swaps[color, by].wait_recv()
            dim = REDUCE_ORDER[color][0]
            part = [slice(None)] * 3
            part[dim] = moved(me, dim, by)[dim]
            other = (dim + 1) % 3

            @pl.loop(0, SIDE)
            def _(v):
                part[other] = v
                at = (*part, slice(color * 2, color * 2 + 2))
                held[at] += pair[at]

            if by:
                started[color] += start_phase(color, 0, by)
    for phase in range(3):
        late = [middle(color, phase, started[color]) for color in range(COLORS)]
        nxt = []
        for color in range(COLORS):
            finish(color, phase, started[color], late[color])
            if phase < 2:
                nxt.append(start_phase(color, phase + 1))
        small_finish(phase, s_out_copies)
        if phase < 2:
            s_out_copies = small_start(phase + 1)
        started = nxt
    mine = held.at[me[0], me[1], me[2]]
    out_far = push(mine, g_out.at[pl.ds(cp * per, per)], osend.at[0], orecv.at[0], mate)
    out_far.start()
    s_far = push(s_acc.at[cp], s_out.at[cp], osend.at[1], orecv.at[1], mate)
    s_far.start()
    out_own = pltpu.make_async_copy(mine, g_out.at[pl.ds(cp * per, per)], msem.at[0])
    out_own.start()
    s_own = pltpu.make_async_copy(s_acc.at[cp], s_out.at[cp], msem.at[1])
    s_own.start()
    for copy in sends:
        copy.wait_send()
    for copy in swaps.values():
        copy.wait_send()
    y_swap.wait()
    y_put.wait()
    out_own.wait()
    s_own.wait()
    out_far.wait()
    s_far.wait()


def reduce_all(g_all, small, y_own, y_oth):
    f32 = jnp.float32
    units, rows = g_all.shape[3:5]
    dma = pltpu.SemaphoreType.DMA
    vm = pltpu.VMEM
    return pl.pallas_call(
        reduce_kernel,
        out_shape=(
            jax.ShapeDtypeStruct((units, rows, 128), f32),
            jax.ShapeDtypeStruct(small.shape, f32),
            jax.ShapeDtypeStruct((2 * y_oth.shape[0], *y_oth.shape[1:]), y_oth.dtype),
        ),
        in_specs=[ANY] * 4,
        out_specs=(ANY,) * 3,
        scratch_shapes=[
            vm(y_own.shape, y_own.dtype),
            vm((SIDE, SIDE, SIDE, PER, rows, 128), f32),
            vm((SIDE, SIDE, SIDE, PER, rows, 128), f32),
            vm((COLORS, 2, SIDE, SIDE, 1, rows, 128), f32),
            vm((COLORS, 2, SIDE, SIDE, 2, rows, 128), f32),
            vm((COLORS, 2, SIDE, 1, rows, 128), f32),
            vm((COLORS, 2, SIDE, 2, rows, 128), f32),
            vm((COLORS, 2, 1, rows, 128), f32),
            vm((COLORS, 2, 2, rows, 128), f32),
            vm(small.shape, f32),
            vm((3, 3) + small.shape[1:], f32),
            vm(small.shape, f32),
            dma((3, 4)), dma((3, 4)), dma((3, 4)), dma((3, 3, 6)), dma((3, 3, 6)), dma((3, 3)), dma((3, 3)), dma((4,)), dma((4,)), dma((5,)),
        ],
        compiler_params=pltpu.CompilerParams(collective_id=1, has_side_effects=True, vmem_limit_bytes=62 * 1024 * 1024),
        name='reduce_grads',
    )(g_all, small, y_own, y_oth)


SEQS = 8
STEP_SEQS = 2
STEPS = SEQS // STEP_SEQS
SEQ = 256
TOK = STEP_SEQS * SEQ
TILES = 5
HEADS_PER = 4
HEAD = 32
LANES = 128
F32 = jnp.float32
BF16 = jnp.bfloat16


def mm(lhs, rhs):
    return lax.dot_general(lhs, rhs, (((1,), (0,)), ((), ())), preferred_element_type=F32)


def mm_t(lhs, rhs):
    return lax.dot_general(lhs, rhs, (((1,), (1,)), ((), ())), preferred_element_type=F32)


def fold8(value):
    return jnp.sum(value.reshape(value.shape[0] // 8, 8, value.shape[1]), axis=0)


def wide(ref, group):
    return jnp.concatenate([ref[group, j] for j in range(GROUP)], axis=1)


def flat(ref, first, count):
    return jnp.concatenate([ref[first + j] for j in range(count)], axis=1)


def add_blocks(ref, group, value):
    for j in range(GROUP):
        ref[group, j] += value[:, j * LANES:(j + 1) * LANES]


def norm_stats(value):
    mean = jnp.mean(value, axis=-1, keepdims=True)
    cent = value - mean
    var = jnp.mean(cent * cent, axis=-1, keepdims=True)
    rstd = lax.rsqrt(var + LN_EPS)
    return cent * rstd, rstd


def norm_back(d_out, gain, xhat, rstd):
    d_hat = d_out * gain
    m1 = jnp.mean(d_hat, axis=-1, keepdims=True)
    m2 = jnp.mean(d_hat * xhat, axis=-1, keepdims=True)
    return rstd * (d_hat - m1 - xhat * m2)


def gelu_pair(u):
    z = u * (0.5 ** 0.5)
    t = 1.0 / (1.0 + 0.3275911 * jnp.abs(z))
    poly = t * (0.127414796 + t * (-0.142248368 + t * (0.710706871 + t * (-0.7265760135 + t * 0.5307027145))))
    ex = jnp.exp(-z * z)
    tail = poly * ex
    cdf = jnp.where(u >= 0, 1.0 - tail, tail)
    return u * cdf, cdf + u * (ex * 0.3989422804014327)


def unturn(z, cos, sin, groups):
    parts = z.reshape(groups, 2, HEAD // 2, z.shape[1])
    lo, up = parts[:, 0], parts[:, 1]
    out = jnp.stack([lo * cos + up * sin, up * cos - lo * sin], axis=1)
    return out.reshape(z.shape)


def turn(z, cos, sin, groups):
    return unturn(z, cos, -sin, groups)


def layer_kernel(tok_ref, keep_in, mask_in, emb_ref, vec_ref, bup_ref, cos_ref, sin_ref, cosn_ref, sinn_ref,
                 w_hbm, g_own, g_oth,
                 y_own, y_oth, grads, small,
                 w, wt, acc, gbuf, e_s, ht, qt, kt, vt, qn, kn, vn, pt, ot32, otb, x1, nm, nmt, y_s, dnm, dot_s, dqkv, keep_ref, mask_ref, bqkv_ref, dtab, dsum, dbq, dbkv, dbup,
                 wsem, gsem, osem):
    step = pl.program_id(0)
    cp = lax.axis_index('cp')
    chips = SIDE ** 3

    def weights(act, first, count):
        @pl.loop(0, chips)
        def _(i):
            for r in range(GROUP):
                src = w_hbm.at[i, pl.ds(first, count), pl.ds(r * NB, NB)]
                dst = w.at[pl.ds(first, count), r, pl.ds(i * NB, NB)]
                getattr(pltpu.make_async_copy(src, dst, wsem.at[first // 4]), act)()

    def ship(act, first, count):
        @pl.loop(0, chips)
        def _(i):
            for r in range(GROUP):
                src = acc.at[pl.ds(first, count), r, pl.ds(i * NB, NB)]
                dst = grads.at[i, pl.ds(first, count), pl.ds(r * NB, NB)]
                getattr(pltpu.make_async_copy(src, dst, osem.at[first // 4]), act)()

    def grad_loads():
        own = pltpu.make_async_copy(g_own.at[pl.ds(cp * SEQS, SEQS)], gbuf.at[:, 0], gsem.at[0])
        oth = pltpu.make_async_copy(g_oth, gbuf.at[:, 1], gsem.at[1])
        return own, oth

    keep_ref[...] = jnp.broadcast_to(keep_in[0], (LANES, TOK)).T
    mask_ref[...] = jnp.broadcast_to(mask_in[0], (LANES, TOK)).T

    @pl.when(step == 0)
    def _():
        own, oth = grad_loads()
        weights('start', 0, 4)
        weights('start', 4, 8)

        own.start()
        oth.start()

        @pl.loop(0, 2 * PER)
        def _(i):
            for r in range(GROUP):
                acc[i, r] = jnp.zeros((640, LANES), F32)

        dtab[...] = jnp.zeros_like(dtab)
        dsum[...] = jnp.zeros_like(dsum)
        dbq[...] = jnp.zeros_like(dbq)
        dbkv[...] = jnp.zeros_like(dbkv)
        dbup[...] = jnp.zeros_like(dbup)

        for kind in range(3):
            for t in range(TILES):
                first = (kind * TILES + t) * LANES
                row = vec_ref[2 + kind:3 + kind, t * LANES:(t + 1) * LANES]
                bqkv_ref[first:first + LANES] = jnp.broadcast_to(row, (LANES, LANES)).T

        weights('wait', 0, 4)

        @pl.loop(0, 3)
        def _(n):
            for r in range(GROUP):
                wt[n * GROUP + r] = w[n, r].T

    def grad_rows():
        return gbuf[pl.ds(step * STEP_SEQS, STEP_SEQS)].reshape(TOK, 640)

    vocab = lax.broadcasted_iota(jnp.int32, (64, TOK), 0)
    one_hot = jnp.where(vocab == tok_ref[0], 1.0, 0.0).astype(BF16)
    e_s[...] = lax.dot_general(one_hot, emb_ref[...], (((0,), (0,)), ((), ())), preferred_element_type=F32)

    @pl.loop(0, TOK // 128, unroll=2)
    def _(r):
        rows = pl.ds(pl.multiple_of(r * 128, 128), 128)
        keep = jnp.concatenate([keep_ref[rows]] * TILES, axis=1)
        emb = e_s[rows] * keep
        e_s[rows] = emb
        xhat, _ = norm_stats(emb)
        nm[rows] = (xhat * vec_ref[0:1] + vec_ref[1:2]).astype(BF16)

    ht[...] = nm[...].T

    cos, sin = cos_ref[cp], sin_ref[cp]
    for kind, (t_ref, n_ref) in enumerate(((qt, qn), (kt, kn), (vt, vn))):
        z = mm(wt[kind * TILES:(kind + 1) * TILES].reshape(640, 640), ht[...])
        bias = bqkv_ref[kind * 640:(kind + 1) * 640]
        z = z + jnp.concatenate([bias] * (TOK // LANES), axis=1)
        if kind == 0:
            z = z * HEAD ** -0.5
        if kind < 2:
            z = turn(z, cos, sin, 20)
        zb = z.astype(BF16)
        for s in range(STEP_SEQS):
            for t in range(TILES):
                piece = zb[t * LANES:(t + 1) * LANES, s * SEQ:(s + 1) * SEQ]
                t_ref[s, t] = piece
                n_ref[s, t] = piece.T

    lane_head = lax.broadcasted_iota(jnp.int32, (1, LANES), 1) // HEAD
    pick = [jnp.where(lane_head == h, 1.0, 0.0).astype(BF16) for h in range(HEADS_PER)]

    def stack(tile):
        return jnp.concatenate([tile * pick[h] for h in range(HEADS_PER)], axis=0)

    def spot(h):
        return slice((h % 2) * SEQ, (h % 2 + 1) * SEQ), (h // 2) * SEQ

    def stage(buf, value):
        for h in range(HEADS_PER):
            down, along = spot(h)
            buf[down, along:along + SEQ] = value[h * SEQ:(h + 1) * SEQ]

    @pl.loop(0, STEP_SEQS)
    def _(s):
        rows = pl.ds(pl.multiple_of(s * SEQ, SEQ), SEQ)
        bufs = (y_s, dnm)

        def scores(t):
            stage(bufs[t % 2], mm(stack(kn[s, t]), qt[s, t]))

        scores(0)
        for t in range(TILES):
            if t + 1 < TILES:
                scores(t + 1)
            bias = mask_ref[rows]
            for h in range(HEADS_PER):
                down, along = spot(h)
                for c in range(0, SEQ, LANES):
                    score = bufs[t % 2][down, along + c:along + c + LANES] + bias
                    p = jnp.exp(score - jnp.max(score, axis=0, keepdims=True))
                    p = p * (1.0 / jnp.sum(p, axis=0, keepdims=True))
                    pt[s, t * HEADS_PER + h, :, c:c + LANES] = p.astype(BF16)
            v_t = vt[s, t]
            out = jnp.concatenate([mm(v_t[h * HEAD:(h + 1) * HEAD], pt[s, t * HEADS_PER + h]) for h in range(HEADS_PER)], axis=0)
            ot32[s, t] = out
            outb = out.astype(BF16)
            otb[t, :, rows] = outb
            dqkv[t, rows] = outb.T

    w_out = wide(w, 3)
    x1[...] = e_s[...] + mm(flat(dqkv, 0, TILES), w_out) + vec_ref[5:6]

    @pl.loop(0, TOK // 128, unroll=2)
    def _(r):
        rows = pl.ds(pl.multiple_of(r * 128, 128), 128)
        xhat, _ = norm_stats(x1[rows])
        nm[rows] = (xhat * vec_ref[6:7] + vec_ref[7:8]).astype(BF16)

    nmt[...] = nm[...].T
    y_s[...] = jnp.zeros_like(y_s)
    dnm[...] = jnp.zeros_like(dnm)

    @pl.when(step == 0)
    def _():
        weights('wait', 4, 8)
        for copy in grad_loads():
            copy.wait()

    @pl.loop(0, 4)
    def _(c):
        g = grad_rows()
        w_up = wide(w, 4 + c)
        u = mm(nm[...], w_up) + bup_ref[c]
        a, slope = gelu_pair(u)
        ab = a.astype(BF16)
        w_down = wide(w, 8 + c)
        du = mm_t(g, w_down) * slope
        dbup[c] += fold8(du)
        dub = du.astype(BF16)
        y_s[...] += mm(ab, w_down)
        dnm[...] += mm_t(dub, w_up)
        add_blocks(acc, 8 + c, mm(ab.T, g))
        add_blocks(acc, 4 + c, mm(nmt[...], dub))

    @pl.when(step == STEPS - 1)
    def _():
        ship('start', 4, 8)

    @pl.loop(0, STEP_SEQS)
    def _(seq):
        for part in range(2):
            rows = pl.ds(pl.multiple_of(seq * SEQ, SEQ) + part * 128, 128)
            x = x1[rows]
            out = (x + y_s[rows] + vec_ref[8:9]).astype(BF16)
            (y_own, y_oth)[part][seq] = out
            xhat, rstd = norm_stats(x)
            d_n = dnm[rows]
            g32 = gbuf[step * STEP_SEQS + seq, part].astype(F32)
            dsum[3] += fold8(d_n * xhat)
            dsum[4] += fold8(d_n)
            d_r = g32 + norm_back(d_n, vec_ref[6:7], xhat, rstd)
            dsum[2] += fold8(d_r)
            dsum[5] += fold8(g32)
            y_s[rows] = d_r
            nm[rows] = d_r.astype(BF16)

    d_rb = nm[...]
    add_blocks(acc, 3, mm(otb[...].reshape(640, TOK), d_rb))
    d_o = mm(wide(w, 3), d_rb.T)
    for t in range(TILES):
        dot_s[t] = d_o[t * LANES:(t + 1) * LANES]

    @pl.loop(0, STEP_SEQS)
    def _(s):
        rows = pl.ds(pl.multiple_of(s * SEQ, SEQ), SEQ)
        bufs = (x1, dnm)
        outs = (nm, nmt)

        def slopes(t):
            stage(bufs[t % 2], mm(stack(vn[s, t]), dot_s[t, :, rows].astype(BF16)))

        slopes(0)
        for t in range(TILES):
            if t + 1 < TILES:
                slopes(t + 1)
            d_ot = dot_s[t, :, rows]
            prod = d_ot * ot32[s, t]
            ds_ref = outs[t % 2]
            for h in range(HEADS_PER):
                down, along = spot(h)
                delta = jnp.sum(prod[h * HEAD:(h + 1) * HEAD], axis=0, keepdims=True)
                for c in range(0, SEQ, LANES):
                    d_p = bufs[t % 2][down, along + c:along + c + LANES]
                    p = pt[s, t * HEADS_PER + h, :, c:c + LANES].astype(F32)
                    ds_ref[down, along + c:along + c + LANES] = (p * (d_p - delta[:, c:c + LANES])).astype(BF16)
            k_t, q_n = kt[s, t], qn[s, t]
            dqs = []
            for h in range(HEADS_PER):
                down, along = spot(h)
                dqs.append(mm(k_t[h * HEAD:(h + 1) * HEAD], ds_ref[down, along:along + SEQ]))
            dq = unturn(jnp.concatenate(dqs, axis=0), cos[:, :SEQ], sin[:, :SEQ], HEADS_PER) * HEAD ** -0.5
            dbq[t] += dq[:, :LANES] + dq[:, LANES:]
            dqkv[t, rows] = dq.astype(BF16).T
            dk = mm(ds_ref[:SEQ, :2 * SEQ], jnp.concatenate([q_n * pick[0], q_n * pick[2]], axis=0))
            dk = dk + mm(ds_ref[SEQ:2 * SEQ, :2 * SEQ], jnp.concatenate([q_n * pick[1], q_n * pick[3]], axis=0))
            p_wide = jnp.concatenate([pt[s, t * HEADS_PER + h] for h in range(HEADS_PER)], axis=1)
            dv = mm(p_wide, stack(d_ot.astype(BF16).T))
            low = lax.rem(lax.broadcasted_iota(jnp.int32, (SEQ, LANES), 1), HEAD) < HEAD // 2
            other = jnp.where(low, pltpu.roll(dk, LANES - HEAD // 2, 1), pltpu.roll(dk, HEAD // 2, 1))
            dk = dk * cosn_ref[cp] + other * sinn_ref[cp]
            dbkv[0, t] += fold8(dk)
            dbkv[1, t] += fold8(dv)
            dqkv[TILES + t, rows] = dk.astype(BF16)
            dqkv[2 * TILES + t, rows] = dv.astype(BF16)

    for kind in range(3):
        add_blocks(acc, kind, mm(ht[...], flat(dqkv, kind * TILES, TILES)))
    dnm[...] = mm(flat(dqkv, 0, 15), wt[...].reshape(1920, 640))

    @pl.loop(0, TOK // 128, unroll=2)
    def _(r):
        rows = pl.ds(pl.multiple_of(r * 128, 128), 128)
        xhat, rstd = norm_stats(e_s[rows])
        d_n = dnm[rows]
        dsum[0] += fold8(d_n * xhat)
        dsum[1] += fold8(d_n)
        keep = jnp.concatenate([keep_ref[rows]] * TILES, axis=1)
        nm[rows] = ((norm_back(d_n, vec_ref[0:1], xhat, rstd) + y_s[rows]) * keep).astype(BF16)

    dtab[...] += mm(one_hot, nm[...])

    @pl.when(step == STEPS - 1)
    def _():
        ship('start', 0, 4)
        for t in range(TILES):
            lanes = slice(t * LANES, (t + 1) * LANES)
            sums = [dsum[0, :, lanes], dsum[1, :, lanes], dbq[t].T, dbkv[0, t], dbkv[1, t]]
            sums += [dsum[k, :, lanes] for k in range(2, 6)] + [dbup[k, :, lanes] for k in range(4)]
            small[t, :VOCAB] = dtab[:VOCAB, lanes]
            for k, value in enumerate(sums):
                small[t, VOCAB + k:VOCAB + k + 1] = jnp.sum(value, axis=0, keepdims=True)
            small[t, VOCAB + 13:] = jnp.zeros((SMALL_BLOCK - VOCAB - 13, LANES), F32)
        ship('wait', 4, 8)
        ship('wait', 0, 4)


def layer_call(tok, keep, mask, emb, vecs, bup, cos, sin, cosn, sinn, w_hbm, g_own, g_oth):
    vm = pltpu.VMEM
    dma = pltpu.SemaphoreType.DMA

    def whole(shape):
        return pl.BlockSpec(shape, lambda i: (0,) * len(shape))

    pair = pl.BlockSpec((STEP_SEQS, 128, 640), lambda i: (i, 0, 0))
    out_shape = (
        jax.ShapeDtypeStruct((SEQS, 128, 640), BF16),
        jax.ShapeDtypeStruct((SEQS, 128, 640), BF16),
        jax.ShapeDtypeStruct((64, 2 * PER, GROUP * NB, LANES), F32),
        jax.ShapeDtypeStruct((TILES, SMALL_BLOCK, LANES), F32),
    )
    out_specs = (pair, pair, ANY) + tuple(whole(o.shape) for o in out_shape[3:])
    in_specs = [
        pl.BlockSpec((1, 1, TOK), lambda i: (i, 0, 0)),
        pl.BlockSpec((1, 1, TOK), lambda i: (i, 0, 0)),
        pl.BlockSpec((1, 1, TOK), lambda i: (i, 0, 0)),
    ] + [whole(a.shape) for a in (emb, vecs, bup, cos, sin, cosn, sinn)] + [ANY] * 3
    halves = (STEP_SEQS, TILES, LANES, SEQ)
    flipped = (STEP_SEQS, TILES, SEQ, LANES)
    scratch = [
        vm((2 * PER, GROUP, 640, LANES), BF16), vm((15, LANES, 640), BF16), vm((2 * PER, GROUP, 640, LANES), F32), vm((SEQS, 2, 128, 640), BF16),
        vm((TOK, 640), F32), vm((640, TOK), BF16),
        vm(halves, BF16), vm(halves, BF16), vm(halves, BF16), vm(flipped, BF16), vm(flipped, BF16), vm(flipped, BF16),
        vm((STEP_SEQS, 20, SEQ, SEQ), BF16), vm(halves, F32), vm((TILES, LANES, TOK), BF16),
        vm((TOK, 640), F32), vm((TOK, 640), BF16), vm((640, TOK), BF16), vm((TOK, 640), F32), vm((TOK, 640), F32),
        vm((TILES, LANES, TOK), F32), vm((15, TOK, LANES), BF16), vm((TOK, LANES), F32), vm((TOK, LANES), F32), vm((1920, LANES), F32),
        vm((64, 640), F32), vm((6, 8, 640), F32), vm((TILES, LANES, LANES), F32), vm((2, TILES, 8, LANES), F32), vm((4, 8, 640), F32),
        dma((2,)), dma((2,)), dma((2,)),
    ]
    return pl.pallas_call(
        layer_kernel,
        grid=(STEPS,),
        out_shape=out_shape,
        in_specs=in_specs,
        out_specs=out_specs,
        scratch_shapes=scratch,
        compiler_params=pltpu.CompilerParams(dimension_semantics=('arbitrary',), vmem_limit_bytes=67043328),
        name='layer',
    )(tok, keep, mask, emb, vecs, bup, cos, sin, cosn, sinn, w_hbm, g_own, g_oth)


def prepare(tokens, lengths, positions, embed_table, vecs_all):
    n_seq, seq_len = tokens.shape
    is_mask = tokens == MASK_ID
    tok_valid = positions[None, :] < lengths[:, None]
    mask_count = jnp.sum(is_mask.astype(jnp.int32), axis=1)
    drop_scale = (1.0 - TRAIN_RATIO) / (1.0 - mask_count.astype(F32) / lengths.astype(F32))
    keep = jnp.where(is_mask | jnp.logical_not(tok_valid), 0.0, drop_scale[:, None])
    mask = jnp.where(tok_valid, 0.0, NEG_BIG).astype(F32)
    emb = jnp.pad(embed_table, ((0, 64 - embed_table.shape[0]), (0, 0)))
    rows = [x.reshape(STEPS, 1, TOK) for x in (tokens, keep, mask)]
    return (*rows, emb, *rope_tables(seq_len // 2))


def rope_tables(half):
    inv_freq = (1.0 / (np.float32(ROPE_BASE) ** (np.arange(0, HEAD, 2, dtype=np.float32) / np.float32(HEAD)))).astype(np.float32)
    tables = []
    for cp in range(2):
        positions = np.concatenate([np.arange(half) + cp * half, np.arange(half) + (1 - cp) * half]).astype(np.float32)
        angles = (positions[:, None] * inv_freq[None, :]).astype(np.float64)
        cos, sin = np.cos(angles), np.sin(angles)
        tables.append((
            np.tile(cos.T, (1, STEP_SEQS)), np.tile(sin.T, (1, STEP_SEQS)),
            np.tile(cos, (1, 8)), np.tile(np.concatenate([sin, -sin], axis=1), (1, 4)),
        ))
    return tuple(jnp.asarray(np.stack(pair), F32) for pair in zip(*tables))


def solution(mesh):
    chips = mesh.shape['fsdp']

    def local_step(tokens, lengths, embed_table, layer_vecs, w_qkv, w_out, w_up, b_up, w_down, grad_out):
        f32 = jnp.float32
        cp = lax.axis_index('cp')
        chip = lax.axis_index('fsdp')
        n_seq, seq_loc = tokens.shape
        half = n_seq // 2
        rows = w_qkv.shape[0]
        vocab, width = embed_table.shape
        w_loc = jnp.concatenate([
            w_qkv.reshape(rows, 15, 128).transpose(1, 0, 2),
            w_out.reshape(rows, 5, 128).transpose(1, 0, 2),
            w_up.reshape(rows, chips, 4, NB).transpose(2, 1, 3, 0).reshape(20, 128, rows).transpose(0, 2, 1),
            w_down.reshape(4, NB, 5, 128).transpose(0, 2, 1, 3).reshape(20, NB, 128),
        ], axis=0)
        s_loc = jnp.pad(jnp.concatenate([layer_vecs.reshape(-1), b_up]), (0, 1024 - 130)).reshape(8, 128)
        w_all, s_all, g_oth, t_oth = gather_all(w_loc.reshape(2 * PER, GROUP * NB, 128), s_loc, grad_out, tokens)
        s_flat = s_all.reshape(chips, 1024)
        vecs_all = s_flat[:, :90].reshape(chips, 9, NB).transpose(1, 0, 2).reshape(9, width)
        up_b = s_flat[:, 90:130].reshape(chips, 4, NB).transpose(1, 0, 2).reshape(-1)
        start = half * cp
        tok_full = jnp.concatenate([lax.dynamic_slice_in_dim(tokens, start, half, 0), t_oth], axis=1)
        len_own = lax.dynamic_slice_in_dim(lengths, start, half, 0)
        positions = jnp.concatenate([cp * seq_loc + jnp.arange(seq_loc), (1 - cp) * seq_loc + jnp.arange(seq_loc)])
        tok, keep, mask, emb, cos, sin, cosn, sinn = prepare(tok_full, len_own, positions, embed_table, vecs_all)
        y_own, y_oth, g_all, small = layer_call(
            tok, keep, mask, emb, vecs_all, up_b.reshape(4, 1, 640), cos, sin, cosn, sinn, w_all.reshape(chips, 2 * PER, GROUP * NB, 128), grad_out, g_oth)
        small = small.reshape(2, SMALL_ROWS, 128)
        g_red, s_red, out_full = reduce_all(g_all.reshape(SIDE, SIDE, SIDE, 2 * PER, GROUP * NB, 128), small, y_own, y_oth)
        g_red = g_red.reshape(60, NB, 128)
        s_rows = s_red.reshape(TILES, SMALL_BLOCK, 128)[:, :VOCAB + 13].transpose(1, 0, 2).reshape(VOCAB + 13, width)
        d_embed = s_rows[:vocab]
        s_mine = lax.dynamic_slice(s_rows, (vocab, chip * NB), (13, NB))
        d_v = s_mine[:9]
        d_b = s_mine[9:].reshape(-1)
        d_qkv = g_red[:15].transpose(1, 0, 2).reshape(w_qkv.shape)
        d_wout = g_red[15:20].transpose(1, 0, 2).reshape(w_out.shape)
        d_wup = g_red[20:40].transpose(0, 2, 1).reshape(4, chips, NB, rows).transpose(3, 1, 0, 2).reshape(w_up.shape)
        d_wdown = g_red[40:60].reshape(4, 5, NB, 128).transpose(0, 2, 1, 3).reshape(w_down.shape)
        return out_full, d_embed, d_v, d_qkv, d_wout, d_wup, d_b, d_wdown

    in_specs = (P('fsdp', 'cp'), P('fsdp'), P(), P(None, 'fsdp'), P('fsdp', None, None, None), P('fsdp', None), P('fsdp', None), P('fsdp'), P('fsdp', None), P('fsdp', 'cp', None))
    out_specs = (P('fsdp', 'cp', None), P(), P(None, 'fsdp'), P('fsdp', None, None, None), P('fsdp', None), P('fsdp', None), P('fsdp'), P('fsdp', None))
    return jax.shard_map(local_step, mesh=mesh, in_specs=in_specs, out_specs=out_specs, check_vma=False)
```
